256 devices in a mesh: groups: 2 (over z), attn: 16 (over y, core), expert: 8 (over x).
Axes of the slice: x: 8, y: 8, z: 2, core: 2. Of those that a mesh axis runs over, the one named last changes fastest.
The devices are a block of a 8x8x16 slice.
Arguments:
- tokens: bfloat16 [4096, 4096], P(('groups', 'attn'), 'expert'), parts along dimension 0, may hold values from -6 to 6
- expert_ids: int32 [4096, 8], P(('groups', 'attn')), parts along dimension 0, may hold values from 0 to 63, all different within a row; in each aligned block of 128 rows (0 to 127, 128 to 255, ...) at most 48 rows name the same one
- gate_weight: bfloat16 [4096, 8], P(('groups', 'attn')), parts along dimension 0, may hold values from 0.049804688 to 0.29882812
- w_gate: bfloat16 [64, 4096, 768], P('attn', 'expert'), may hold values from -0.09375 to 0.09375
- w_up: bfloat16 [64, 4096, 768], P('attn', 'expert'), may hold values from -0.09375 to 0.09375
- w_down: bfloat16 [64, 768, 4096], P('attn', None, 'expert'), may hold values from -0.21875 to 0.21875
- query: bfloat16 [512, 64, 128], P(('groups', 'attn', 'expert')), parts along dimension 0, may hold values from -100 to 100
- cache_k: bfloat16 [512, 768, 4, 128], P(('groups', 'attn', 'expert')), parts along dimension 0, may hold values from -6 to 6
- cache_v: bfloat16 [512, 768, 4, 128], P(('groups', 'attn', 'expert')), parts along dimension 0, may hold values from -6 to 6
- lengths: int32 [512], P(('groups', 'attn', 'expert')), parts along dimension 0, may hold values from 2 to 768, as said below
Outputs:
- moe_out: bfloat16 [4096, 4096], P(('groups', 'attn'), 'expert'), parts along dimension 0
- attn_out: bfloat16 [512, 8192], P(('groups', 'attn', 'expert')), parts along dimension 0
The draws below stay inside these ranges and needn't reach their ends.
There are 2 independent parts, one for each index of `groups`. The reference program is written for one: setup_inputs(seed, part) draws one part's arguments, and reference() takes and returns one part's arrays. A program takes and returns all parts, laid end to end along the dimension named above; an argument that names none is the same for every part. Nothing has to cross between parts.
Inputs may be any that keep to these rules, and one draw needn't show every extreme that they name: `expert_ids`: each row names 8 different experts. In the rows of one index of attn (aligned blocks of 128 rows) no expert is named by more than 48 rows, and in some block some expert by exactly 48. `lengths`: some sequence has all 768 positions live.
All inputs are finite; a program needn't handle non-finite values.
Results may differ from the reference program's by a relative error of at most 0.025.
Values may be sent and summed in bfloat16 or wider, within the bound.
No kernel may reach another device: no remote copies, remote signals or barrier semaphores. Data moves between devices by JAX's collectives and lax.ppermute only.
A program may use at most 64 MiB of HBM per device.

```python
import math
import jax
import jax.numpy as jnp
import numpy as np
from jax import lax

D = 4096
FF = 768
TOPK = 8
TOK_DEV = 128
Q_HEADS = 64
KV_HEADS = 4
HEAD_DIM = 128
CTX = 768
EXPERTS = 64
TOKENS = 2048
SEQS = 256
FEAT_DEV = 512
CAPACITY = 256
SLOT = 48
N_EXPERT = 8


def attention_inputs(key):
    keys_key = jax.random.fold_in(key, 101)
    query_key = jax.random.fold_in(key, 102)
    shape_keys = (SEQS, CTX, KV_HEADS, HEAD_DIM)
    shape_query = (SEQS, Q_HEADS, HEAD_DIM)
    key_rows = jnp.clip(jax.random.normal(keys_key, shape_keys, jnp.float32), -6.0, 6.0)
    query_rows = jnp.clip(jax.random.normal(query_key, shape_query, jnp.float32), -6.0, 6.0)
    return (key_rows, query_rows)


def draw_query(key, part):
    return attention_inputs(key)[1].astype(jnp.bfloat16)


def draw_cache_k(key, part):
    return attention_inputs(key)[0].astype(jnp.bfloat16)


def draw_lengths(key, part):
    base_lengths = jax.random.randint(jax.random.fold_in(key, 201), (SEQS,), 2, CTX + 1, dtype=jnp.int32)
    full_index = jax.random.randint(jax.random.fold_in(key, 202), (), 0, SEQS, dtype=jnp.int32)
    return jnp.where(jnp.arange(SEQS, dtype=jnp.int32) == full_index, CTX, base_lengths).astype(jnp.int32)


def block_scale(own_key, shape, cuts, smallest, top_value):
    factor_of = 1.0
    for axis_at, shards_of in cuts:
        steps = jax.random.uniform(jax.random.fold_in(jax.random.fold_in(own_key, 6), axis_at), (shards_of,), jnp.float32, smallest / len(cuts), top_value / len(cuts))
        factor_of = factor_of * jnp.repeat(jnp.exp(steps), shape[axis_at] // shards_of).reshape((-1,) + (1,) * (len(shape) - 1 - axis_at))
    return factor_of


def deal_out(stream_key, own, number, rows, count, top, most, slope):
    order = jax.random.permutation(stream_key, count)
    crowded, ordinary = shares(count, rows * top, most, slope, True), shares(count, rows * top, most, slope, False)
    places = jnp.arange(count)

    def named(sizes, offset_by):
        used = int((sizes > 0).sum())
        fixed = max(1, used // 4)
        passed = fixed + (places - fixed + offset_by * (used - fixed)) % max(1, count - fixed)
        return jnp.zeros((count,), jnp.int32).at[order[jnp.where(places < fixed, places, passed)]].set(jnp.asarray(sizes, jnp.int32))

    sizes = jnp.where(number % 4 == 0, named(crowded, number // 4), named(ordinary, number - number // 4 - 1))
    mixed = jax.random.permutation(jax.random.fold_in(own, 3), count)
    donor, taker = mixed[0:count // 2 * 2:2], mixed[1:count // 2 * 2:2]
    margin = jnp.minimum(sizes[donor] - 1, most - sizes[taker]) // 2
    margin = jnp.where((donor == order[0]) | (taker == order[0]) | (sizes[taker] == 0), 0, jnp.maximum(margin, 0))
    passed = jax.random.randint(jax.random.fold_in(own, 4), (count // 2,), 0, 1 << 20) % (margin + 1)
    sizes = sizes.at[donor].add(-passed).at[taker].add(passed)
    items = jnp.searchsorted(jnp.cumsum(sizes), jnp.arange(rows * top), side="right").astype(jnp.int32)
    table = items.reshape(top, rows).T
    table = table[jax.random.permutation(jax.random.fold_in(own, 1), rows)]
    offset_by = jax.random.randint(jax.random.fold_in(own, 2), (rows, 1), 0, top)
    return jnp.take_along_axis(table, (jnp.arange(top)[None, :] + offset_by) % top, axis=1)


def shares(number_of, total, reach, slope, full):
    portions = [(1 << 20) // math.isqrt(rank ** slope) + 1 for rank in range(1, number_of + 1)]
    largest = reach if full else min(reach, max(-(-total // number_of), total * portions[0] // sum(portions)))
    least = 1 if total - largest >= number_of - 1 else 0
    given, rest = [largest] + [least] * (number_of - 1), total - largest - least * (number_of - 1)
    while rest > 0:
        movable = [i for i in range(1, number_of) if given[i] < largest] or [i for i in range(1, number_of) if given[i] < reach]
        mass, remaining = sum([portions[i] for i in movable]), rest
        for i in movable:
            addition = min(reach - given[i], max(1, remaining * portions[i] // mass), rest)
            given[i] = given[i] + addition
            rest = rest - addition
    return np.array(given)


def centred(rng, extent, scale, reach, split=(), held_as=jnp.bfloat16):
    values = scale * jax.random.normal(rng, extent, jnp.float32)
    if split:
        values = values * block_scale(rng, extent, split, -0.22, 0.18)
    return jnp.clip(values, -reach, reach).astype(held_as)


def setup_inputs(seed: int = 0, part: int = 0) -> dict:
    keys = jax.random.split(jax.random.key(seed), 11)
    own_keys = jax.random.split(jax.random.fold_in(keys[10], part), 11)
    tokens = centred(own_keys[0], (TOKENS, D), 1.0, 6.0, ((0, 16), (1, 8)))
    expert_ids_keys = jax.random.split(jax.random.fold_in(own_keys[1], 1), TOKENS // TOK_DEV)
    expert_ids_turns = jax.random.permutation(jax.random.fold_in(own_keys[1], 3), TOKENS // TOK_DEV)
    expert_ids = jax.vmap(lambda own, number: deal_out(jax.random.fold_in(own_keys[1], 2), own, number, TOK_DEV, EXPERTS, TOPK, SLOT, 2))(expert_ids_keys, expert_ids_turns).reshape((TOKENS, TOPK))
    gate_weight = jnp.clip(0.049804688 + 0.24902344 * jax.random.uniform(own_keys[2], (TOKENS, TOPK), jnp.float32) ** block_scale(own_keys[2], (TOKENS, TOPK), ((0, 16),), -0.2, 0.2), 0.049804688, 0.29882812).astype(jnp.bfloat16)
    w_gate = centred(keys[3], (EXPERTS, D, FF), D ** -0.5, 0.09375, ((0, 16), (1, 8)))
    w_up = centred(keys[4], (EXPERTS, D, FF), D ** -0.5, 0.09375, ((0, 16), (1, 8)))
    w_down = centred(keys[5], (EXPERTS, FF, D), FF ** -0.5, 0.21875, ((0, 16), (2, 8)))
    query = draw_query(jax.random.fold_in(jax.random.fold_in(keys[10], part), 71), part)
    cache_k = draw_cache_k(jax.random.fold_in(jax.random.fold_in(keys[10], part), 71), part)
    cache_v = centred(own_keys[8], (SEQS, CTX, KV_HEADS, HEAD_DIM), 1.0, 6.0, ((0, 128),))
    lengths = draw_lengths(jax.random.fold_in(jax.random.fold_in(keys[10], part), 71), part)
    return {"tokens": tokens, "expert_ids": expert_ids, "gate_weight": gate_weight, "w_gate": w_gate, "w_up": w_up, "w_down": w_down, "query": query, "cache_k": cache_k, "cache_v": cache_v, "lengths": lengths}


def one_expert(operands):
    expert_rows, gate_mat, up_mat, down_mat = operands
    blocked = expert_rows.astype(jnp.float32).reshape(CAPACITY, N_EXPERT, FEAT_DEV)
    both_mats = jnp.concatenate([gate_mat, up_mat], axis=1).astype(jnp.float32).reshape(N_EXPERT, FEAT_DEV, 2 * FF)
    partials = jnp.einsum("rbd,bdf->brf", blocked, both_mats)
    rounded = lax.optimization_barrier(partials.astype(jnp.bfloat16))
    both_sums = jnp.sum(rounded.astype(jnp.float32), axis=0)
    hidden = (jax.nn.silu(both_sums[:, :FF]) * both_sums[:, FF:]).astype(jnp.bfloat16)
    return jnp.dot(hidden, down_mat, preferred_element_type=jnp.float32).astype(jnp.bfloat16)


def reference(tokens, expert_ids, gate_weight, w_gate, w_up, w_down, query, cache_k, cache_v, lengths):
    total_rows = tokens.shape[0]
    experts = w_gate.shape[0]
    wanted = jnp.arange(experts, dtype=jnp.int32)
    member = jnp.any(expert_ids[:, :, None] == wanted[None, None, :], axis=1).astype(jnp.int32)
    position = jnp.cumsum(member, axis=0, dtype=jnp.int32) - member
    taken = (member > 0) & (position < CAPACITY)
    target = jnp.where(taken, wanted[None, :] * CAPACITY + position, experts * CAPACITY)
    owners = jnp.broadcast_to(jnp.arange(total_rows, dtype=jnp.int32)[:, None], (total_rows, experts))
    token_index = jnp.full((experts * CAPACITY,), total_rows, jnp.int32).at[target.reshape(-1)].set(owners.reshape(-1), mode="drop")
    padded = jnp.concatenate([tokens, jnp.zeros((1, D), tokens.dtype)], axis=0)
    packed = padded[token_index].reshape(experts, CAPACITY, D)
    results = lax.map(one_expert, (packed, w_gate, w_up, w_down))
    results = lax.optimization_barrier(results)
    place_of = jnp.take_along_axis(position, expert_ids, axis=1)
    keep_mask = place_of < CAPACITY
    flat_index = jnp.where(keep_mask, expert_ids * CAPACITY + place_of, 0)
    picked = results.reshape(experts * CAPACITY, D)[flat_index]
    factor = jnp.where(keep_mask, gate_weight.astype(jnp.float32), 0.0)
    moe_out = jnp.sum(factor[:, :, None] * picked.astype(jnp.float32), axis=1).astype(jnp.bfloat16)

    seq_count = query.shape[0]
    grouped = query.astype(jnp.float32).reshape(seq_count, KV_HEADS, Q_HEADS // KV_HEADS, HEAD_DIM)
    scores = jnp.einsum("skgd,slkd->skgl", grouped, cache_k.astype(jnp.float32)) * (HEAD_DIM ** -0.5)
    live_mask = jnp.arange(CTX, dtype=jnp.int32)[None, None, None, :] < lengths[:, None, None, None]
    masked = jnp.where(live_mask, scores, -jnp.inf)
    row_peak = jnp.max(masked, axis=3, keepdims=True)
    weighted = jnp.exp(masked - row_peak)
    denominator = jnp.sum(weighted, axis=3, keepdims=True)
    prob_bf = lax.optimization_barrier((weighted / denominator).astype(jnp.bfloat16))
    attended = jnp.einsum("skgl,slkd->skgd", prob_bf.astype(jnp.float32), cache_v.astype(jnp.float32))
    attn_out = attended.reshape(seq_count, Q_HEADS * HEAD_DIM).astype(jnp.bfloat16)
    return (moe_out, attn_out)
```

```python
import functools

import jax
import jax.numpy as jnp
from jax import lax
from jax.experimental import pallas as pl
from jax.experimental.pallas import tpu as pltpu
from jax.sharding import PartitionSpec as P


F32 = jnp.float32
BF16 = jnp.bfloat16
META = 16


def grouped_attention(query, cache_k, cache_v, lengths):
    seq_count, head_total, head_size = query.shape
    context = cache_k.shape[1]
    kv_count = cache_k.shape[2]
    grouped = query.reshape(seq_count, kv_count, head_total // kv_count, head_size)
    scores = jnp.einsum(
        "skgd,slkd->skgl", grouped, cache_k, preferred_element_type=jnp.float32
    ) * head_size ** (-0.5)
    live_mask = (
        lax.broadcasted_iota(jnp.int32, (seq_count, 1, 1, context), 3)
        < lengths[:, None, None, None]
    )
    masked = jnp.where(live_mask, scores, -jnp.inf)
    row_peak = jnp.max(masked, axis=3, keepdims=True)
    weighted = jnp.exp(masked - row_peak)
    denominator = jnp.sum(weighted, axis=3, keepdims=True)
    prob_bf = (weighted / denominator).astype(jnp.bfloat16)
    attended = jnp.einsum("skgl,slkd->skgd", prob_bf, cache_v, preferred_element_type=jnp.float32)
    return attended.reshape(seq_count, head_total * head_size).astype(jnp.bfloat16)


def shift(value, axis, step):
    count = lax.axis_size(axis)
    return lax.ppermute(value, axis, [(i, (i + step) % count) for i in range(count)])


def swap_cores(value):
    return lax.ppermute(value, "attn", [(i, i ^ 1) for i in range(lax.axis_size("attn"))])


def pack_kernel(plan, half, info, *refs):
    n_ops = sum(len(p) for p in plan)
    ops = refs[:n_ops]
    wg, wu, out, route, tok, meta, mem, onehot = refs[n_ops:]
    n_blocks = len(plan)
    rows = tok.shape[0] // n_blocks
    local = wg.shape[0]
    ff = wg.shape[2]
    n_dest, _, dest_rows, _ = out.shape
    capacity = n_dest * dest_rows
    for i, p in enumerate(plan):
        at = info[1 + i]
        if len(p) == 1:
            tok[i * rows : (i + 1) * rows, :] = ops[p[0]][0:rows, :]
            meta[at] = ops[p[0]][rows : rows + META, 0:128].astype(F32)
        else:
            tok[i * rows : i * rows + half, :] = ops[p[0]][...]
            tok[i * rows + half : (i + 1) * rows, :] = ops[p[1]][0 : rows - half, :]
            meta[at] = ops[p[1]][rows - half : rows - half + META, 0:128].astype(F32)
    first = info[0]
    for b in range(n_blocks):
        ids = meta[b, 0:8, :]
        gates = meta[b, 8:16, :]
        for j in range(local):
            hit = ids == (first + j).astype(F32)
            mem[b * 8 + j : b * 8 + j + 1, :] = jnp.sum(jnp.where(hit, 1.0, 0.0), axis=0, keepdims=True)
            route[b, 4 + j : 5 + j, :] = jnp.sum(jnp.where(hit, gates, 0.0), axis=0, keepdims=True)
        mem[b * 8 + local : b * 8 + 8, :] = jnp.zeros((8 - local, rows), F32)
    member = mem[...]
    size = n_blocks * 8
    r = lax.broadcasted_iota(jnp.int32, (rows, rows), 0)
    c = lax.broadcasted_iota(jnp.int32, (rows, rows), 1)
    upper = jnp.where(r < c, 1.0, 0.0).astype(BF16)
    rr = lax.broadcasted_iota(jnp.int32, (size, size), 0)
    cc = lax.broadcasted_iota(jnp.int32, (size, size), 1)
    earlier = jnp.where((rr % 8 == cc % 8) & (cc // 8 < rr // 8), 1.0, 0.0).astype(BF16)
    member_b = member.astype(BF16)
    before = jnp.dot(earlier, member_b, preferred_element_type=F32).astype(BF16)
    place = jnp.dot(member_b, upper, preferred_element_type=F32) + jnp.dot(
        before, jnp.ones((rows, rows), BF16), preferred_element_type=F32
    )
    place = jnp.where((member > 0.5) & (place < capacity), place, -1.0)
    mem[...] = place
    for b in range(n_blocks):
        route[b, 0:local, :] = mem[b * 8 : b * 8 + local, :]
    row_id = lax.broadcasted_iota(jnp.int32, (capacity, rows), 0).astype(F32)
    for j in range(local):
        for i in range(n_blocks):
            at = info[1 + i]
            here = route[at, j : j + 1, :]
            onehot[:, i * rows : (i + 1) * rows] = jnp.where(row_id == here, 1.0, 0.0).astype(BF16)
        packed = jnp.dot(onehot[...], tok[...], preferred_element_type=F32).astype(BF16)
        gate = jnp.dot(packed, wg[j], preferred_element_type=F32).astype(BF16)
        up = jnp.dot(packed, wu[j], preferred_element_type=F32).astype(BF16)
        for d in range(n_dest):
            out[d, j, :, 0:ff] = gate[d * dest_rows : (d + 1) * dest_rows]
            out[d, j, :, ff:] = up[d * dest_rows : (d + 1) * dest_rows]


def combine_kernel(plan, info, *refs):
    n_ops = len(plan)
    ops = refs[:n_ops]
    wd, route, away, home, hid, res, mix = refs[n_ops:]
    local = wd.shape[0]
    capacity = hid.shape[1]
    n_dest, rows, _ = home.shape
    for op, (j0, slot) in zip(ops, plan):
        at = pl.multiple_of(info[slot], op.shape[1])
        for j in range(op.shape[0]):
            hid[j0 + j, pl.ds(at, op.shape[1]), :] = op[j]
    for j in range(local):
        res[j * capacity : (j + 1) * capacity, :] = jnp.dot(
            hid[j], wd[j], preferred_element_type=F32
        ).astype(BF16)
    r = lax.broadcasted_iota(jnp.int32, (rows, rows), 0)
    c = lax.broadcasted_iota(jnp.int32, (rows, rows), 1)
    eye = jnp.where(r == c, 1.0, 0.0).astype(BF16)
    col_id = lax.broadcasted_iota(jnp.int32, (rows, capacity), 1).astype(F32)
    core = info[0]
    step = 4
    for which, ref in ((1, away), (0, home)):
        side = jnp.where(core == which, 0, 1) if which == 1 else core
        for d0 in range(0, n_dest, step):
            for d in range(step):
                b = 2 * (d0 + d) + side
                rt = lax.dot_general(
                    eye, route[b].astype(BF16), (((1,), (1,)), ((), ())), preferred_element_type=F32
                )
                for j in range(local):
                    mix[d * rows : (d + 1) * rows, j * capacity : (j + 1) * capacity] = jnp.where(
                        col_id == rt[:, j : j + 1], rt[:, 4 + j : 5 + j], 0.0
                    ).astype(BF16)
            got = jnp.dot(mix[...], res[...], preferred_element_type=F32).astype(BF16)
            for d in range(step):
                ref[d0 + d] = got[d * rows : (d + 1) * rows]


VMEM_SPEC = pl.BlockSpec(memory_space=pltpu.VMEM)
SMEM_SPEC = pl.BlockSpec(memory_space=pltpu.SMEM)


def own_chunk(parts, at, lo, hi):
    return lax.dynamic_index_in_dim(parts[:, lo:hi], at, 0, keepdims=False)


def scatter_sum(pieces, axis, stride, me, count):
    half = count // 2
    totals = []
    legs = {}
    for way in (1, -1):
        for s in range(2):
            start = half if (way == 1) == (s == 0) else half - 1
            legs[(way, s)] = [start, pieces[s]((me + way * start) % count)]
    for hop in range(half, 0, -1):
        for way in (1, -1):
            for s in range(2):
                leg = legs[(way, s)]
                if leg[0] != hop:
                    continue
                got = shift(leg[1], axis, way * stride).astype(F32)
                if hop > 1:
                    mine = pieces[s]((me + way * (hop - 1)) % count).astype(F32)
                    legs[(way, s)] = [hop - 1, (got + mine).astype(BF16)]
                else:
                    legs[(way, s)] = [0, got]
    for s in range(2):
        totals.append(pieces[s](me).astype(F32) + legs[(1, s)][1] + legs[(-1, s)][1])
    return totals


def body(tokens, expert_ids, gate_weight, w_gate, w_up, w_down, query, cache_k, cache_v, lengths):
    rows, feat = tokens.shape
    local, _, ff = w_gate.shape
    attn_count = lax.axis_size("attn")
    n_expert = lax.axis_size("expert")
    chips = attn_count // 2
    top = expert_ids.shape[1]
    capacity = rows * top // local
    me = lax.axis_index("attn")
    col = lax.axis_index("expert")
    y = me // 2
    core = me % 2

    meta = jnp.concatenate([expert_ids.astype(BF16).T, gate_weight.T], axis=0)
    block = jnp.concatenate([tokens, jnp.pad(meta, ((0, 0), (0, feat - rows)))], axis=0)
    half = (rows + META) // 2
    ups, downs = [block], [block]
    others = [(0, swap_cores(block))]
    mine = [(0, block)]
    far = chips // 2
    for hop in range(1, far):
        ups.append(shift(ups[-1], "attn", 2))
        downs.append(shift(downs[-1], "attn", -2))
        mine += [(-hop, ups[-1]), (hop, downs[-1])]
        others += [(-hop, swap_cores(ups[-1])), (hop, swap_cores(downs[-1]))]
    far_up = shift(ups[-1][:half], "attn", 2)
    far_down = shift(downs[-1][half:], "attn", -2)
    operands, plan, info = [], [], [local * me]
    for flip, blocks, ends in (
        (0, mine, (far_up, far_down)),
        (1, others, (swap_cores(far_up), swap_cores(far_down))),
    ):
        for off, b in blocks:
            plan.append((len(operands),))
            operands.append(b)
            info.append(2 * ((y + off + chips) % chips) + (core ^ flip))
        plan.append((len(operands), len(operands) + 1))
        operands += list(ends)
        info.append(2 * ((y + far) % chips) + (core ^ flip))

    dest_rows = capacity // n_expert
    parts, route = pl.pallas_call(
        functools.partial(pack_kernel, plan, half),
        out_shape=(
            jax.ShapeDtypeStruct((n_expert, local, dest_rows, 2 * ff), BF16),
            jax.ShapeDtypeStruct((attn_count, 8, rows), F32),
        ),
        in_specs=[SMEM_SPEC] + [VMEM_SPEC] * (len(operands) + 2),
        out_specs=(VMEM_SPEC, VMEM_SPEC),
        scratch_shapes=[
            pltpu.VMEM((attn_count * rows, feat), BF16),
            pltpu.VMEM((attn_count, META, rows), F32),
            pltpu.VMEM((attn_count * 8, rows), F32),
            pltpu.VMEM((capacity, attn_count * rows), BF16),
        ],
        compiler_params=pltpu.CompilerParams(vmem_limit_bytes=40 << 20),
        cost_estimate=pl.CostEstimate(flops=4 * 10**9, bytes_accessed=12 * 10**6, transcendentals=0),
        name="pack",
    )(jnp.stack(info).astype(jnp.int32), *operands, w_gate, w_up)

    cut = local // 2
    pieces = [
        lambda at: own_chunk(parts, at, 0, cut),
        lambda at: own_chunk(parts, at, cut, local),
    ]
    sums = scatter_sum(pieces, "expert", 1, col, n_expert)
    hidden = [(jax.nn.silu(t[..., :ff]) * t[..., ff:]).astype(BF16) for t in sums]

    pieces_in, where, slots = [], [], [core]
    n_half = n_expert // 2
    got = {}
    for s in range(2):
        got[(s, 0)] = hidden[s]
    for hop in range(1, n_half + 1):
        for s in range(2):
            for way in (1, -1):
                if hop == n_half and (way == 1) != (s == 0):
                    continue
                got[(s, way * hop)] = shift(got[(s, way * (hop - 1))], "expert", way)
    for (s, off), value in got.items():
        pieces_in.append(value)
        where.append((s * cut, len(slots)))
        slots.append(((col - off + n_expert) % n_expert) * dest_rows)

    away, home = pl.pallas_call(
        functools.partial(combine_kernel, where),
        out_shape=(
            jax.ShapeDtypeStruct((chips, rows, feat), BF16),
            jax.ShapeDtypeStruct((chips, rows, feat), BF16),
        ),
        in_specs=[SMEM_SPEC] + [VMEM_SPEC] * (len(pieces_in) + 2),
        out_specs=(VMEM_SPEC, VMEM_SPEC),
        scratch_shapes=[
            pltpu.VMEM((local, capacity, ff), BF16),
            pltpu.VMEM((local * capacity, feat), BF16),
            pltpu.VMEM((4 * rows, local * capacity), BF16),
        ],
        compiler_params=pltpu.CompilerParams(vmem_limit_bytes=40 << 20),
        cost_estimate=pl.CostEstimate(flops=3 * 10**9, bytes_accessed=8 * 10**6, transcendentals=0),
        name="combine",
    )(jnp.stack(slots).astype(jnp.int32), *pieces_in, w_down, route)

    chip_sum = (home.astype(F32) + swap_cores(away).astype(F32)).astype(BF16)
    mid = rows // 2
    back = scatter_sum(
        [lambda at: own_chunk(chip_sum, at, 0, mid), lambda at: own_chunk(chip_sum, at, mid, rows)],
        "attn",
        2,
        y,
        chips,
    )
    moe_out = jnp.concatenate(back, axis=0).astype(BF16)
    attn_out = grouped_attention(query, cache_k, cache_v, lengths)
    return (moe_out, attn_out)


def solution(mesh):
    return jax.shard_map(
        body,
        mesh=mesh,
        in_specs=(
            P(("groups", "attn"), "expert"),
            P(("groups", "attn"), None),
            P(("groups", "attn"), None),
            P("attn", "expert", None),
            P("attn", "expert", None),
            P("attn", None, "expert"),
            P(("groups", "attn", "expert"), None, None),
            P(("groups", "attn", "expert"), None, None, None),
            P(("groups", "attn", "expert"), None, None, None),
            P(("groups", "attn", "expert")),
        ),
        out_specs=(P(("groups", "attn"), "expert"), P(("groups", "attn", "expert"), None)),
        check_vma=False,
    )
```

```python
import functools

import jax
import jax.numpy as jnp
from jax import lax
from jax.experimental import pallas as pl
from jax.experimental.pallas import tpu as pltpu
from jax.sharding import PartitionSpec as P


F32 = jnp.float32
BF16 = jnp.bfloat16
META = 16
VMEM_SPEC = pl.BlockSpec(memory_space=pltpu.VMEM)
SMEM_SPEC = pl.BlockSpec(memory_space=pltpu.SMEM)
HBM_SPEC = pl.BlockSpec(memory_space=pltpu.HBM)


def in_hbm(value):
    return pltpu.with_memory_space_constraint(value, pltpu.HBM)


def in_vmem(value):
    return pltpu.with_memory_space_constraint(value, pltpu.VMEM)


def attention_kernel(lengths, query, cache_k, cache_v, out):
    heads, size = query.shape[1:]
    spots, groups, _ = cache_k.shape[1:]
    columns = spots * groups
    keys = cache_k[0].reshape(columns, size)
    values = cache_v[0].reshape(columns, size)
    scores = lax.dot_general(
        query[0], keys, (((1,), (1,)), ((), ())), preferred_element_type=F32
    ) * size ** (-0.5)
    place = lax.broadcasted_iota(jnp.int32, (heads, columns), 1)
    head = lax.broadcasted_iota(jnp.int32, (heads, columns), 0)
    live = (place % groups == head // (heads // groups)) & (
        place < lengths[pl.program_id(0)] * groups
    )
    masked = jnp.where(live, scores, -jnp.inf)
    weighted = jnp.exp(masked - jnp.max(masked, axis=1, keepdims=True))
    prob = (weighted / jnp.sum(weighted, axis=1, keepdims=True)).astype(BF16)
    out[0] = jnp.dot(prob, values, preferred_element_type=F32).astype(BF16)


def grouped_attention(query, cache_k, cache_v, lengths):
    count, heads, size = query.shape
    _, spots, groups, _ = cache_k.shape
    cache = pl.BlockSpec((1, spots, groups, size), lambda i: (i, 0, 0, 0))
    row = pl.BlockSpec((1, heads, size), lambda i: (i, 0, 0))
    out = pl.pallas_call(
        attention_kernel,
        grid=(count,),
        out_shape=jax.ShapeDtypeStruct((count, heads, size), BF16),
        in_specs=[SMEM_SPEC, row, cache, cache],
        out_specs=row,
        compiler_params=pltpu.CompilerParams(vmem_limit_bytes=12 << 20),
        cost_estimate=pl.CostEstimate(
            flops=10**9, bytes_accessed=3 * 10**6, transcendentals=4 * 10**5
        ),
        name="attention",
    )(lengths, query, in_hbm(cache_k), in_hbm(cache_v))
    return out.reshape(count, heads * size)


def shift(value, axis, step):
    count = lax.axis_size(axis)
    return lax.ppermute(value, axis, [(i, (i + step) % count) for i in range(count)])


def swap_cores(value):
    return lax.ppermute(value, "attn", [(i, i ^ 1) for i in range(lax.axis_size("attn"))])


def pack_kernel(plan, half, info, *refs):
    n_ops = 1 + max(op for p in plan for op, _ in p)
    ops = refs[:n_ops]
    wg_hbm, wu_hbm, out, route, tok, meta, mem, onehot, wg, wu, sems = refs[n_ops:]
    n_blocks = len(plan)
    rows = tok.shape[0] // n_blocks
    local = wg.shape[0]
    ff = wg.shape[2]
    n_dest, _, dest_rows, _ = out.shape
    capacity = n_dest * dest_rows

    def fetch(j):
        return (
            pltpu.make_async_copy(wg_hbm.at[j], wg.at[j], sems.at[0, j]),
            pltpu.make_async_copy(wu_hbm.at[j], wu.at[j], sems.at[1, j]),
        )

    for j in range(local):
        for copy in fetch(j):
            copy.start()
    for i, p in enumerate(plan):
        at = info[1 + i]
        op, r0 = p[0]
        if len(p) == 1:
            tok[i * rows : (i + 1) * rows, :] = ops[op][r0 : r0 + rows, :]
            meta[at] = ops[op][r0 + rows : r0 + rows + META, 0:128].astype(F32)
        else:
            op1, r1 = p[1]
            tok[i * rows : i * rows + half, :] = ops[op][r0 : r0 + half, :]
            tok[i * rows + half : (i + 1) * rows, :] = ops[op1][r1 : r1 + rows - half, :]
            meta[at] = ops[op1][r1 + rows - half : r1 + half, 0:128].astype(F32)
    first = info[0]

    def members(b, carry):
        ids = meta[b, 0:8, :]
        gates = meta[b, 8:16, :]
        for j in range(local):
            hit = ids == (first + j).astype(F32)
            mem[b, j : j + 1, :] = jnp.sum(jnp.where(hit, 1.0, 0.0), axis=0, keepdims=True)
            route[b, 4 + j : 5 + j, :] = jnp.sum(jnp.where(hit, gates, 0.0), axis=0, keepdims=True)
        mem[b, local:8, :] = jnp.zeros((8 - local, rows), F32)
        return carry

    lax.fori_loop(0, n_blocks, members, 0, unroll=4)
    size = n_blocks * 8
    member = mem[...].reshape(size, rows)
    r = lax.broadcasted_iota(jnp.int32, (rows, rows), 0)
    c = lax.broadcasted_iota(jnp.int32, (rows, rows), 1)
    upper = jnp.where(r < c, 1.0, 0.0).astype(BF16)
    rr = lax.broadcasted_iota(jnp.int32, (size, size), 0)
    cc = lax.broadcasted_iota(jnp.int32, (size, size), 1)
    earlier = jnp.where((rr % 8 == cc % 8) & (cc // 8 < rr // 8), 1.0, 0.0).astype(BF16)
    member_b = member.astype(BF16)
    before = jnp.dot(earlier, member_b, preferred_element_type=F32).astype(BF16)
    place = jnp.dot(member_b, upper, preferred_element_type=F32) + jnp.dot(
        before, jnp.ones((rows, rows), BF16), preferred_element_type=F32
    )
    place = jnp.where((member > 0.5) & (place < capacity), place, -1.0)
    mem[...] = place.reshape(n_blocks, 8, rows)
    route[:, 0:local, :] = mem[:, 0:local, :]
    row_id = lax.broadcasted_iota(jnp.int32, (capacity, rows), 0).astype(F32)

    def expert(j, carry):
        for i in range(n_blocks):
            here = mem[info[1 + i], pl.ds(j, 1), :]
            onehot[:, i * rows : (i + 1) * rows] = jnp.where(row_id == here, 1.0, 0.0).astype(BF16)
        packed = jnp.dot(onehot[...], tok[...], preferred_element_type=F32).astype(BF16)
        for copy in fetch(j):
            copy.wait()
        gate = jnp.dot(packed, wg[j], preferred_element_type=F32).astype(BF16)
        up = jnp.dot(packed, wu[j], preferred_element_type=F32).astype(BF16)
        out[:, j, :, 0:ff] = gate.reshape(n_dest, dest_rows, ff)
        out[:, j, :, ff:] = up.reshape(n_dest, dest_rows, ff)
        return carry

    lax.fori_loop(0, local, expert, 0)


def mix_rows(side, route, res, mix, ref):
    n_dest, rows, _ = ref.shape
    group = mix.shape[0] // rows
    local = 4
    capacity = res.shape[0] // local
    r = lax.broadcasted_iota(jnp.int32, (rows, rows), 0)
    c = lax.broadcasted_iota(jnp.int32, (rows, rows), 1)
    eye = jnp.where(r == c, 1.0, 0.0).astype(BF16)
    col_id = lax.broadcasted_iota(jnp.int32, (rows, capacity), 1).astype(F32)

    def some(g, carry):
        for d in range(group):
            b = 2 * (g * group + d) + side
            rt = lax.dot_general(
                eye, route[b].astype(BF16), (((1,), (1,)), ((), ())), preferred_element_type=F32
            )
            for j in range(local):
                mix[d * rows : (d + 1) * rows, j * capacity : (j + 1) * capacity] = jnp.where(
                    col_id == rt[:, j : j + 1], rt[:, 4 + j : 5 + j], 0.0
                ).astype(BF16)
        got = jnp.dot(mix[...], res[...], preferred_element_type=F32).astype(BF16)
        ref[pl.ds(g * group, group)] = got.reshape(group, rows, got.shape[1])
        return carry

    lax.fori_loop(0, n_dest // group, some, 0)


def down_kernel(plan, info, *refs):
    n_ops = len(plan)
    ops = refs[:n_ops]
    wd_hbm, route, away, res, hid, mix, wd, sems = refs[n_ops:]
    local = wd.shape[0]
    capacity = hid.shape[1]

    def fetch(j):
        return pltpu.make_async_copy(wd_hbm.at[j], wd.at[j], sems.at[j])

    for j in range(local):
        fetch(j).start()
    for op, (j0, slot) in zip(ops, plan):
        at = pl.multiple_of(info[slot], op.shape[1])
        for j in range(op.shape[0]):
            hid[j0 + j, pl.ds(at, op.shape[1]), :] = op[j]

    def expert(j, carry):
        fetch(j).wait()
        res[pl.ds(pl.multiple_of(j * capacity, capacity), capacity), :] = jnp.dot(
            hid[j], wd[j], preferred_element_type=F32
        ).astype(BF16)
        return carry

    lax.fori_loop(0, local, expert, 0)
    mix_rows(1 - info[0], route, res, mix, away)


def home_kernel(info, res, route, home, mix):
    mix_rows(info[0], route, res, mix, home)


def own_chunk(parts, at, lo, hi):
    return lax.dynamic_index_in_dim(parts[:, lo:hi], at, 0, keepdims=False)


def scatter_sum(pieces, axis, stride, at):
    count = len(at)
    half = count // 2
    legs = {}
    for way in (1, -1):
        for s in range(2):
            start = half if (way == 1) == (s == 0) else half - 1
            legs[(way, s)] = [start, pieces[s](at[way * start % count]).astype(BF16)]
    for hop in range(half, 0, -1):
        for way in (1, -1):
            for s in range(2):
                leg = legs[(way, s)]
                if leg[0] != hop:
                    continue
                got = shift(leg[1], axis, way * stride).astype(F32)
                if hop > 1:
                    mine = pieces[s](at[way * (hop - 1) % count]).astype(F32)
                    legs[(way, s)] = [hop - 1, (got + mine).astype(BF16)]
                else:
                    legs[(way, s)] = [0, got]
    return [pieces[s](at[0]).astype(F32) + legs[(1, s)][1] + legs[(-1, s)][1] for s in range(2)]


def scatter_sum_whole(piece, axis, stride, at, rows):
    count = len(at)
    half = count // 2
    mid = rows // 2
    span = {1: (0, mid), -1: (mid, rows)}
    legs = {way: piece(at[half], *span[way]).astype(BF16) for way in (1, -1)}
    for hop in range(half, 0, -1):
        for way in (1, -1):
            got = shift(legs[way], axis, way * stride).astype(F32)
            if hop == half:
                lo, hi = span[way]
                both = piece(at[way * (hop - 1) % count], lo, hi).astype(F32) + got
                rest = piece(at[way * (hop - 1) % count], mid - lo, rows + mid - hi).astype(F32)
                parts = (both, rest) if way == 1 else (rest, both)
                legs[way] = jnp.concatenate(parts, axis=0).astype(BF16)
            elif hop > 1:
                legs[way] = (piece(at[way * (hop - 1) % count], 0, rows).astype(F32) + got).astype(
                    BF16
                )
            else:
                legs[way] = got
    return piece(at[0], 0, rows).astype(F32) + legs[1] + legs[-1]


def body(tokens, expert_ids, gate_weight, w_gate, w_up, w_down, query, cache_k, cache_v, lengths):
    rows, feat = tokens.shape
    local, _, ff = w_gate.shape
    attn_count = lax.axis_size("attn")
    n_expert = lax.axis_size("expert")
    chips = attn_count // 2
    top = expert_ids.shape[1]
    capacity = rows * top // local
    me = lax.axis_index("attn")
    col = lax.axis_index("expert")
    y = me // 2
    core = me % 2
    far = chips // 2
    dest_rows = capacity // n_expert

    y_at = [lax.rem(y + k, chips) for k in range(chips)]
    x_at = [lax.rem(col + k, n_expert) for k in range(n_expert)]
    offsets = [0]
    for hop in range(1, far):
        offsets += [-hop, hop]
    offsets.append(far)
    pack_info = [local * me]
    for flip in (0, 1):
        pack_info += [2 * y_at[off % chips] + (core ^ flip) for off in offsets]
    row_at = [core] + [x_at[k] * dest_rows for k in range(n_expert)]
    pack_info = jnp.stack(pack_info).astype(jnp.int32)
    row_at = jnp.stack(row_at).astype(jnp.int32)
    core_at = core.reshape(1).astype(jnp.int32)
    tokens, pack_info, row_at, core_at, y_at, x_at = lax.optimization_barrier(
        (tokens, pack_info, row_at, core_at, y_at, x_at)
    )

    meta = jnp.concatenate([expert_ids.astype(BF16).T, gate_weight.T], axis=0)
    block = jnp.concatenate([tokens, jnp.pad(meta, ((0, 0), (0, feat - rows)))], axis=0)
    half = (rows + META) // 2
    attn_out = grouped_attention(query, cache_k, cache_v, lengths)
    up = down = block
    mine, others = [block], [swap_cores(block)]
    for hop in range(1, far):
        up, down = shift(up, "attn", 2), shift(down, "attn", -2)
        if hop == 1:
            up, down, attn_out = lax.optimization_barrier((up, down, attn_out))
        mine += [up, down]
        others.append(swap_cores(jnp.concatenate([up, down], axis=0)))
    ends = [shift(up[:half], "attn", 2), shift(down[half:], "attn", -2)]
    mine += ends
    others.append(swap_cores(jnp.concatenate(ends, axis=0)))
    operands = mine + others
    height = rows + META
    plan = [((i, 0),) for i in range(len(mine) - 2)] + [((len(mine) - 2, 0), (len(mine) - 1, 0))]
    plan.append(((len(mine), 0),))
    for hop in range(1, far):
        plan += [((len(mine) + hop, 0),), ((len(mine) + hop, height),)]
    plan.append(((len(operands) - 1, 0), (len(operands) - 1, half)))

    parts, route = pl.pallas_call(
        functools.partial(pack_kernel, plan, half),
        out_shape=(
            jax.ShapeDtypeStruct((n_expert, local, dest_rows, 2 * ff), BF16),
            jax.ShapeDtypeStruct((attn_count, 8, rows), F32),
        ),
        in_specs=[SMEM_SPEC] + [VMEM_SPEC] * len(operands) + [HBM_SPEC] * 2,
        out_specs=(VMEM_SPEC, VMEM_SPEC),
        scratch_shapes=[
            pltpu.VMEM((attn_count * rows, feat), BF16),
            pltpu.VMEM((attn_count, META, rows), F32),
            pltpu.VMEM((attn_count, 8, rows), F32),
            pltpu.VMEM((capacity, attn_count * rows), BF16),
            pltpu.VMEM(w_gate.shape, BF16),
            pltpu.VMEM(w_up.shape, BF16),
            pltpu.SemaphoreType.DMA((2, local)),
        ],
        compiler_params=pltpu.CompilerParams(vmem_limit_bytes=13 << 20),
        cost_estimate=pl.CostEstimate(flops=4 * 10**9, bytes_accessed=12 * 10**6, transcendentals=0),
        name="pack",
    )(pack_info, *map(in_vmem, operands), in_hbm(w_gate), in_hbm(w_up))

    cut = local // 2
    pieces = [
        lambda at: own_chunk(parts, at, 0, cut),
        lambda at: own_chunk(parts, at, cut, local),
    ]
    sums = scatter_sum(pieces, "expert", 1, x_at)
    hidden = [(jax.nn.silu(t[..., :ff]) * t[..., ff:]).astype(BF16) for t in sums]

    pieces_in, where = [], []
    n_half = n_expert // 2
    got = {}
    for s in range(2):
        got[(s, 0)] = hidden[s]
    for hop in range(1, n_half + 1):
        for s in range(2):
            for way in (1, -1):
                if hop == n_half and (way == 1) != (s == 0):
                    continue
                got[(s, way * hop)] = shift(got[(s, way * (hop - 1))], "expert", way)
    for (s, off), value in got.items():
        pieces_in.append(value)
        where.append((s * cut, 1 + (-off) % n_expert))

    away, res = pl.pallas_call(
        functools.partial(down_kernel, where),
        out_shape=(
            jax.ShapeDtypeStruct((chips, rows, feat), BF16),
            jax.ShapeDtypeStruct((local * capacity, feat), BF16),
        ),
        in_specs=[SMEM_SPEC] + [VMEM_SPEC] * len(pieces_in) + [HBM_SPEC, VMEM_SPEC],
        out_specs=(VMEM_SPEC, VMEM_SPEC),
        scratch_shapes=[
            pltpu.VMEM((local, capacity, ff), BF16),
            pltpu.VMEM((4 * rows, local * capacity), BF16),
            pltpu.VMEM(w_down.shape, BF16),
            pltpu.SemaphoreType.DMA((local,)),
        ],
        compiler_params=pltpu.CompilerParams(vmem_limit_bytes=(15 << 20) // 2),
        cost_estimate=pl.CostEstimate(flops=2 * 10**9, bytes_accessed=6 * 10**6, transcendentals=0),
        name="down",
    )(row_at, *map(in_vmem, pieces_in), in_hbm(w_down), in_vmem(route))
    swapped = swap_cores(away)
    home = pl.pallas_call(
        home_kernel,
        out_shape=jax.ShapeDtypeStruct((chips, rows, feat), BF16),
        in_specs=[SMEM_SPEC, VMEM_SPEC, VMEM_SPEC],
        out_specs=VMEM_SPEC,
        scratch_shapes=[pltpu.VMEM((4 * rows, local * capacity), BF16)],
        compiler_params=pltpu.CompilerParams(vmem_limit_bytes=(5 << 20) // 2),
        cost_estimate=pl.CostEstimate(flops=10**9, bytes_accessed=2 * 10**6, transcendentals=0),
        name="home",
    )(core_at, in_vmem(res), in_vmem(route))

    def chip_sum(at, lo, hi):
        return (
            own_chunk(home, at, lo, hi).astype(F32) + own_chunk(swapped, at, lo, hi).astype(F32)
        )

    moe_out = scatter_sum_whole(chip_sum, "attn", 2, y_at, rows).astype(BF16)
    return (moe_out, attn_out)


def solution(mesh):
    return jax.shard_map(
        body,
        mesh=mesh,
        in_specs=(
            P(("groups", "attn"), "expert"),
            P(("groups", "attn"), None),
            P(("groups", "attn"), None),
            P("attn", "expert", None),
            P("attn", "expert", None),
            P("attn", None, "expert"),
            P(("groups", "attn", "expert"), None, None),
            P(("groups", "attn", "expert"), None, None, None),
            P(("groups", "attn", "expert"), None, None, None),
            P(("groups", "attn", "expert")),
        ),
        out_specs=(P(("groups", "attn"), "expert"), P(("groups", "attn", "expert"), None)),
        check_vma=False,
    )
```

```python
import functools

import jax
import jax.numpy as jnp
from jax import lax
from jax.experimental import pallas as pl
from jax.experimental.pallas import tpu as pltpu
from jax.sharding import PartitionSpec as P


F32 = jnp.float32
BF16 = jnp.bfloat16
META = 16
VMEM_SPEC = pl.BlockSpec(memory_space=pltpu.VMEM)
SMEM_SPEC = pl.BlockSpec(memory_space=pltpu.SMEM)
HBM_SPEC = pl.BlockSpec(memory_space=pltpu.HBM)


def sum_kernel(info, home, swapped, total, right, left):
    count, rows, _ = home.shape
    mid = rows // 2
    total[...] = (home[...].astype(F32) + swapped[...].astype(F32)).astype(BF16)
    right[0:rows, :] = total[info[2]]
    right[rows:, :] = total[info[4], 0:mid, :]
    left[0:rows, :] = total[info[count - 2]]
    left[rows:, :] = total[info[4], mid:, :]


def relay_kernel(info, total, right, left, far_right, far_left, near_right, near_left):
    count, rows, _ = total.shape
    mid = rows // 2
    here = total[info[3]]
    far_right[0:mid, :] = (here[0:mid].astype(F32) + right[rows:, :].astype(F32)).astype(BF16)
    far_right[mid:, :] = here[mid:]
    here = total[info[count - 3]]
    far_left[0:mid, :] = here[0:mid]
    far_left[mid:, :] = (here[mid:].astype(F32) + left[rows:, :].astype(F32)).astype(BF16)
    near_right[...] = (total[info[1]].astype(F32) + right[0:rows, :].astype(F32)).astype(BF16)
    near_left[...] = (total[info[count - 1]].astype(F32) + left[0:rows, :].astype(F32)).astype(BF16)


def finish_kernel(info, total, a, b, c, d, out):
    out[...] = (
        total[info[0]].astype(F32)
        + (a[...].astype(F32) + b[...].astype(F32))
        + (c[...].astype(F32) + d[...].astype(F32))
    ).astype(BF16)


def in_hbm(value):
    return pltpu.with_memory_space_constraint(value, pltpu.HBM)


def in_vmem(value):
    return pltpu.with_memory_space_constraint(value, pltpu.VMEM)


def attention_kernel(lengths, query, cache_k, cache_v, out):
    heads, size = query.shape[1:]
    spots, groups, _ = cache_k.shape[1:]
    columns = spots * groups
    keys = cache_k[0].reshape(columns, size)
    values = cache_v[0].reshape(columns, size)
    scores = lax.dot_general(
        query[0], keys, (((1,), (1,)), ((), ())), preferred_element_type=F32
    ) * size ** (-0.5)
    place = lax.broadcasted_iota(jnp.int32, (heads, columns), 1)
    head = lax.broadcasted_iota(jnp.int32, (heads, columns), 0)
    live = (place % groups == head // (heads // groups)) & (
        place < lengths[pl.program_id(0)] * groups
    )
    masked = jnp.where(live, scores, -jnp.inf)
    weighted = jnp.exp(masked - jnp.max(masked, axis=1, keepdims=True))
    prob = (weighted / jnp.sum(weighted, axis=1, keepdims=True)).astype(BF16)
    out[0] = jnp.dot(prob, values, preferred_element_type=F32).astype(BF16)


def grouped_attention(query, cache_k, cache_v, lengths):
    count, heads, size = query.shape
    _, spots, groups, _ = cache_k.shape
    cache = pl.BlockSpec((1, spots, groups, size), lambda i: (i, 0, 0, 0))
    row = pl.BlockSpec((1, heads, size), lambda i: (i, 0, 0))
    out = pl.pallas_call(
        attention_kernel,
        grid=(count,),
        out_shape=jax.ShapeDtypeStruct((count, heads, size), BF16),
        in_specs=[SMEM_SPEC, row, cache, cache],
        out_specs=row,
        compiler_params=pltpu.CompilerParams(vmem_limit_bytes=12 << 20),
        cost_estimate=pl.CostEstimate(
            flops=10**9, bytes_accessed=3 * 10**6, transcendentals=4 * 10**5
        ),
        name="attention",
    )(lengths, query, in_hbm(cache_k), in_hbm(cache_v))
    return out.reshape(count, heads * size)


def shift(value, axis, step):
    count = lax.axis_size(axis)
    return lax.ppermute(value, axis, [(i, (i + step) % count) for i in range(count)])


def swap_cores(value):
    return lax.ppermute(value, "attn", [(i, i ^ 1) for i in range(lax.axis_size("attn"))])


def expert_parts(j0, info, place, tok, wg_hbm, wu_hbm, wg, wu, sems, onehot, out, work):
    n_blocks = place.shape[0]
    rows = tok.shape[0] // n_blocks
    n_dest, here_count, dest_rows, ff2 = out.shape
    ff = ff2 // 2
    capacity = n_dest * dest_rows

    def fetch(j):
        return (
            pltpu.make_async_copy(wg_hbm.at[j0 + j], wg.at[j], sems.at[0, j]),
            pltpu.make_async_copy(wu_hbm.at[j0 + j], wu.at[j], sems.at[1, j]),
        )

    for j in range(here_count):
        for copy in fetch(j):
            copy.start()
    work()
    row_id = lax.broadcasted_iota(jnp.int32, (capacity, rows), 0).astype(F32)

    def expert(j, carry):
        for i in range(n_blocks):
            spot = place[info[1 + i], pl.ds(j0 + j, 1), :]
            onehot[:, i * rows : (i + 1) * rows] = jnp.where(row_id == spot, 1.0, 0.0).astype(BF16)
        packed = jnp.dot(onehot[...], tok[...], preferred_element_type=F32).astype(BF16)
        for copy in fetch(j):
            copy.wait()
        gate = jnp.dot(packed, wg[j], preferred_element_type=F32).astype(BF16)
        up = jnp.dot(packed, wu[j], preferred_element_type=F32).astype(BF16)
        out[:, j, :, 0:ff] = gate.reshape(n_dest, dest_rows, ff)
        out[:, j, :, ff:] = up.reshape(n_dest, dest_rows, ff)
        return carry

    lax.fori_loop(0, here_count, expert, 0)


def pack_kernel(plan, half, local, info, *refs):
    n_ops = 1 + max(op for p in plan for op, _ in p)
    ops = refs[:n_ops]
    wg_hbm, wu_hbm, out, route, tok, meta, mem, onehot, wg, wu, sems = refs[n_ops:]
    n_blocks = len(plan)
    rows = tok.shape[0] // n_blocks
    capacity = out.shape[0] * out.shape[2]

    def work():
        for i, p in enumerate(plan):
            at = info[1 + i]
            op, r0 = p[0]
            if len(p) == 1:
                tok[i * rows : (i + 1) * rows, :] = ops[op][r0 : r0 + rows, :]
                meta[at] = ops[op][r0 + rows : r0 + rows + META, 0:128].astype(F32)
            else:
                op1, r1 = p[1]
                tok[i * rows : i * rows + half, :] = ops[op][r0 : r0 + half, :]
                tok[i * rows + half : (i + 1) * rows, :] = ops[op1][r1 : r1 + rows - half, :]
                meta[at] = ops[op1][r1 + rows - half : r1 + half, 0:128].astype(F32)
        first = info[0]

        def members(b, carry):
            ids = meta[b, 0:8, :]
            gates = meta[b, 8:16, :]
            for j in range(local):
                hit = ids == (first + j).astype(F32)
                mem[b, j : j + 1, :] = jnp.sum(jnp.where(hit, 1.0, 0.0), axis=0, keepdims=True)
                route[b, 4 + j : 5 + j, :] = jnp.sum(
                    jnp.where(hit, gates, 0.0), axis=0, keepdims=True
                )
            mem[b, local:8, :] = jnp.zeros((8 - local, rows), F32)
            return carry

        lax.fori_loop(0, n_blocks, members, 0)
        size = n_blocks * 8
        member = mem[...].reshape(size, rows)
        r = lax.broadcasted_iota(jnp.int32, (rows, rows), 0)
        c = lax.broadcasted_iota(jnp.int32, (rows, rows), 1)
        upper = jnp.where(r < c, 1.0, 0.0).astype(BF16)
        rr = lax.broadcasted_iota(jnp.int32, (size, size), 0)
        cc = lax.broadcasted_iota(jnp.int32, (size, size), 1)
        earlier = jnp.where((rr % 8 == cc % 8) & (cc // 8 < rr // 8), 1.0, 0.0).astype(BF16)
        member_b = member.astype(BF16)
        before = jnp.dot(earlier, member_b, preferred_element_type=F32).astype(BF16)
        place = jnp.dot(member_b, upper, preferred_element_type=F32) + jnp.dot(
            before, jnp.ones((rows, rows), BF16), preferred_element_type=F32
        )
        place = jnp.where((member > 0.5) & (place < capacity), place, -1.0)
        mem[...] = place.reshape(n_blocks, 8, rows)
        route[:, 0:local, :] = mem[:, 0:local, :]

    expert_parts(0, info, route, tok, wg_hbm, wu_hbm, wg, wu, sems, onehot, out, work)


def pack_more_kernel(j0, info, tok, route, wg_hbm, wu_hbm, out, onehot, wg, wu, sems):
    expert_parts(
        j0, info, route, tok, wg_hbm, wu_hbm, wg, wu, sems, onehot, out, lambda: None
    )


def mix_rows(side, route, res, mix, ref):
    n_dest, rows, _ = ref.shape
    group = mix.shape[0] // rows
    local = 4
    capacity = res.shape[0] // local
    r = lax.broadcasted_iota(jnp.int32, (rows, rows), 0)
    c = lax.broadcasted_iota(jnp.int32, (rows, rows), 1)
    eye = jnp.where(r == c, 1.0, 0.0).astype(BF16)
    col_id = lax.broadcasted_iota(jnp.int32, (rows, capacity), 1).astype(F32)

    def some(g, carry):
        for d in range(group):
            b = 2 * (g * group + d) + side
            rt = lax.dot_general(
                eye, route[b].astype(BF16), (((1,), (1,)), ((), ())), preferred_element_type=F32
            )
            for j in range(local):
                mix[d * rows : (d + 1) * rows, j * capacity : (j + 1) * capacity] = jnp.where(
                    col_id == rt[:, j : j + 1], rt[:, 4 + j : 5 + j], 0.0
                ).astype(BF16)
        got = jnp.dot(mix[...], res[...], preferred_element_type=F32).astype(BF16)
        ref[pl.ds(g * group, group)] = got.reshape(group, rows, got.shape[1])
        return carry

    lax.fori_loop(0, n_dest // group, some, 0)


def down_kernel(plan, info, *refs):
    n_ops = len(plan)
    ops = refs[:n_ops]
    wd_hbm, route, away, res, hid, mix, wd, sems = refs[n_ops:]
    local = wd.shape[0]
    capacity = hid.shape[1]

    def fetch(j):
        return pltpu.make_async_copy(wd_hbm.at[j], wd.at[j], sems.at[j])

    for j in range(local):
        fetch(j).start()
    for op, (j0, slot) in zip(ops, plan):
        at = pl.multiple_of(info[slot], op.shape[1])
        for j in range(op.shape[0]):
            hid[j0 + j, pl.ds(at, op.shape[1]), :] = op[j]

    def expert(j, carry):
        fetch(j).wait()
        res[pl.ds(pl.multiple_of(j * capacity, capacity), capacity), :] = jnp.dot(
            hid[j], wd[j], preferred_element_type=F32
        ).astype(BF16)
        return carry

    lax.fori_loop(0, local, expert, 0)
    mix_rows(1 - info[0], route, res, mix, away)


def home_kernel(info, res, route, home, mix):
    mix_rows(info[0], route, res, mix, home)


def scatter_sum(pieces, axis, stride, at):
    count = len(at)
    half = count // 2
    legs = {}
    for way in (1, -1):
        for s in range(2):
            start = half if (way == 1) == (s == 0) else half - 1
            legs[(way, s)] = [start, pieces[s](at[way * start % count]).astype(BF16)]
    for hop in range(half, 0, -1):
        for way in (1, -1):
            for s in range(2):
                leg = legs[(way, s)]
                if leg[0] != hop:
                    continue
                got = shift(leg[1], axis, way * stride).astype(F32)
                if hop > 1:
                    mine = pieces[s](at[way * (hop - 1) % count]).astype(F32)
                    legs[(way, s)] = [hop - 1, (got + mine).astype(BF16)]
                else:
                    legs[(way, s)] = [0, got]
    return [pieces[s](at[0]).astype(F32) + legs[(1, s)][1] + legs[(-1, s)][1] for s in range(2)]


def step(tokens, expert_ids, gate_weight, w_gate, w_up, w_down, query, cache_k, cache_v, lengths):
    rows, feat = tokens.shape
    local, _, ff = w_gate.shape
    attn_count = lax.axis_size("attn")
    n_expert = lax.axis_size("expert")
    chips = attn_count // 2
    top = expert_ids.shape[1]
    capacity = rows * top // local
    me = lax.axis_index("attn")
    col = lax.axis_index("expert")
    y = me // 2
    core = me % 2
    far = chips // 2
    dest_rows = capacity // n_expert

    y_at = [lax.rem(y + k, chips) for k in range(chips)]
    x_at = [lax.rem(col + k, n_expert).astype(jnp.uint32) for k in range(n_expert)]
    offsets = [0, -1, 1, -3, 3, -2, 2, far]
    pack_info = [local * me]
    for flip in (0, 1):
        pack_info += [2 * y_at[off % chips] + (core ^ flip) for off in offsets]
    row_at = [core] + [x.astype(jnp.int32) * dest_rows for x in x_at]
    pack_info = jnp.stack(pack_info).astype(jnp.int32)
    row_at = jnp.stack(row_at).astype(jnp.int32)
    core_at = core.reshape(1).astype(jnp.int32)
    y_info = jnp.stack(y_at).astype(jnp.int32)
    tokens, pack_info, row_at, core_at, y_info, x_at = lax.optimization_barrier(
        (tokens, pack_info, row_at, core_at, y_info, x_at)
    )

    meta = jnp.concatenate([expert_ids.astype(BF16).T, gate_weight.T], axis=0)
    block = jnp.concatenate([tokens, jnp.pad(meta, ((0, 0), (0, feat - rows)))], axis=0)
    half = (rows + META) // 2
    attn_out = grouped_attention(query, cache_k, cache_v, lengths)
    near = [shift(block, "attn", 2), shift(block, "attn", -2)]
    away3 = [shift(block, "attn", 6), shift(block, "attn", -6)]
    *near, attn_out = lax.optimization_barrier((*near, attn_out))
    right = shift(jnp.concatenate([near[0], away3[0][:half]], axis=0), "attn", 2)
    left = shift(jnp.concatenate([near[1], away3[1][half:]], axis=0), "attn", -2)
    swap_first = swap_cores(jnp.concatenate([block, *near, *away3], axis=0))
    swap_last = swap_cores(jnp.concatenate([right, left], axis=0))
    operands = [block, *near, *away3, right, left, swap_first, swap_last]
    height = rows + META
    plan = [((i, 0),) for i in range(7)] + [((5, height), (6, height))]
    plan += [((7, i * height),) for i in range(5)]
    plan += [((8, 0),), ((8, height + half),), ((8, height), (8, 2 * height + half))]

    cut = local // 2
    pack_scratch = [
        pltpu.VMEM((capacity, attn_count * rows), BF16),
        pltpu.VMEM((cut, *w_gate.shape[1:]), BF16),
        pltpu.VMEM((cut, *w_up.shape[1:]), BF16),
        pltpu.SemaphoreType.DMA((2, cut)),
    ]
    part_shape = jax.ShapeDtypeStruct((n_expert, cut, dest_rows, 2 * ff), BF16)
    pack_cost = pl.CostEstimate(flops=2 * 10**9, bytes_accessed=6 * 10**6, transcendentals=0)
    parts_a, route, tok = pl.pallas_call(
        functools.partial(pack_kernel, plan, half, local),
        out_shape=(
            part_shape,
            jax.ShapeDtypeStruct((attn_count, 8, rows), F32),
            jax.ShapeDtypeStruct((attn_count * rows, feat), BF16),
        ),
        in_specs=[SMEM_SPEC] + [VMEM_SPEC] * len(operands) + [HBM_SPEC] * 2,
        out_specs=(VMEM_SPEC, VMEM_SPEC, VMEM_SPEC),
        scratch_shapes=[
            pltpu.VMEM((attn_count, META, rows), F32),
            pltpu.VMEM((attn_count, 8, rows), F32),
            *pack_scratch,
        ],
        compiler_params=pltpu.CompilerParams(vmem_limit_bytes=7 << 20),
        cost_estimate=pack_cost,
        name="pack",
    )(pack_info, *map(in_vmem, operands), in_hbm(w_gate), in_hbm(w_up))
    parts_b = pl.pallas_call(
        functools.partial(pack_more_kernel, cut),
        out_shape=part_shape,
        in_specs=[SMEM_SPEC, VMEM_SPEC, VMEM_SPEC, HBM_SPEC, HBM_SPEC],
        out_specs=VMEM_SPEC,
        scratch_shapes=pack_scratch,
        compiler_params=pltpu.CompilerParams(vmem_limit_bytes=7 << 20),
        cost_estimate=pack_cost,
        name="pack_more",
    )(pack_info, in_vmem(tok), in_vmem(route), in_hbm(w_gate), in_hbm(w_up))

    sums = scatter_sum(
        [lambda at, p=p: lax.dynamic_index_in_dim(p, at, 0, keepdims=False) for p in (parts_a, parts_b)],
        "expert",
        1,
        x_at,
    )
    hidden = jnp.concatenate(
        [(jax.nn.silu(t[..., :ff]) * t[..., ff:]).astype(BF16) for t in sums], axis=0
    )

    n_half = n_expert // 2
    pieces_in, where = [hidden], [(0, 1)]
    rightward = leftward = hidden
    for hop in range(1, n_half + 1):
        if hop == n_half:
            rightward, leftward = rightward[:cut], leftward[cut:]
        rightward, leftward = shift(rightward, "expert", 1), shift(leftward, "expert", -1)
        pieces_in += [rightward, leftward]
        where += [(0, 1 + n_expert - hop), (cut if hop == n_half else 0, 1 + hop)]

    away, res = pl.pallas_call(
        functools.partial(down_kernel, where),
        out_shape=(
            jax.ShapeDtypeStruct((chips, rows, feat), BF16),
            jax.ShapeDtypeStruct((local * capacity, feat), BF16),
        ),
        in_specs=[SMEM_SPEC] + [VMEM_SPEC] * len(pieces_in) + [HBM_SPEC, VMEM_SPEC],
        out_specs=(VMEM_SPEC, VMEM_SPEC),
        scratch_shapes=[
            pltpu.VMEM((local, capacity, ff), BF16),
            pltpu.VMEM((2 * rows, local * capacity), BF16),
            pltpu.VMEM(w_down.shape, BF16),
            pltpu.SemaphoreType.DMA((local,)),
        ],
        compiler_params=pltpu.CompilerParams(vmem_limit_bytes=(15 << 20) // 2),
        cost_estimate=pl.CostEstimate(flops=2 * 10**9, bytes_accessed=6 * 10**6, transcendentals=0),
        name="down",
    )(row_at, *map(in_vmem, pieces_in), in_hbm(w_down), in_vmem(route))
    swapped = swap_cores(away)
    home = pl.pallas_call(
        home_kernel,
        out_shape=jax.ShapeDtypeStruct((chips, rows, feat), BF16),
        in_specs=[SMEM_SPEC, VMEM_SPEC, VMEM_SPEC],
        out_specs=VMEM_SPEC,
        scratch_shapes=[pltpu.VMEM((2 * rows, local * capacity), BF16)],
        compiler_params=pltpu.CompilerParams(vmem_limit_bytes=(5 << 20) // 2),
        cost_estimate=pl.CostEstimate(flops=10**9, bytes_accessed=2 * 10**6, transcendentals=0),
        name="home",
    )(core_at, in_vmem(res), in_vmem(route))

    block_shape = jax.ShapeDtypeStruct((rows, feat), BF16)
    long_shape = jax.ShapeDtypeStruct((rows + rows // 2, feat), BF16)
    small = {"compiler_params": pltpu.CompilerParams(vmem_limit_bytes=2 << 20)}
    total, right, left = pl.pallas_call(
        sum_kernel,
        out_shape=(jax.ShapeDtypeStruct(home.shape, BF16), long_shape, long_shape),
        in_specs=[SMEM_SPEC, VMEM_SPEC, VMEM_SPEC],
        out_specs=(VMEM_SPEC,) * 3,
        name="sum",
        **small,
    )(y_info, in_vmem(home), in_vmem(swapped))
    right, left = shift(right, "attn", 2), shift(left, "attn", -2)
    far_right, far_left, near_right, near_left = pl.pallas_call(
        relay_kernel,
        out_shape=(block_shape,) * 4,
        in_specs=[SMEM_SPEC] + [VMEM_SPEC] * 3,
        out_specs=(VMEM_SPEC,) * 4,
        name="relay",
        **small,
    )(y_info, in_vmem(total), in_vmem(right), in_vmem(left))
    last = [
        shift(far_right, "attn", 6),
        shift(far_left, "attn", -6),
        shift(near_right, "attn", 2),
        shift(near_left, "attn", -2),
    ]
    moe_out = pl.pallas_call(
        finish_kernel,
        out_shape=block_shape,
        in_specs=[SMEM_SPEC] + [VMEM_SPEC] * 5,
        out_specs=VMEM_SPEC,
        name="finish",
        **small,
    )(y_info, in_vmem(total), *map(in_vmem, last))
    return (moe_out, attn_out)


def solution(mesh):
    return jax.shard_map(
        step,
        mesh=mesh,
        in_specs=(
            P(("groups", "attn"), "expert"),
            P(("groups", "attn"), None),
            P(("groups", "attn"), None),
            P("attn", "expert", None),
            P("attn", "expert", None),
            P("attn", None, "expert"),
            P(("groups", "attn", "expert"), None, None),
            P(("groups", "attn", "expert"), None, None, None),
            P(("groups", "attn", "expert"), None, None, None),
            P(("groups", "attn", "expert")),
        ),
        out_specs=(P(("groups", "attn"), "expert"), P(("groups", "attn", "expert"), None)),
        check_vma=False,
    )
```

```python
import functools

import jax
import jax.numpy as jnp
from jax import lax
from jax.experimental import pallas as pl
from jax.experimental.pallas import tpu as pltpu
from jax.sharding import PartitionSpec as P


F32 = jnp.float32
BF16 = jnp.bfloat16
META = 8
VMEM_SPEC = pl.BlockSpec(memory_space=pltpu.VMEM)
SMEM_SPEC = pl.BlockSpec(memory_space=pltpu.SMEM)
HBM_SPEC = pl.BlockSpec(memory_space=pltpu.HBM)
SMALL = {"compiler_params": pltpu.CompilerParams(vmem_limit_bytes=2 << 20)}


def both_cores(home, swapped, at):
    return home[at].astype(F32) + swapped[at].astype(F32)


def first_kernel(info, home, swapped, right, left):
    count, rows, _ = home.shape
    mid = rows // 2
    right[0:rows, :] = both_cores(home, swapped, info[2]).astype(BF16)
    left[0:rows, :] = both_cores(home, swapped, info[count - 2]).astype(BF16)
    across = both_cores(home, swapped, info[count // 2]).astype(BF16)
    right[rows:, :] = across[0:mid]
    left[rows:, :] = across[mid:]


def rest_kernel(info, home, swapped, total):
    count = home.shape[0]
    for i, k in enumerate((0, 1, count - 1, 3, count - 3)):
        total[i] = both_cores(home, swapped, info[k]).astype(BF16)


def relay_kernel(total, right, left, far_right, far_left, near_right, near_left):
    _, rows, _ = total.shape
    mid = rows // 2
    far_right[0:mid, :] = (total[3, 0:mid].astype(F32) + right[rows:, :].astype(F32)).astype(BF16)
    far_right[mid:, :] = total[3, mid:]
    far_left[0:mid, :] = total[4, 0:mid]
    far_left[mid:, :] = (total[4, mid:].astype(F32) + left[rows:, :].astype(F32)).astype(BF16)
    near_right[...] = (total[1].astype(F32) + right[0:rows, :].astype(F32)).astype(BF16)
    near_left[...] = (total[2].astype(F32) + left[0:rows, :].astype(F32)).astype(BF16)


def finish_kernel(total, a, b, c, d, out):
    out[...] = (
        total[0].astype(F32)
        + (a[...].astype(F32) + b[...].astype(F32))
        + (c[...].astype(F32) + d[...].astype(F32))
    ).astype(BF16)


def in_hbm(value):
    return pltpu.with_memory_space_constraint(value, pltpu.HBM)


def in_vmem(value):
    return pltpu.with_memory_space_constraint(value, pltpu.VMEM)


def attention_kernel(lengths, query, cache_k, cache_v, out):
    heads, size = query.shape[1:]
    spots, groups, _ = cache_k.shape[1:]
    columns = spots * groups
    keys = cache_k[0].reshape(columns, size)
    values = cache_v[0].reshape(columns, size)
    scores = lax.dot_general(
        query[0], keys, (((1,), (1,)), ((), ())), preferred_element_type=F32
    ) * size ** (-0.5)
    place = lax.broadcasted_iota(jnp.int32, (heads, columns), 1)
    head = lax.broadcasted_iota(jnp.int32, (heads, columns), 0)
    live = (place % groups == head // (heads // groups)) & (
        place < lengths[pl.program_id(0)] * groups
    )
    masked = jnp.where(live, scores, -jnp.inf)
    weighted = jnp.exp(masked - jnp.max(masked, axis=1, keepdims=True))
    prob = (weighted / jnp.sum(weighted, axis=1, keepdims=True)).astype(BF16)
    out[0] = jnp.dot(prob, values, preferred_element_type=F32).astype(BF16)


def grouped_attention(query, cache_k, cache_v, lengths):
    count, heads, size = query.shape
    _, spots, groups, _ = cache_k.shape
    cache = pl.BlockSpec((1, spots, groups, size), lambda i: (i, 0, 0, 0))
    row = pl.BlockSpec((1, heads, size), lambda i: (i, 0, 0))
    out = pl.pallas_call(
        attention_kernel,
        grid=(count,),
        out_shape=jax.ShapeDtypeStruct((count, heads, size), BF16),
        in_specs=[SMEM_SPEC, row, cache, cache],
        out_specs=row,
        compiler_params=pltpu.CompilerParams(vmem_limit_bytes=12 << 20),
        cost_estimate=pl.CostEstimate(
            flops=10**9, bytes_accessed=3 * 10**6, transcendentals=4 * 10**5
        ),
        name="attention",
    )(lengths, query, in_hbm(cache_k), in_hbm(cache_v))
    return out.reshape(count, heads * size)


def shift(value, axis, step):
    count = lax.axis_size(axis)
    return lax.ppermute(value, axis, [(i, (i + step) % count) for i in range(count)])


def swap_cores(value):
    return lax.ppermute(value, "attn", [(i, i ^ 1) for i in range(lax.axis_size("attn"))])


def prepare_kernel(tokens, ids, gates, block, ids_v, gates_v, sems):
    rows = tokens.shape[0]
    copies = (
        pltpu.make_async_copy(tokens, block.at[0:rows], sems.at[0]),
        pltpu.make_async_copy(ids, ids_v, sems.at[1]),
        pltpu.make_async_copy(gates, gates_v, sems.at[2]),
    )
    for copy in copies:
        copy.start()
    block[rows:, 2 * rows :] = jnp.zeros((META, block.shape[1] - 2 * rows), BF16)
    for copy in copies[1:]:
        copy.wait()
    block[rows:, 0:rows] = ids_v[...].astype(F32).astype(BF16)
    block[rows:, rows : 2 * rows] = gates_v[...]
    copies[0].wait()


def bundle_kernel(*refs):
    out = refs[-1]
    height = refs[0].shape[0]
    for i, ref in enumerate(refs[:-1]):
        out[i * height : (i + 1) * height, :] = ref[...]


def expert_parts(j0, info, place, tok, wg_hbm, wu_hbm, wg, wu, sems, onehot, out, work):
    n_blocks = place.shape[0]
    rows = tok.shape[0] // n_blocks
    n_dest = len(out)
    here_count, dest_rows, ff2 = out[0].shape
    ff = ff2 // 2
    capacity = n_dest * dest_rows

    def fetch(j):
        return (
            pltpu.make_async_copy(wg_hbm.at[j0 + j], wg.at[j], sems.at[0, j]),
            pltpu.make_async_copy(wu_hbm.at[j0 + j], wu.at[j], sems.at[1, j]),
        )

    for j in range(here_count):
        for copy in fetch(j):
            copy.start()
    work()
    row_id = lax.broadcasted_iota(jnp.int32, (capacity, rows), 0) + info[1 + n_blocks]
    row_id = jnp.where(row_id < capacity, row_id, row_id - capacity).astype(F32)

    def expert(j, carry):
        for i in range(n_blocks):
            spot = place[info[1 + i], pl.ds(j0 + j, 1), :]
            onehot[:, i * rows : (i + 1) * rows] = jnp.where(row_id == spot, 1.0, 0.0).astype(BF16)
        packed = jnp.dot(onehot[...], tok[...], preferred_element_type=F32).astype(BF16)
        for copy in fetch(j):
            copy.wait()
        gate = jnp.dot(packed, wg[j], preferred_element_type=F32).astype(BF16)
        up = jnp.dot(packed, wu[j], preferred_element_type=F32).astype(BF16)
        for d in range(n_dest):
            out[d][j, :, 0:ff] = gate[d * dest_rows : (d + 1) * dest_rows]
            out[d][j, :, ff:] = up[d * dest_rows : (d + 1) * dest_rows]
        return carry

    lax.fori_loop(0, here_count, expert, 0)


def pack_kernel(plan, half, local, n_dest, info, *refs):
    n_ops = 1 + max(op for p in plan for op, _ in p)
    ops = refs[:n_ops]
    wg_hbm, wu_hbm = refs[n_ops : n_ops + 2]
    out = refs[n_ops + 2 : n_ops + 2 + n_dest]
    route, tok, meta, onehot, wg, wu, sems = refs[n_ops + 2 + n_dest :]
    n_blocks = len(plan)
    rows = tok.shape[0] // n_blocks
    capacity = n_dest * out[0].shape[1]

    def work():
        for i, p in enumerate(plan):
            at = pl.ds(pl.multiple_of(info[1 + i] * rows, rows), rows)
            op, r0 = p[0]
            if len(p) == 1:
                tok[i * rows : (i + 1) * rows, :] = ops[op][r0 : r0 + rows, :]
                low = r0 + rows
            else:
                tok[i * rows : i * rows + half, :] = ops[op][r0 : r0 + half, :]
                op, r0 = p[1]
                low = r0 + rows - half
                tok[i * rows + half : (i + 1) * rows, :] = ops[op][r0:low, :]
            meta[0:8, at] = ops[op][low : low + META, 0:rows].astype(F32)
            meta[8:16, at] = ops[op][low : low + META, rows : 2 * rows].astype(F32)
        ids = meta[0:8, :]
        gates = meta[8:16, :]
        hits = [ids == (info[0] + j).astype(F32) for j in range(local)]
        stack = jnp.concatenate(
            [jnp.where(h, 1.0, 0.0) for h in hits] + [jnp.where(h, gates, 0.0) for h in hits], axis=0
        ).astype(BF16)
        one = lax.broadcasted_iota(jnp.int32, (8, 64), 0)
        two = lax.broadcasted_iota(jnp.int32, (8, 64), 1)
        pick = jnp.where(one == two // 8, 1.0, 0.0).astype(BF16)
        both = jnp.dot(pick, stack, preferred_element_type=F32)
        member = jnp.concatenate(
            [both[:, b * rows : (b + 1) * rows] for b in range(n_blocks)], axis=0
        )
        size = n_blocks * 8
        r = lax.broadcasted_iota(jnp.int32, (rows, rows), 0)
        c = lax.broadcasted_iota(jnp.int32, (rows, rows), 1)
        upper = jnp.where(r < c, 1.0, 0.0).astype(BF16)
        rr = lax.broadcasted_iota(jnp.int32, (size, size), 0)
        cc = lax.broadcasted_iota(jnp.int32, (size, size), 1)
        earlier = jnp.where((rr % 8 == cc % 8) & (cc // 8 < rr // 8), 1.0, 0.0).astype(BF16)
        member_b = member.astype(BF16)
        before = jnp.dot(earlier, member_b, preferred_element_type=F32).astype(BF16)
        place = jnp.dot(member_b, upper, preferred_element_type=F32) + jnp.dot(
            before, jnp.ones((rows, rows), BF16), preferred_element_type=F32
        )
        place = jnp.where((member > 0.5) & (place < capacity), place, -1.0)
        row = lax.broadcasted_iota(jnp.int32, (size, rows), 0)
        route[...] = jnp.where(row % 8 < local, place, member).reshape(n_blocks, 8, rows)

    expert_parts(0, info, route, tok, wg_hbm, wu_hbm, wg, wu, sems, onehot, out, work)


def pack_more_kernel(j0, info, tok, route, wg_hbm, wu_hbm, *refs):
    *out, onehot, wg, wu, sems = refs
    expert_parts(
        j0, info, route, tok, wg_hbm, wu_hbm, wg, wu, sems, onehot, out, lambda: None
    )


def hidden_kernel(*refs):
    *terms, out = refs
    ways = 3
    row = 0
    for s in range(len(terms) // ways):
        a, b, c = (t[...].astype(F32) for t in terms[s * ways : (s + 1) * ways])
        total = a + (b + c)
        ff = total.shape[-1] // 2
        v = total[..., :ff]
        out[row : row + total.shape[0]] = (v / (1.0 + jnp.exp(-v)) * total[..., ff:]).astype(BF16)
        row += total.shape[0]


def mix_kernel(info, route, wd_hbm, away, home, wd, sem):
    copy = pltpu.make_async_copy(wd_hbm, wd, sem)
    copy.start()
    n_blocks, _, rows = route.shape
    local = wd.shape[0]
    capacity = away.shape[1] // local
    r = lax.broadcasted_iota(jnp.int32, (rows, rows), 0)
    c = lax.broadcasted_iota(jnp.int32, (rows, rows), 1)
    eye = jnp.where(r == c, 1.0, 0.0).astype(BF16)
    col_id = lax.broadcasted_iota(jnp.int32, (rows, capacity), 1).astype(F32)

    def block(d, carry):
        at = pl.ds(pl.multiple_of(d * rows, rows), rows)
        for side, ref in ((1 - info[0], away), (info[0], home)):
            rt = lax.dot_general(
                eye,
                route[2 * d + side].astype(BF16),
                (((1,), (1,)), ((), ())),
                preferred_element_type=F32,
            )
            for j in range(local):
                ref[at, j * capacity : (j + 1) * capacity] = jnp.where(
                    col_id == rt[:, j : j + 1], rt[:, local + j : local + j + 1], 0.0
                ).astype(BF16)
        return carry

    lax.fori_loop(0, n_blocks // 2, block, 0)
    copy.wait()


def mix_rows(mix, res, ref):
    n_dest, rows, feat = ref.shape
    group = 2

    def some(g, carry):
        at = pl.ds(pl.multiple_of(g * group * rows, group * rows), group * rows)
        got = jnp.dot(mix[at, :], res[...], preferred_element_type=F32).astype(BF16)
        ref[pl.ds(g * group, group)] = got.reshape(group, rows, feat)
        return carry

    lax.fori_loop(0, n_dest // group, some, 0)


def down_kernel(plan, info, *refs):
    n_ops = len(plan)
    ops = refs[:n_ops]
    wd, mix, away, res, hid = refs[n_ops:]
    local = wd.shape[0]
    capacity = hid.shape[1]
    for op, (j0, slot) in zip(ops, plan):
        at = pl.multiple_of(info[slot], op.shape[1])
        for j in range(op.shape[0]):
            hid[j0 + j, pl.ds(at, op.shape[1]), :] = op[j]

    def expert(j, carry):
        res[pl.ds(pl.multiple_of(j * capacity, capacity), capacity), :] = jnp.dot(
            hid[j], wd[j], preferred_element_type=F32
        ).astype(BF16)
        return carry

    lax.fori_loop(0, local, expert, 0)
    mix_rows(mix, res, away)


def home_kernel(mix, res, home):
    mix_rows(mix, res, home)


def scatter_sum(pieces, axis):
    count = len(pieces[0])
    half = count // 2
    legs = {}
    for way in (1, -1):
        for s in range(2):
            start = half if (way == 1) == (s == 0) else half - 1
            legs[(way, s)] = [start, pieces[s][way * start % count]]
    for hop in range(half, 0, -1):
        for way in (1, -1):
            for s in range(2):
                leg = legs[(way, s)]
                if leg[0] != hop:
                    continue
                got = shift(leg[1], axis, way)
                if hop > 1:
                    mine = pieces[s][way * (hop - 1) % count]
                    got = (got.astype(F32) + mine.astype(F32)).astype(BF16)
                legs[(way, s)] = [hop - 1, got]
    return [(pieces[s][0], legs[(1, s)][1], legs[(-1, s)][1]) for s in range(2)]


def step(tokens, expert_ids, gate_weight, w_gate, w_up, w_down, query, cache_k, cache_v, lengths):
    rows, feat = tokens.shape
    local, _, ff = w_gate.shape
    attn_count = lax.axis_size("attn")
    n_expert = lax.axis_size("expert")
    chips = attn_count // 2
    top = expert_ids.shape[1]
    capacity = rows * top // local
    me = lax.axis_index("attn")
    col = lax.axis_index("expert")
    y = me // 2
    core = me % 2
    far = chips // 2
    dest_rows = capacity // n_expert

    y_at = [lax.rem(y + k, chips) for k in range(chips)]
    x_at = [lax.rem(col + k, n_expert) for k in range(n_expert)]
    offsets = [0, -1, 1, -3, 3, -2, 2, far]
    pack_info = [local * me]
    for flip in (0, 1):
        pack_info += [2 * y_at[off % chips] + (core ^ flip) for off in offsets]
    row_at = [core] + [x * dest_rows for x in x_at]
    pack_info.append(col * dest_rows)
    pack_info = jnp.stack(pack_info).astype(jnp.int32)
    row_at = jnp.stack(row_at).astype(jnp.int32)
    core_at = core.reshape(1).astype(jnp.int32)
    y_info = jnp.stack(y_at).astype(jnp.int32)
    tokens, pack_info, row_at, core_at, y_info = lax.optimization_barrier(
        (tokens, pack_info, row_at, core_at, y_info)
    )

    height = rows + META
    half = rows // 2
    block = pl.pallas_call(
        prepare_kernel,
        out_shape=jax.ShapeDtypeStruct((height, feat), BF16),
        in_specs=[HBM_SPEC] * 3,
        out_specs=VMEM_SPEC,
        scratch_shapes=[
            pltpu.VMEM((top, rows), jnp.int32),
            pltpu.VMEM((top, rows), BF16),
            pltpu.SemaphoreType.DMA((3,)),
        ],
        name="prepare",
        **SMALL,
    )(in_hbm(tokens), in_hbm(expert_ids.T), in_hbm(gate_weight.T))
    attn_out = grouped_attention(query, cache_k, cache_v, lengths)

    away3 = [shift(block, "attn", 6), shift(block, "attn", -6)]
    near = [shift(block, "attn", 2), shift(block, "attn", -2)]
    *near, attn_out = lax.optimization_barrier((*near, attn_out))
    right = shift(jnp.concatenate([near[0], away3[0][:half]], axis=0), "attn", 2)
    left = shift(jnp.concatenate([near[1], away3[1][half:]], axis=0), "attn", -2)
    bundle = pl.pallas_call(
        bundle_kernel,
        out_shape=jax.ShapeDtypeStruct((5 * height, feat), BF16),
        in_specs=[VMEM_SPEC] * 5,
        out_specs=VMEM_SPEC,
        name="bundle",
        **SMALL,
    )(*map(in_vmem, (block, *near, *away3)))
    swap_first = swap_cores(bundle)
    swap_last = swap_cores(jnp.concatenate([right, left], axis=0))
    operands = [block, *near, *away3, right, left, swap_first, swap_last]
    plan = [((i, 0),) for i in range(7)] + [((5, height), (6, height))]
    plan += [((7, i * height),) for i in range(5)]
    second = height + half
    plan += [((8, 0),), ((8, second),), ((8, height), (8, second + height))]

    cut = local // 2
    pack_scratch = [
        pltpu.VMEM((capacity, attn_count * rows), BF16),
        pltpu.VMEM((cut, *w_gate.shape[1:]), BF16),
        pltpu.VMEM((cut, *w_up.shape[1:]), BF16),
        pltpu.SemaphoreType.DMA((2, cut)),
    ]
    part_shapes = (jax.ShapeDtypeStruct((cut, dest_rows, 2 * ff), BF16),) * n_expert
    pack_cost = pl.CostEstimate(flops=2 * 10**9, bytes_accessed=6 * 10**6, transcendentals=0)
    *parts_a, route, tok = pl.pallas_call(
        functools.partial(pack_kernel, plan, half, local, n_expert),
        out_shape=(
            *part_shapes,
            jax.ShapeDtypeStruct((attn_count, 8, rows), F32),
            jax.ShapeDtypeStruct((attn_count * rows, feat), BF16),
        ),
        in_specs=[SMEM_SPEC] + [VMEM_SPEC] * len(operands) + [HBM_SPEC] * 2,
        out_specs=(VMEM_SPEC,) * (n_expert + 2),
        scratch_shapes=[
            pltpu.VMEM((2 * META, attn_count * rows), F32),
            *pack_scratch,
        ],
        compiler_params=pltpu.CompilerParams(vmem_limit_bytes=7 << 20),
        cost_estimate=pack_cost,
        name="pack",
    )(pack_info, *map(in_vmem, operands), in_hbm(w_gate), in_hbm(w_up))
    parts_b = pl.pallas_call(
        functools.partial(pack_more_kernel, cut),
        out_shape=part_shapes,
        in_specs=[SMEM_SPEC, VMEM_SPEC, VMEM_SPEC, HBM_SPEC, HBM_SPEC],
        out_specs=(VMEM_SPEC,) * n_expert,
        scratch_shapes=pack_scratch,
        compiler_params=pltpu.CompilerParams(vmem_limit_bytes=7 << 20),
        cost_estimate=pack_cost,
        name="pack_more",
    )(pack_info, in_vmem(tok), in_vmem(route), in_hbm(w_gate), in_hbm(w_up))

    terms = sum(scatter_sum([parts_a, parts_b], "expert"), ())
    hidden = pl.pallas_call(
        hidden_kernel,
        out_shape=jax.ShapeDtypeStruct((local, dest_rows, ff), BF16),
        in_specs=[VMEM_SPEC] * len(terms),
        out_specs=VMEM_SPEC,
        name="hidden",
        **SMALL,
    )(*map(in_vmem, terms))

    r2, l2 = shift(hidden, "expert", 2), shift(hidden, "expert", -2)
    r1, l1 = shift(hidden, "expert", 1), shift(hidden, "expert", -1)
    r4, l4 = shift(r2[:cut], "expert", 2), shift(l2[cut:], "expert", -2)
    r3, l3 = shift(r2, "expert", 1), shift(l2, "expert", -1)
    pieces_in = [hidden, r1, l1, r2, l2, r3, l3, r4, l4]
    where = [(0, 1 + k % n_expert) for k in (0, -1, 1, -2, 2, -3, 3, -4)] + [(cut, 1 + 4)]

    mix_shape = jax.ShapeDtypeStruct((chips * rows, local * capacity), BF16)
    mix_away, mix_home, wd = pl.pallas_call(
        mix_kernel,
        out_shape=(mix_shape, mix_shape, jax.ShapeDtypeStruct(w_down.shape, BF16)),
        in_specs=[SMEM_SPEC, VMEM_SPEC, HBM_SPEC],
        out_specs=(VMEM_SPEC,) * 3,
        scratch_shapes=[pltpu.SemaphoreType.DMA],
        name="mix",
        **SMALL,
    )(core_at, in_vmem(route), in_hbm(w_down))
    away, res = pl.pallas_call(
        functools.partial(down_kernel, where),
        out_shape=(
            jax.ShapeDtypeStruct((chips, rows, feat), BF16),
            jax.ShapeDtypeStruct((local * capacity, feat), BF16),
        ),
        in_specs=[SMEM_SPEC] + [VMEM_SPEC] * (len(pieces_in) + 2),
        out_specs=(VMEM_SPEC, VMEM_SPEC),
        scratch_shapes=[pltpu.VMEM((local, capacity, ff), BF16)],
        compiler_params=pltpu.CompilerParams(vmem_limit_bytes=4 << 20),
        cost_estimate=pl.CostEstimate(flops=2 * 10**9, bytes_accessed=6 * 10**6, transcendentals=0),
        name="down",
    )(row_at, *map(in_vmem, pieces_in), in_vmem(wd), in_vmem(mix_away))
    swapped = swap_cores(away)
    home = pl.pallas_call(
        home_kernel,
        out_shape=jax.ShapeDtypeStruct((chips, rows, feat), BF16),
        in_specs=[VMEM_SPEC, VMEM_SPEC],
        out_specs=VMEM_SPEC,
        cost_estimate=pl.CostEstimate(flops=10**9, bytes_accessed=2 * 10**6, transcendentals=0),
        name="home",
        **SMALL,
    )(in_vmem(mix_home), in_vmem(res))

    block_shape = jax.ShapeDtypeStruct((rows, feat), BF16)
    long_shape = jax.ShapeDtypeStruct((rows + rows // 2, feat), BF16)
    right, left = pl.pallas_call(
        first_kernel,
        out_shape=(long_shape, long_shape),
        in_specs=[SMEM_SPEC, VMEM_SPEC, VMEM_SPEC],
        out_specs=(VMEM_SPEC,) * 2,
        name="first",
        **SMALL,
    )(y_info, in_vmem(home), in_vmem(swapped))
    right, left = shift(right, "attn", 2), shift(left, "attn", -2)
    total = pl.pallas_call(
        rest_kernel,
        out_shape=jax.ShapeDtypeStruct((5, rows, feat), BF16),
        in_specs=[SMEM_SPEC, VMEM_SPEC, VMEM_SPEC],
        out_specs=VMEM_SPEC,
        name="rest",
        **SMALL,
    )(y_info, in_vmem(home), in_vmem(swapped))
    far_right, far_left, near_right, near_left = pl.pallas_call(
        relay_kernel,
        out_shape=(block_shape,) * 4,
        in_specs=[VMEM_SPEC] * 3,
        out_specs=(VMEM_SPEC,) * 4,
        name="relay",
        **SMALL,
    )(in_vmem(total), in_vmem(right), in_vmem(left))
    last = [
        shift(far_right, "attn", 6),
        shift(far_left, "attn", -6),
        shift(near_right, "attn", 2),
        shift(near_left, "attn", -2),
    ]
    moe_out = pl.pallas_call(
        finish_kernel,
        out_shape=block_shape,
        in_specs=[VMEM_SPEC] * 5,
        out_specs=VMEM_SPEC,
        name="finish",
        **SMALL,
    )(in_vmem(total), *map(in_vmem, last))
    return (moe_out, attn_out)


def solution(mesh):
    return jax.shard_map(
        step,
        mesh=mesh,
        in_specs=(
            P(("groups", "attn"), "expert"),
            P(("groups", "attn"), None),
            P(("groups", "attn"), None),
            P("attn", "expert", None),
            P("attn", "expert", None),
            P("attn", None, "expert"),
            P(("groups", "attn", "expert"), None, None),
            P(("groups", "attn", "expert"), None, None, None),
            P(("groups", "attn", "expert"), None, None, None),
            P(("groups", "attn", "expert")),
        ),
        out_specs=(P(("groups", "attn"), "expert"), P(("groups", "attn", "expert"), None)),
        check_vma=False,
    )
```

```python
import functools

import jax
import jax.numpy as jnp
from jax import lax
from jax.experimental import pallas as pl
from jax.experimental.pallas import tpu as pltpu
from jax.sharding import PartitionSpec as P


F32 = jnp.float32
BF16 = jnp.bfloat16
META = 8
VMEM_SPEC = pl.BlockSpec(memory_space=pltpu.VMEM)
SMEM_SPEC = pl.BlockSpec(memory_space=pltpu.SMEM)
HBM_SPEC = pl.BlockSpec(memory_space=pltpu.HBM)
SMALL = {"compiler_params": pltpu.CompilerParams(vmem_limit_bytes=2 << 20)}


def both_cores(home, swapped, at):
    return home[at].astype(F32) + swapped[at].astype(F32)


def first_kernel(info, home, swapped, right, left):
    count, rows, _ = home.shape
    mid = rows // 2
    right[0:rows, :] = both_cores(home, swapped, info[2]).astype(BF16)
    left[0:rows, :] = both_cores(home, swapped, info[count - 2]).astype(BF16)
    across = both_cores(home, swapped, info[count // 2]).astype(BF16)
    right[rows:, :] = across[0:mid]
    left[rows:, :] = across[mid:]


def rest_kernel(info, home, swapped, total):
    count = home.shape[0]
    for i, k in enumerate((0, 1, count - 1, 3, count - 3)):
        total[i] = both_cores(home, swapped, info[k]).astype(BF16)


def relay_kernel(total, right, left, far_right, far_left, near_right, near_left):
    _, rows, _ = total.shape
    mid = rows // 2
    far_right[0:mid, :] = (total[3, 0:mid].astype(F32) + right[rows:, :].astype(F32)).astype(BF16)
    far_right[mid:, :] = total[3, mid:]
    far_left[0:mid, :] = total[4, 0:mid]
    far_left[mid:, :] = (total[4, mid:].astype(F32) + left[rows:, :].astype(F32)).astype(BF16)
    near_right[...] = (total[1].astype(F32) + right[0:rows, :].astype(F32)).astype(BF16)
    near_left[...] = (total[2].astype(F32) + left[0:rows, :].astype(F32)).astype(BF16)


def finish_kernel(total, a, b, c, d, out):
    out[...] = (
        total[0].astype(F32)
        + (a[...].astype(F32) + b[...].astype(F32))
        + (c[...].astype(F32) + d[...].astype(F32))
    ).astype(BF16)


def in_hbm(value):
    return pltpu.with_memory_space_constraint(value, pltpu.HBM)


def in_vmem(value):
    return pltpu.with_memory_space_constraint(value, pltpu.VMEM)


def attention_kernel(lengths, query, cache_k, cache_v, out):
    heads, size = query.shape[1:]
    spots, groups, _ = cache_k.shape[1:]
    columns = spots * groups
    keys = cache_k[0].reshape(columns, size)
    values = cache_v[0].reshape(columns, size)
    scores = lax.dot_general(
        query[0], keys, (((1,), (1,)), ((), ())), preferred_element_type=F32
    ) * size ** (-0.5)
    place = lax.broadcasted_iota(jnp.int32, (heads, columns), 1)
    head = lax.broadcasted_iota(jnp.int32, (heads, columns), 0)
    live = (place % groups == head // (heads // groups)) & (
        place < lengths[pl.program_id(0)] * groups
    )
    masked = jnp.where(live, scores, -jnp.inf)
    weighted = jnp.exp(masked - jnp.max(masked, axis=1, keepdims=True))
    prob = (weighted / jnp.sum(weighted, axis=1, keepdims=True)).astype(BF16)
    out[0] = jnp.dot(prob, values, preferred_element_type=F32).astype(BF16)


def grouped_attention(query, cache_k, cache_v, lengths):
    count, heads, size = query.shape
    _, spots, groups, _ = cache_k.shape
    cache = pl.BlockSpec((1, spots, groups, size), lambda i: (i, 0, 0, 0))
    row = pl.BlockSpec((1, heads, size), lambda i: (i, 0, 0))
    out = pl.pallas_call(
        attention_kernel,
        grid=(count,),
        out_shape=jax.ShapeDtypeStruct((count, heads, size), BF16),
        in_specs=[SMEM_SPEC, row, cache, cache],
        out_specs=row,
        compiler_params=pltpu.CompilerParams(vmem_limit_bytes=12 << 20),
        cost_estimate=pl.CostEstimate(
            flops=10**9, bytes_accessed=3 * 10**6, transcendentals=4 * 10**5
        ),
        name="attention",
    )(lengths, query, in_hbm(cache_k), in_hbm(cache_v))
    return out.reshape(count, heads * size)


def shift(value, axis, step):
    count = lax.axis_size(axis)
    return lax.ppermute(value, axis, [(i, (i + step) % count) for i in range(count)])


def swap_cores(value):
    return lax.ppermute(value, "attn", [(i, i ^ 1) for i in range(lax.axis_size("attn"))])


def prepare_kernel(tokens, ids, gates, block, ids_v, gates_v, sems):
    rows = tokens.shape[0]
    copies = (
        pltpu.make_async_copy(tokens, block.at[0:rows], sems.at[0]),
        pltpu.make_async_copy(ids, ids_v, sems.at[1]),
        pltpu.make_async_copy(gates, gates_v, sems.at[2]),
    )
    for copy in copies:
        copy.start()
    block[rows:, 2 * rows :] = jnp.zeros((META, block.shape[1] - 2 * rows), BF16)
    for copy in copies[1:]:
        copy.wait()
    block[rows:, 0:rows] = ids_v[...].astype(F32).astype(BF16)
    block[rows:, rows : 2 * rows] = gates_v[...]
    copies[0].wait()


def bundle_kernel(*refs):
    out = refs[-1]
    height = refs[0].shape[0]
    for i, ref in enumerate(refs[:-1]):
        out[i * height : (i + 1) * height, :] = ref[...]


def expert_parts(j0, info, place, tok, wg, wu, onehot, packed, out):
    n_blocks = place.shape[0]
    rows = tok.shape[0] // n_blocks
    n_dest = len(out)
    here_count, dest_rows, ff2 = out[0].shape
    ff = ff2 // 2
    capacity = n_dest * dest_rows
    row_id = lax.broadcasted_iota(jnp.int32, (capacity, rows), 0) + info[1 + n_blocks]
    row_id = jnp.where(row_id < capacity, row_id, row_id - capacity).astype(F32)

    def select(i, carry):
        at = pl.ds(pl.multiple_of(i * rows, rows), rows)
        block = info[1 + i]
        for j in range(here_count):
            spot = place[block, j0 + j : j0 + j + 1, :]
            onehot[j * capacity : (j + 1) * capacity, at] = jnp.where(
                row_id == spot, 1.0, 0.0
            ).astype(BF16)
        return carry

    lax.fori_loop(0, n_blocks, select, 0, unroll=2)
    packed[...] = jnp.dot(onehot[...], tok[...], preferred_element_type=F32).astype(BF16)

    def expert(j, carry):
        mine = packed[pl.ds(pl.multiple_of(j * capacity, capacity), capacity), :]
        gate = jnp.dot(mine, wg[j0 + j], preferred_element_type=F32).astype(BF16)
        up = jnp.dot(mine, wu[j0 + j], preferred_element_type=F32).astype(BF16)
        for d in range(n_dest):
            out[d][j, :, 0:ff] = gate[d * dest_rows : (d + 1) * dest_rows]
            out[d][j, :, ff:] = up[d * dest_rows : (d + 1) * dest_rows]
        return carry

    lax.fori_loop(0, here_count, expert, 0)


def fetch_kernel(wg_hbm, wu_hbm, wg, wu, sems):
    copies = (
        pltpu.make_async_copy(wg_hbm, wg, sems.at[0]),
        pltpu.make_async_copy(wu_hbm, wu, sems.at[1]),
    )
    for copy in copies:
        copy.start()
    for copy in copies:
        copy.wait()


def pack_kernel(plan, half, local, n_dest, info, *refs):
    n_ops = 1 + max(op for p in plan for op, _ in p)
    ops = refs[:n_ops]
    wg, wu = refs[n_ops : n_ops + 2]
    out = refs[n_ops + 2 : n_ops + 2 + n_dest]
    route, tok, meta, onehot, packed = refs[n_ops + 2 + n_dest :]
    n_blocks = len(plan)
    rows = tok.shape[0] // n_blocks
    capacity = n_dest * out[0].shape[1]

    for i, p in enumerate(plan):
        at = pl.ds(pl.multiple_of(info[1 + i] * rows, rows), rows)
        op, r0 = p[0]
        if len(p) == 1:
            tok[i * rows : (i + 1) * rows, :] = ops[op][r0 : r0 + rows, :]
            low = r0 + rows
        else:
            tok[i * rows : i * rows + half, :] = ops[op][r0 : r0 + half, :]
            op, r0 = p[1]
            low = r0 + rows - half
            tok[i * rows + half : (i + 1) * rows, :] = ops[op][r0:low, :]
        meta[0:8, at] = ops[op][low : low + META, 0:rows].astype(F32)
        meta[8:16, at] = ops[op][low : low + META, rows : 2 * rows].astype(F32)
    ids = meta[0:8, :]
    gates = meta[8:16, :]
    hits = [ids == (info[0] + j).astype(F32) for j in range(local)]
    stack = jnp.concatenate(
        [jnp.where(h, 1.0, 0.0) for h in hits] + [jnp.where(h, gates, 0.0) for h in hits], axis=0
    ).astype(BF16)
    one = lax.broadcasted_iota(jnp.int32, (8, 64), 0)
    two = lax.broadcasted_iota(jnp.int32, (8, 64), 1)
    pick = jnp.where(one == two // 8, 1.0, 0.0).astype(BF16)
    both = jnp.dot(pick, stack, preferred_element_type=F32)
    member = jnp.concatenate(
        [both[:, b * rows : (b + 1) * rows] for b in range(n_blocks)], axis=0
    )
    size = n_blocks * 8
    r = lax.broadcasted_iota(jnp.int32, (rows, rows), 0)
    c = lax.broadcasted_iota(jnp.int32, (rows, rows), 1)
    upper = jnp.where(r < c, 1.0, 0.0).astype(BF16)
    rr = lax.broadcasted_iota(jnp.int32, (size, size), 0)
    cc = lax.broadcasted_iota(jnp.int32, (size, size), 1)
    earlier = jnp.where((rr % 8 == cc % 8) & (cc // 8 < rr // 8), 1.0, 0.0).astype(BF16)
    member_b = member.astype(BF16)
    before = jnp.dot(earlier, member_b, preferred_element_type=F32).astype(BF16)
    place = jnp.dot(member_b, upper, preferred_element_type=F32) + jnp.dot(
        before, jnp.ones((rows, rows), BF16), preferred_element_type=F32
    )
    place = jnp.where((member > 0.5) & (place < capacity), place, -1.0)
    row = lax.broadcasted_iota(jnp.int32, (size, rows), 0)
    route[...] = jnp.where(row % 8 < local, place, member).reshape(n_blocks, 8, rows)

    expert_parts(0, info, route, tok, wg, wu, onehot, packed, out)


def pack_more_kernel(j0, info, tok, route, wg, wu, *refs):
    *out, onehot, packed = refs
    expert_parts(j0, info, route, tok, wg, wu, onehot, packed, out)


def hidden_kernel(*refs):
    *terms, out = refs
    ways = 3
    row = 0
    for s in range(len(terms) // ways):
        a, b, c = (t[...].astype(F32) for t in terms[s * ways : (s + 1) * ways])
        total = a + (b + c)
        ff = total.shape[-1] // 2
        v = total[..., :ff]
        out[row : row + total.shape[0]] = (v / (1.0 + jnp.exp(-v)) * total[..., ff:]).astype(BF16)
        row += total.shape[0]


def mix_kernel(info, route, wd_hbm, away, home, wd, sem):
    copy = pltpu.make_async_copy(wd_hbm, wd, sem)
    copy.start()
    n_blocks, _, rows = route.shape
    local = wd.shape[0]
    capacity = away.shape[1] // local
    r = lax.broadcasted_iota(jnp.int32, (rows, rows), 0)
    c = lax.broadcasted_iota(jnp.int32, (rows, rows), 1)
    eye = jnp.where(r == c, 1.0, 0.0).astype(BF16)
    col_id = lax.broadcasted_iota(jnp.int32, (rows, capacity), 1).astype(F32)

    def block(d, carry):
        at = pl.ds(pl.multiple_of(d * rows, rows), rows)
        for side, ref in ((1 - info[0], away), (info[0], home)):
            rt = lax.dot_general(
                eye,
                route[2 * d + side].astype(BF16),
                (((1,), (1,)), ((), ())),
                preferred_element_type=F32,
            )
            for j in range(local):
                ref[at, j * capacity : (j + 1) * capacity] = jnp.where(
                    col_id == rt[:, j : j + 1], rt[:, local + j : local + j + 1], 0.0
                ).astype(BF16)
        return carry

    lax.fori_loop(0, n_blocks // 2, block, 0)
    copy.wait()


def mix_rows(mix, res, ref):
    n_dest, rows, feat = ref.shape
    group = 4

    def some(g, carry):
        at = pl.ds(pl.multiple_of(g * group * rows, group * rows), group * rows)
        got = jnp.dot(mix[at, :], res[...], preferred_element_type=F32).astype(BF16)
        ref[pl.ds(g * group, group)] = got.reshape(group, rows, feat)
        return carry

    lax.fori_loop(0, n_dest // group, some, 0)


def down_kernel(plan, info, *refs):
    n_ops = len(plan)
    ops = refs[:n_ops]
    wd, mix, away, res, hid = refs[n_ops:]
    local = wd.shape[0]
    capacity = hid.shape[1]
    for op, (j0, slot) in zip(ops, plan):
        at = pl.multiple_of(info[slot], op.shape[1])
        for j in range(op.shape[0]):
            hid[j0 + j, pl.ds(at, op.shape[1]), :] = op[j]

    def expert(j, carry):
        res[pl.ds(pl.multiple_of(j * capacity, capacity), capacity), :] = jnp.dot(
            hid[j], wd[j], preferred_element_type=F32
        ).astype(BF16)
        return carry

    lax.fori_loop(0, local, expert, 0)
    mix_rows(mix, res, away)


def home_kernel(mix, res, home):
    mix_rows(mix, res, home)


def scatter_sum(pieces, axis):
    count = len(pieces[0])
    half = count // 2
    legs = {}
    for way in (1, -1):
        for s in range(2):
            start = half if (way == 1) == (s == 0) else half - 1
            legs[(way, s)] = [start, pieces[s][way * start % count]]
    for hop in range(half, 0, -1):
        for way in (1, -1):
            for s in range(2):
                leg = legs[(way, s)]
                if leg[0] != hop:
                    continue
                got = shift(leg[1], axis, way)
                if hop > 1:
                    mine = pieces[s][way * (hop - 1) % count]
                    got = (got.astype(F32) + mine.astype(F32)).astype(BF16)
                legs[(way, s)] = [hop - 1, got]
    return [(pieces[s][0], legs[(1, s)][1], legs[(-1, s)][1]) for s in range(2)]


def step(tokens, expert_ids, gate_weight, w_gate, w_up, w_down, query, cache_k, cache_v, lengths):
    rows, feat = tokens.shape
    local, _, ff = w_gate.shape
    attn_count = lax.axis_size("attn")
    n_expert = lax.axis_size("expert")
    chips = attn_count // 2
    top = expert_ids.shape[1]
    capacity = rows * top // local
    me = lax.axis_index("attn")
    col = lax.axis_index("expert")
    y = me // 2
    core = me % 2
    far = chips // 2
    dest_rows = capacity // n_expert

    y_at = [lax.rem(y + k, chips) for k in range(chips)]
    x_at = [lax.rem(col + k, n_expert) for k in range(n_expert)]
    offsets = [0, -1, 1, -3, 3, -2, 2, far]
    pack_info = [local * me]
    for flip in (0, 1):
        pack_info += [2 * y_at[off % chips] + (core ^ flip) for off in offsets]
    row_at = [core] + [x * dest_rows for x in x_at]
    pack_info.append(col * dest_rows)
    pack_info = jnp.stack(pack_info).astype(jnp.int32)
    row_at = jnp.stack(row_at).astype(jnp.int32)
    core_at = core.reshape(1).astype(jnp.int32)
    y_info = jnp.stack(y_at).astype(jnp.int32)
    tokens, pack_info, row_at, core_at, y_info = lax.optimization_barrier(
        (tokens, pack_info, row_at, core_at, y_info)
    )

    height = rows + META
    half = rows // 2
    block = pl.pallas_call(
        prepare_kernel,
        out_shape=jax.ShapeDtypeStruct((height, feat), BF16),
        in_specs=[HBM_SPEC] * 3,
        out_specs=VMEM_SPEC,
        scratch_shapes=[
            pltpu.VMEM((top, rows), jnp.int32),
            pltpu.VMEM((top, rows), BF16),
            pltpu.SemaphoreType.DMA((3,)),
        ],
        name="prepare",
        **SMALL,
    )(in_hbm(tokens), in_hbm(expert_ids.T), in_hbm(gate_weight.T))
    attn_out = grouped_attention(query, cache_k, cache_v, lengths)

    away3 = [shift(block, "attn", 6), shift(block, "attn", -6)]
    near = [shift(block, "attn", 2), shift(block, "attn", -2)]
    *near, attn_out = lax.optimization_barrier((*near, attn_out))
    right = shift(jnp.concatenate([near[0], away3[0][:half]], axis=0), "attn", 2)
    left = shift(jnp.concatenate([near[1], away3[1][half:]], axis=0), "attn", -2)
    bundle = pl.pallas_call(
        bundle_kernel,
        out_shape=jax.ShapeDtypeStruct((5 * height, feat), BF16),
        in_specs=[VMEM_SPEC] * 5,
        out_specs=VMEM_SPEC,
        name="bundle",
        **SMALL,
    )(*map(in_vmem, (block, *near, *away3)))
    swap_first = swap_cores(bundle)
    swap_last = swap_cores(jnp.concatenate([right, left], axis=0))
    operands = [block, *near, *away3, right, left, swap_first, swap_last]
    plan = [((i, 0),) for i in range(7)] + [((5, height), (6, height))]
    plan += [((7, i * height),) for i in range(5)]
    second = height + half
    plan += [((8, 0),), ((8, second),), ((8, height), (8, second + height))]

    cut = local // 2
    pack_scratch = [
        pltpu.VMEM((cut * capacity, attn_count * rows), BF16),
        pltpu.VMEM((cut * capacity, feat), BF16),
    ]
    wg, wu = pl.pallas_call(
        fetch_kernel,
        out_shape=tuple(jax.ShapeDtypeStruct(w.shape, BF16) for w in (w_gate, w_up)),
        in_specs=[HBM_SPEC] * 2,
        out_specs=(VMEM_SPEC,) * 2,
        scratch_shapes=[pltpu.SemaphoreType.DMA((2,))],
        name="weights",
        **SMALL,
    )(in_hbm(w_gate), in_hbm(w_up))
    part_shapes = (jax.ShapeDtypeStruct((cut, dest_rows, 2 * ff), BF16),) * n_expert
    pack_cost = pl.CostEstimate(flops=2 * 10**9, bytes_accessed=6 * 10**6, transcendentals=0)
    *parts_a, route, tok = pl.pallas_call(
        functools.partial(pack_kernel, plan, half, local, n_expert),
        out_shape=(
            *part_shapes,
            jax.ShapeDtypeStruct((attn_count, 8, rows), F32),
            jax.ShapeDtypeStruct((attn_count * rows, feat), BF16),
        ),
        in_specs=[SMEM_SPEC] + [VMEM_SPEC] * (len(operands) + 2),
        out_specs=(VMEM_SPEC,) * (n_expert + 2),
        scratch_shapes=[
            pltpu.VMEM((2 * META, attn_count * rows), F32),
            *pack_scratch,
        ],
        compiler_params=pltpu.CompilerParams(vmem_limit_bytes=7 << 20),
        cost_estimate=pack_cost,
        name="pack",
    )(pack_info, *map(in_vmem, (*operands, wg, wu)))
    parts_b = pl.pallas_call(
        functools.partial(pack_more_kernel, cut),
        out_shape=part_shapes,
        in_specs=[SMEM_SPEC] + [VMEM_SPEC] * 4,
        out_specs=(VMEM_SPEC,) * n_expert,
        scratch_shapes=pack_scratch,
        compiler_params=pltpu.CompilerParams(vmem_limit_bytes=7 << 20),
        cost_estimate=pack_cost,
        name="pack_more",
    )(pack_info, *map(in_vmem, (tok, route, wg, wu)))

    terms = sum(scatter_sum([parts_a, parts_b], "expert"), ())
    hidden = pl.pallas_call(
        hidden_kernel,
        out_shape=jax.ShapeDtypeStruct((local, dest_rows, ff), BF16),
        in_specs=[VMEM_SPEC] * len(terms),
        out_specs=VMEM_SPEC,
        name="hidden",
        **SMALL,
    )(*map(in_vmem, terms))

    r2, l2 = shift(hidden, "expert", 2), shift(hidden, "expert", -2)
    r1, l1 = shift(hidden, "expert", 1), shift(hidden, "expert", -1)
    r4, l4 = shift(r2[:cut], "expert", 2), shift(l2[cut:], "expert", -2)
    r3, l3 = shift(r2, "expert", 1), shift(l2, "expert", -1)
    pieces_in = [hidden, r1, l1, r2, l2, r3, l3, r4, l4]
    where = [(0, 1 + k % n_expert) for k in (0, -1, 1, -2, 2, -3, 3, -4)] + [(cut, 1 + 4)]

    mix_shape = jax.ShapeDtypeStruct((chips * rows, local * capacity), BF16)
    mix_away, mix_home, wd = pl.pallas_call(
        mix_kernel,
        out_shape=(mix_shape, mix_shape, jax.ShapeDtypeStruct(w_down.shape, BF16)),
        in_specs=[SMEM_SPEC, VMEM_SPEC, HBM_SPEC],
        out_specs=(VMEM_SPEC,) * 3,
        scratch_shapes=[pltpu.SemaphoreType.DMA],
        name="mix",
        **SMALL,
    )(core_at, in_vmem(route), in_hbm(w_down))
    away, res = pl.pallas_call(
        functools.partial(down_kernel, where),
        out_shape=(
            jax.ShapeDtypeStruct((chips, rows, feat), BF16),
            jax.ShapeDtypeStruct((local * capacity, feat), BF16),
        ),
        in_specs=[SMEM_SPEC] + [VMEM_SPEC] * (len(pieces_in) + 2),
        out_specs=(VMEM_SPEC, VMEM_SPEC),
        scratch_shapes=[pltpu.VMEM((local, capacity, ff), BF16)],
        compiler_params=pltpu.CompilerParams(vmem_limit_bytes=4 << 20),
        cost_estimate=pl.CostEstimate(flops=2 * 10**9, bytes_accessed=6 * 10**6, transcendentals=0),
        name="down",
    )(row_at, *map(in_vmem, pieces_in), in_vmem(wd), in_vmem(mix_away))
    swapped = swap_cores(away)
    home = pl.pallas_call(
        home_kernel,
        out_shape=jax.ShapeDtypeStruct((chips, rows, feat), BF16),
        in_specs=[VMEM_SPEC, VMEM_SPEC],
        out_specs=VMEM_SPEC,
        cost_estimate=pl.CostEstimate(flops=10**9, bytes_accessed=2 * 10**6, transcendentals=0),
        name="home",
        **SMALL,
    )(in_vmem(mix_home), in_vmem(res))

    block_shape = jax.ShapeDtypeStruct((rows, feat), BF16)
    long_shape = jax.ShapeDtypeStruct((rows + rows // 2, feat), BF16)
    right, left = pl.pallas_call(
        first_kernel,
        out_shape=(long_shape, long_shape),
        in_specs=[SMEM_SPEC, VMEM_SPEC, VMEM_SPEC],
        out_specs=(VMEM_SPEC,) * 2,
        name="first",
        **SMALL,
    )(y_info, in_vmem(home), in_vmem(swapped))
    right, left = shift(right, "attn", 2), shift(left, "attn", -2)
    total = pl.pallas_call(
        rest_kernel,
        out_shape=jax.ShapeDtypeStruct((5, rows, feat), BF16),
        in_specs=[SMEM_SPEC, VMEM_SPEC, VMEM_SPEC],
        out_specs=VMEM_SPEC,
        name="rest",
        **SMALL,
    )(y_info, in_vmem(home), in_vmem(swapped))
    far_right, far_left, near_right, near_left = pl.pallas_call(
        relay_kernel,
        out_shape=(block_shape,) * 4,
        in_specs=[VMEM_SPEC] * 3,
        out_specs=(VMEM_SPEC,) * 4,
        name="relay",
        **SMALL,
    )(in_vmem(total), in_vmem(right), in_vmem(left))
    last = [
        shift(far_right, "attn", 6),
        shift(far_left, "attn", -6),
        shift(near_right, "attn", 2),
        shift(near_left, "attn", -2),
    ]
    moe_out = pl.pallas_call(
        finish_kernel,
        out_shape=block_shape,
        in_specs=[VMEM_SPEC] * 5,
        out_specs=VMEM_SPEC,
        name="finish",
        **SMALL,
    )(in_vmem(total), *map(in_vmem, last))
    return (moe_out, attn_out)


def solution(mesh):
    return jax.shard_map(
        step,
        mesh=mesh,
        in_specs=(
            P(("groups", "attn"), "expert"),
            P(("groups", "attn"), None),
            P(("groups", "attn"), None),
            P("attn", "expert", None),
            P("attn", "expert", None),
            P("attn", None, "expert"),
            P(("groups", "attn", "expert"), None, None),
            P(("groups", "attn", "expert"), None, None, None),
            P(("groups", "attn", "expert"), None, None, None),
            P(("groups", "attn", "expert")),
        ),
        out_specs=(P(("groups", "attn"), "expert"), P(("groups", "attn", "expert"), None)),
        check_vma=False,
    )
```

```python
import functools

import jax
import jax.numpy as jnp
from jax import lax
from jax.experimental import pallas as pl
from jax.experimental.pallas import tpu as pltpu
from jax.sharding import PartitionSpec as P


F32 = jnp.float32
BF16 = jnp.bfloat16
META = 8
VMEM_SPEC = pl.BlockSpec(memory_space=pltpu.VMEM)
SMEM_SPEC = pl.BlockSpec(memory_space=pltpu.SMEM)
HBM_SPEC = pl.BlockSpec(memory_space=pltpu.HBM)
SMALL = {"compiler_params": pltpu.CompilerParams(vmem_limit_bytes=2 << 20)}


def both_cores(home, swapped, i):
    return home[i].astype(F32) + swapped[i].astype(F32)


def first_kernel(home, swapped, three, four, one):
    rows = home.shape[1]
    four[...] = both_cores(home, swapped, 6).astype(BF16)
    for c in range(2):
        three[c * rows : (c + 1) * rows, :] = both_cores(home, swapped, 4 + c).astype(BF16)
        one[c * rows : (c + 1) * rows, :] = both_cores(home, swapped, c).astype(BF16)


def relay_kernel(home, swapped, three, four, two):
    rows = home.shape[1]
    came = three[...].astype(F32)
    two[0:rows, :] = (
        both_cores(home, swapped, 2) + (came[0:rows] + four[...].astype(F32))
    ).astype(BF16)
    two[rows:, :] = (both_cores(home, swapped, 3) + came[rows:]).astype(BF16)


def cross_kernel(home, swapped, one, two, own, other):
    rows = home.shape[1]
    total = one[...].astype(F32) + two[...].astype(F32)
    other[...] = total[rows:].astype(BF16)
    own[...] = total[0:rows] + both_cores(home, swapped, 7)


def finish_kernel(own, came, out):
    out[...] = (own[...] + came[...].astype(F32)).astype(BF16)


def in_hbm(value):
    return pltpu.with_memory_space_constraint(value, pltpu.HBM)


def in_vmem(value):
    return pltpu.with_memory_space_constraint(value, pltpu.VMEM)


def attention_kernel(lengths, query, cache_k, cache_v, out):
    heads, size = query.shape[1:]
    spots, groups, _ = cache_k.shape[1:]
    columns = spots * groups
    keys = cache_k[0].reshape(columns, size)
    values = cache_v[0].reshape(columns, size)
    scores = lax.dot_general(
        query[0], keys, (((1,), (1,)), ((), ())), preferred_element_type=F32
    ) * size ** (-0.5)
    place = lax.broadcasted_iota(jnp.int32, (heads, columns), 1)
    head = lax.broadcasted_iota(jnp.int32, (heads, columns), 0)
    live = (place % groups == head // (heads // groups)) & (
        place < lengths[pl.program_id(0)] * groups
    )
    masked = jnp.where(live, scores, -jnp.inf)
    weighted = jnp.exp(masked - jnp.max(masked, axis=1, keepdims=True))
    prob = (weighted / jnp.sum(weighted, axis=1, keepdims=True)).astype(BF16)
    out[0] = jnp.dot(prob, values, preferred_element_type=F32).astype(BF16)


def grouped_attention(query, cache_k, cache_v, lengths):
    count, heads, size = query.shape
    _, spots, groups, _ = cache_k.shape
    cache = pl.BlockSpec((1, spots, groups, size), lambda i: (i, 0, 0, 0))
    row = pl.BlockSpec((1, heads, size), lambda i: (i, 0, 0))
    out = pl.pallas_call(
        attention_kernel,
        grid=(count,),
        out_shape=jax.ShapeDtypeStruct((count, heads, size), BF16),
        in_specs=[SMEM_SPEC, row, cache, cache],
        out_specs=row,
        compiler_params=pltpu.CompilerParams(vmem_limit_bytes=12 << 20),
        cost_estimate=pl.CostEstimate(
            flops=10**9, bytes_accessed=3 * 10**6, transcendentals=4 * 10**5
        ),
        name="attention",
    )(lengths, in_hbm(query), in_hbm(cache_k), in_hbm(cache_v))
    return out.reshape(count, heads * size)


def shift(value, axis, step):
    count = lax.axis_size(axis)
    return lax.ppermute(value, axis, [(i, (i + step) % count) for i in range(count)])


def both_ways(value, places):
    count = lax.axis_size("attn")
    pairs = [(i, (i + (-2 if i % 2 else 2) * places) % count) for i in range(count)]
    return lax.ppermute(value, "attn", pairs)


def swap_cores(value):
    return lax.ppermute(value, "attn", [(i, i ^ 1) for i in range(lax.axis_size("attn"))])


def prepare_kernel(tokens, ids, gates, block, ids_v, gates_v, sems):
    rows = tokens.shape[0]
    copies = (
        pltpu.make_async_copy(tokens, block.at[0:rows], sems.at[0]),
        pltpu.make_async_copy(ids, ids_v, sems.at[1]),
        pltpu.make_async_copy(gates, gates_v, sems.at[2]),
    )
    for copy in copies:
        copy.start()
    block[rows:, 2 * rows :] = jnp.zeros((META, block.shape[1] - 2 * rows), BF16)
    for copy in copies[1:]:
        copy.wait()
    block[rows:, 0:rows] = ids_v[...].astype(F32).astype(BF16)
    block[rows:, rows : 2 * rows] = gates_v[...]
    copies[0].wait()


def bundle_kernel(*refs):
    out = refs[-1]
    height = refs[0].shape[0]
    for i, ref in enumerate(refs[:-1]):
        out[i * height : (i + 1) * height, :] = ref[...]


def expert_parts(j0, info, place, tok, wg, wu, onehot, packed, out):
    n_blocks = place.shape[0]
    rows = tok.shape[0] // n_blocks
    n_dest = len(out)
    here_count, dest_rows, ff2 = out[0].shape
    ff = ff2 // 2
    capacity = n_dest * dest_rows
    row_id = lax.broadcasted_iota(jnp.int32, (capacity, rows), 0) + info[1 + n_blocks]
    row_id = jnp.where(row_id < capacity, row_id, row_id - capacity).astype(F32)

    def select(i, carry):
        at = pl.ds(pl.multiple_of(i * rows, rows), rows)
        block = info[1 + i]
        for j in range(here_count):
            spot = place[block, j0 + j : j0 + j + 1, :]
            onehot[j * capacity : (j + 1) * capacity, at] = jnp.where(
                row_id == spot, 1.0, 0.0
            ).astype(BF16)
        return carry

    lax.fori_loop(0, n_blocks, select, 0, unroll=2)
    packed[...] = jnp.dot(onehot[...], tok[...], preferred_element_type=F32).astype(BF16)

    def expert(j, carry):
        mine = packed[pl.ds(pl.multiple_of(j * capacity, capacity), capacity), :]
        gate = jnp.dot(mine, wg[j0 + j], preferred_element_type=F32).astype(BF16)
        up = jnp.dot(mine, wu[j0 + j], preferred_element_type=F32).astype(BF16)
        for d in range(n_dest):
            out[d][j, :, 0:ff] = gate[d * dest_rows : (d + 1) * dest_rows]
            out[d][j, :, ff:] = up[d * dest_rows : (d + 1) * dest_rows]
        return carry

    lax.fori_loop(0, here_count, expert, 0)


def fetch_kernel(wg_hbm, wu_hbm, wg, wu, sems):
    copies = (
        pltpu.make_async_copy(wg_hbm, wg, sems.at[0]),
        pltpu.make_async_copy(wu_hbm, wu, sems.at[1]),
    )
    for copy in copies:
        copy.start()
    for copy in copies:
        copy.wait()


def pack_kernel(plan, local, n_dest, info, *refs):
    n_ops = 1 + max(op for op, _ in plan)
    ops = refs[:n_ops]
    wg, wu = refs[n_ops : n_ops + 2]
    out = refs[n_ops + 2 : n_ops + 2 + n_dest]
    route, tok, meta, onehot, packed = refs[n_ops + 2 + n_dest :]
    n_blocks = len(plan)
    rows = tok.shape[0] // n_blocks
    capacity = n_dest * out[0].shape[1]

    for i, (op, r0) in enumerate(plan):
        at = pl.ds(pl.multiple_of(info[1 + i] * rows, rows), rows)
        low = r0 + rows
        tok[i * rows : (i + 1) * rows, :] = ops[op][r0:low, :]
        meta[0:8, at] = ops[op][low : low + META, 0:rows].astype(F32)
        meta[8:16, at] = ops[op][low : low + META, rows : 2 * rows].astype(F32)
    ids = meta[0:8, :]
    gates = meta[8:16, :]
    hits = [ids == (info[0] + j).astype(F32) for j in range(local)]
    stack = jnp.concatenate(
        [jnp.where(h, 1.0, 0.0) for h in hits] + [jnp.where(h, gates, 0.0) for h in hits], axis=0
    ).astype(BF16)
    one = lax.broadcasted_iota(jnp.int32, (8, 64), 0)
    two = lax.broadcasted_iota(jnp.int32, (8, 64), 1)
    pick = jnp.where(one == two // 8, 1.0, 0.0).astype(BF16)
    both = jnp.dot(pick, stack, preferred_element_type=F32)
    member = jnp.concatenate(
        [both[:, b * rows : (b + 1) * rows] for b in range(n_blocks)], axis=0
    )
    size = n_blocks * 8
    r = lax.broadcasted_iota(jnp.int32, (rows, rows), 0)
    c = lax.broadcasted_iota(jnp.int32, (rows, rows), 1)
    upper = jnp.where(r < c, 1.0, 0.0).astype(BF16)
    rr = lax.broadcasted_iota(jnp.int32, (size, size), 0)
    cc = lax.broadcasted_iota(jnp.int32, (size, size), 1)
    earlier = jnp.where((rr % 8 == cc % 8) & (cc // 8 < rr // 8), 1.0, 0.0).astype(BF16)
    member_b = member.astype(BF16)
    before = jnp.dot(earlier, member_b, preferred_element_type=F32).astype(BF16)
    place = jnp.dot(member_b, upper, preferred_element_type=F32) + jnp.dot(
        before, jnp.ones((rows, rows), BF16), preferred_element_type=F32
    )
    place = jnp.where((member > 0.5) & (place < capacity), place, -1.0)
    row = lax.broadcasted_iota(jnp.int32, (size, rows), 0)
    route[...] = jnp.where(row % 8 < local, place, member).reshape(n_blocks, 8, rows)

    expert_parts(0, info, route, tok, wg, wu, onehot, packed, out)


def pack_more_kernel(j0, info, tok, route, wg, wu, *refs):
    *out, onehot, packed = refs
    expert_parts(j0, info, route, tok, wg, wu, onehot, packed, out)


def hidden_kernel(*refs):
    *terms, out = refs
    ways = 3
    row = 0
    for s in range(len(terms) // ways):
        a, b, c = (t[...].astype(F32) for t in terms[s * ways : (s + 1) * ways])
        total = a + (b + c)
        ff = total.shape[-1] // 2
        v = total[..., :ff]
        out[row : row + total.shape[0]] = (v / (1.0 + jnp.exp(-v)) * total[..., ff:]).astype(BF16)
        row += total.shape[0]


def mix_kernel(info, route, wd_hbm, mix, wd, sem):
    copy = pltpu.make_async_copy(wd_hbm, wd, sem)
    copy.start()
    n_blocks, _, rows = route.shape
    local = wd.shape[0]
    capacity = mix.shape[1] // local
    r = lax.broadcasted_iota(jnp.int32, (rows, rows), 0)
    c = lax.broadcasted_iota(jnp.int32, (rows, rows), 1)
    eye = jnp.where(r == c, 1.0, 0.0).astype(BF16)
    col_id = lax.broadcasted_iota(jnp.int32, (rows, capacity), 1).astype(F32)

    def block(i, carry):
        at = pl.ds(pl.multiple_of(i * rows, rows), rows)
        rt = lax.dot_general(
            eye, route[info[i]].astype(BF16), (((1,), (1,)), ((), ())), preferred_element_type=F32
        )
        for j in range(local):
            mix[at, j * capacity : (j + 1) * capacity] = jnp.where(
                col_id == rt[:, j : j + 1], rt[:, local + j : local + j + 1], 0.0
            ).astype(BF16)
        return carry

    lax.fori_loop(0, n_blocks, block, 0, unroll=2)
    copy.wait()


def mix_rows(first, mix, res, ref):
    n_dest, rows, feat = ref.shape
    group = 4

    def some(g, carry):
        at = pl.ds(pl.multiple_of(first + g * group * rows, group * rows), group * rows)
        got = jnp.dot(mix[at, :], res[...], preferred_element_type=F32).astype(BF16)
        ref[pl.ds(g * group, group)] = got.reshape(group, rows, feat)
        return carry

    lax.fori_loop(0, n_dest // group, some, 0)


def down_kernel(plan, info, *refs):
    n_ops = len(plan)
    ops = refs[:n_ops]
    wd, mix, away, res, hid = refs[n_ops:]
    local = wd.shape[0]
    capacity = hid.shape[1]
    for op, (j0, slot) in zip(ops, plan):
        at = pl.multiple_of(info[slot], op.shape[1])
        for j in range(op.shape[0]):
            hid[j0 + j, pl.ds(at, op.shape[1]), :] = op[j]

    def expert(j, carry):
        res[pl.ds(pl.multiple_of(j * capacity, capacity), capacity), :] = jnp.dot(
            hid[j], wd[j], preferred_element_type=F32
        ).astype(BF16)
        return carry

    lax.fori_loop(0, local, expert, 0)
    mix_rows(0, mix, res, away)


def home_kernel(mix, res, home):
    mix_rows(mix.shape[0] // 2, mix, res, home)


def scatter_sum(pieces, axis):
    count = len(pieces[0])
    half = count // 2
    legs = {}
    for way in (1, -1):
        for s in range(2):
            start = half if (way == 1) == (s == 0) else half - 1
            legs[(way, s)] = [start, pieces[s][way * start % count]]
    for hop in range(half, 0, -1):
        for way in (1, -1):
            for s in range(2):
                leg = legs[(way, s)]
                if leg[0] != hop:
                    continue
                got = shift(leg[1], axis, way)
                if hop > 1:
                    mine = pieces[s][way * (hop - 1) % count]
                    got = (got.astype(F32) + mine.astype(F32)).astype(BF16)
                legs[(way, s)] = [hop - 1, got]
    return [(pieces[s][0], legs[(1, s)][1], legs[(-1, s)][1]) for s in range(2)]


def step(tokens, expert_ids, gate_weight, w_gate, w_up, w_down, query, cache_k, cache_v, lengths):
    rows, feat = tokens.shape
    local, _, ff = w_gate.shape
    attn_count = lax.axis_size("attn")
    n_expert = lax.axis_size("expert")
    chips = attn_count // 2
    top = expert_ids.shape[1]
    capacity = rows * top // local
    me = lax.axis_index("attn")
    col = lax.axis_index("expert")
    y = me // 2
    core = me % 2
    far = chips // 2
    dest_rows = capacity // n_expert

    x_at = [lax.rem(col + k, n_expert) for k in range(n_expert)]
    ahead = jnp.where(core == 0, 1, -1)

    def token_block(places, flip):
        return 2 * lax.rem(y + places * ahead + chips, chips) + (core ^ flip)

    order = [(0, 0), (0, 1)]
    order += [(-k, flip) for k in (1, 2, 3) for flip in (0, 1)] + [(far, 0)]
    order += [(k, flip) for k in (1, 2, 3) for flip in (1, 0)] + [(far, 1)]
    pack_info = [local * me] + [token_block(*at) for at in order]
    onward = [(k, flip) for k in (1, 2, 3) for flip in (0, 1)] + [(far, 0), (0, 0)]
    mix_info = [token_block(-k, 1 - flip) for k, flip in onward]
    mix_info += [token_block(k, flip) for k, flip in onward]
    row_at = [x * dest_rows for x in x_at]
    pack_info.append(col * dest_rows)
    pack_info = jnp.stack(pack_info).astype(jnp.int32)
    mix_info = jnp.stack(mix_info).astype(jnp.int32)
    row_at = jnp.stack(row_at).astype(jnp.int32)
    tokens, pack_info, mix_info, row_at = lax.optimization_barrier(
        (tokens, pack_info, mix_info, row_at)
    )

    height = rows + META
    block = pl.pallas_call(
        prepare_kernel,
        out_shape=jax.ShapeDtypeStruct((height, feat), BF16),
        in_specs=[HBM_SPEC] * 3,
        out_specs=VMEM_SPEC,
        scratch_shapes=[
            pltpu.VMEM((top, rows), jnp.int32),
            pltpu.VMEM((top, rows), BF16),
            pltpu.SemaphoreType.DMA((3,)),
        ],
        name="prepare",
        **SMALL,
    )(in_hbm(tokens), in_hbm(expert_ids.T), in_hbm(gate_weight.T))
    attn_out = grouped_attention(query, cache_k, cache_v, lengths)

    pair = pl.pallas_call(
        bundle_kernel,
        out_shape=jax.ShapeDtypeStruct((2 * height, feat), BF16),
        in_specs=[VMEM_SPEC] * 2,
        out_specs=VMEM_SPEC,
        name="pair",
        **SMALL,
    )(*map(in_vmem, (block, swap_cores(block))))
    two, one = both_ways(pair, 2), both_ways(pair, 1)
    four, three = both_ways(two[:height], 2), both_ways(two, 1)
    operands = [pair, one, two, three, four]
    operands += [swap_cores(one), swap_cores(two), swap_cores(three), swap_cores(four)]
    pairs = [((i, 0), (i, height)) for i in range(8) if i != 4]
    plan = [at for p in pairs[:4] for at in p] + [(4, 0)] + [at for p in pairs[4:] for at in p] + [(8, 0)]

    cut = local // 2
    pack_scratch = [
        pltpu.VMEM((cut * capacity, attn_count * rows), BF16),
        pltpu.VMEM((cut * capacity, feat), BF16),
    ]
    wg, wu = pl.pallas_call(
        fetch_kernel,
        out_shape=tuple(jax.ShapeDtypeStruct(w.shape, BF16) for w in (w_gate, w_up)),
        in_specs=[HBM_SPEC] * 2,
        out_specs=(VMEM_SPEC,) * 2,
        scratch_shapes=[pltpu.SemaphoreType.DMA((2,))],
        name="weights",
        **SMALL,
    )(in_hbm(w_gate), in_hbm(w_up))
    part_shapes = (jax.ShapeDtypeStruct((cut, dest_rows, 2 * ff), BF16),) * n_expert
    pack_cost = pl.CostEstimate(flops=2 * 10**9, bytes_accessed=6 * 10**6, transcendentals=0)
    *parts_a, route, tok = pl.pallas_call(
        functools.partial(pack_kernel, plan, local, n_expert),
        out_shape=(
            *part_shapes,
            jax.ShapeDtypeStruct((attn_count, 8, rows), F32),
            jax.ShapeDtypeStruct((attn_count * rows, feat), BF16),
        ),
        in_specs=[SMEM_SPEC] + [VMEM_SPEC] * (len(operands) + 2),
        out_specs=(VMEM_SPEC,) * (n_expert + 2),
        scratch_shapes=[
            pltpu.VMEM((2 * META, attn_count * rows), F32),
            *pack_scratch,
        ],
        compiler_params=pltpu.CompilerParams(vmem_limit_bytes=7 << 20),
        cost_estimate=pack_cost,
        name="pack",
    )(pack_info, *map(in_vmem, (*operands, wg, wu)))
    parts_b = pl.pallas_call(
        functools.partial(pack_more_kernel, cut),
        out_shape=part_shapes,
        in_specs=[SMEM_SPEC] + [VMEM_SPEC] * 4,
        out_specs=(VMEM_SPEC,) * n_expert,
        scratch_shapes=pack_scratch,
        compiler_params=pltpu.CompilerParams(vmem_limit_bytes=7 << 20),
        cost_estimate=pack_cost,
        name="pack_more",
    )(pack_info, *map(in_vmem, (tok, route, wg, wu)))

    terms = sum(scatter_sum([parts_a, parts_b], "expert"), ())
    hidden = pl.pallas_call(
        hidden_kernel,
        out_shape=jax.ShapeDtypeStruct((local, dest_rows, ff), BF16),
        in_specs=[VMEM_SPEC] * len(terms),
        out_specs=VMEM_SPEC,
        name="hidden",
        **SMALL,
    )(*map(in_vmem, terms))

    r2, l2 = shift(hidden, "expert", 2), shift(hidden, "expert", -2)
    r1, l1 = shift(hidden, "expert", 1), shift(hidden, "expert", -1)
    r4, l4 = shift(r2[:cut], "expert", 2), shift(l2[cut:], "expert", -2)
    r3, l3 = shift(r2, "expert", 1), shift(l2, "expert", -1)
    pieces_in = [hidden, r1, l1, r2, l2, r3, l3, r4, l4]
    where = [(0, k % n_expert) for k in (0, -1, 1, -2, 2, -3, 3, -4)] + [(cut, n_expert // 2)]

    mix, wd = pl.pallas_call(
        mix_kernel,
        out_shape=(
            jax.ShapeDtypeStruct((attn_count * rows, local * capacity), BF16),
            jax.ShapeDtypeStruct(w_down.shape, BF16),
        ),
        in_specs=[SMEM_SPEC, VMEM_SPEC, HBM_SPEC],
        out_specs=(VMEM_SPEC,) * 2,
        scratch_shapes=[pltpu.SemaphoreType.DMA],
        name="mix",
        **SMALL,
    )(mix_info, in_vmem(route), in_hbm(w_down))
    away, res = pl.pallas_call(
        functools.partial(down_kernel, where),
        out_shape=(
            jax.ShapeDtypeStruct((chips, rows, feat), BF16),
            jax.ShapeDtypeStruct((local * capacity, feat), BF16),
        ),
        in_specs=[SMEM_SPEC] + [VMEM_SPEC] * (len(pieces_in) + 2),
        out_specs=(VMEM_SPEC, VMEM_SPEC),
        scratch_shapes=[pltpu.VMEM((local, capacity, ff), BF16)],
        compiler_params=pltpu.CompilerParams(vmem_limit_bytes=4 << 20),
        cost_estimate=pl.CostEstimate(flops=2 * 10**9, bytes_accessed=6 * 10**6, transcendentals=0),
        name="down",
    )(row_at, *map(in_vmem, pieces_in), in_vmem(wd), in_vmem(mix))
    swapped = swap_cores(away)
    home = pl.pallas_call(
        home_kernel,
        out_shape=jax.ShapeDtypeStruct((chips, rows, feat), BF16),
        in_specs=[VMEM_SPEC, VMEM_SPEC],
        out_specs=VMEM_SPEC,
        cost_estimate=pl.CostEstimate(flops=10**9, bytes_accessed=2 * 10**6, transcendentals=0),
        name="home",
        **SMALL,
    )(in_vmem(mix), in_vmem(res))

    def small_call(kernel, shapes, *operands):
        out = pl.pallas_call(
            kernel,
            out_shape=tuple(jax.ShapeDtypeStruct((r, feat), t) for r, t in shapes),
            in_specs=[VMEM_SPEC] * len(operands),
            out_specs=(VMEM_SPEC,) * len(shapes),
            **SMALL,
        )(*map(in_vmem, operands))
        return out if len(shapes) > 1 else out[0]

    twice = (2 * rows, BF16)
    once = (rows, BF16)
    three, four, one = small_call(first_kernel, (twice, once, twice), home, swapped)
    four, three, one = both_ways(four, 2), both_ways(three, 1), both_ways(one, 1)
    two = small_call(relay_kernel, (twice,), home, swapped, three, four)
    two = both_ways(two, 2)
    own, other = small_call(cross_kernel, ((rows, F32), once), home, swapped, one, two)
    moe_out = small_call(finish_kernel, (once,), own, swap_cores(other))
    return (moe_out, attn_out)


def solution(mesh):
    return jax.shard_map(
        step,
        mesh=mesh,
        in_specs=(
            P(("groups", "attn"), "expert"),
            P(("groups", "attn"), None),
            P(("groups", "attn"), None),
            P("attn", "expert", None),
            P("attn", "expert", None),
            P("attn", None, "expert"),
            P(("groups", "attn", "expert"), None, None),
            P(("groups", "attn", "expert"), None, None, None),
            P(("groups", "attn", "expert"), None, None, None),
            P(("groups", "attn", "expert")),
        ),
        out_specs=(P(("groups", "attn"), "expert"), P(("groups", "attn", "expert"), None)),
        check_vma=False,
    )
```

```python
import functools

import jax
import jax.numpy as jnp
from jax import lax
from jax.experimental import pallas as pl
from jax.experimental.pallas import tpu as pltpu
from jax.sharding import PartitionSpec as P


F32 = jnp.float32
BF16 = jnp.bfloat16
META = 8
VMEM_SPEC = pl.BlockSpec(memory_space=pltpu.VMEM)
SMEM_SPEC = pl.BlockSpec(memory_space=pltpu.SMEM)
HBM_SPEC = pl.BlockSpec(memory_space=pltpu.HBM)
SMALL = {"compiler_params": pltpu.CompilerParams(vmem_limit_bytes=2 << 20)}


def both_cores(home, swapped, i):
    return home[i].astype(F32) + swapped[i].astype(F32)


def far_kernel(home, swapped, three, four):
    rows = home.shape[1]
    four[...] = both_cores(home, swapped, 2).astype(BF16)
    for c in range(2):
        three[c * rows : (c + 1) * rows, :] = both_cores(home, swapped, c).astype(BF16)


def one_kernel(home, swapped, own, other):
    own[...] = both_cores(home, swapped, 0).astype(BF16)
    other[...] = both_cores(home, swapped, 1).astype(BF16)


def relay_kernel(home, swapped, three, four, own, other):
    rows = home.shape[1]
    came = three[...].astype(F32)
    own[...] = (both_cores(home, swapped, 2) + (came[0:rows] + four[...].astype(F32))).astype(BF16)
    other[...] = (both_cores(home, swapped, 3) + came[rows:]).astype(BF16)


def finish_kernel(home, swapped, a, b, c, d, out):
    came = (a[...].astype(F32) + b[...].astype(F32)) + (c[...].astype(F32) + d[...].astype(F32))
    out[...] = (both_cores(home, swapped, 3) + came).astype(BF16)


def in_hbm(value):
    return pltpu.with_memory_space_constraint(value, pltpu.HBM)


def in_vmem(value):
    return pltpu.with_memory_space_constraint(value, pltpu.VMEM)


def attention_kernel(lengths, query, cache_k, cache_v, out):
    heads, size = query.shape[1:]
    spots, groups, _ = cache_k.shape[1:]
    columns = spots * groups
    keys = cache_k[0].reshape(columns, size)
    values = cache_v[0].reshape(columns, size)
    scores = lax.dot_general(
        query[0], keys, (((1,), (1,)), ((), ())), preferred_element_type=F32
    ) * size ** (-0.5)
    place = lax.broadcasted_iota(jnp.int32, (heads, columns), 1)
    head = lax.broadcasted_iota(jnp.int32, (heads, columns), 0)
    live = (place % groups == head // (heads // groups)) & (
        place < lengths[pl.program_id(0)] * groups
    )
    masked = jnp.where(live, scores, -jnp.inf)
    weighted = jnp.exp(masked - jnp.max(masked, axis=1, keepdims=True))
    prob = (weighted / jnp.sum(weighted, axis=1, keepdims=True)).astype(BF16)
    out[0] = jnp.dot(prob, values, preferred_element_type=F32).astype(BF16)


def grouped_attention(query, cache_k, cache_v, lengths):
    count, heads, size = query.shape
    _, spots, groups, _ = cache_k.shape
    cache = pl.BlockSpec((1, spots, groups, size), lambda i: (i, 0, 0, 0))
    row = pl.BlockSpec((1, heads, size), lambda i: (i, 0, 0))
    out = pl.pallas_call(
        attention_kernel,
        grid=(count,),
        out_shape=jax.ShapeDtypeStruct((count, heads, size), BF16),
        in_specs=[SMEM_SPEC, row, cache, cache],
        out_specs=row,
        compiler_params=pltpu.CompilerParams(vmem_limit_bytes=12 << 20),
        cost_estimate=pl.CostEstimate(
            flops=10**9, bytes_accessed=3 * 10**6, transcendentals=4 * 10**5
        ),
        name="attention",
    )(lengths, in_hbm(query), in_hbm(cache_k), in_hbm(cache_v))
    return out.reshape(count, heads * size)


def shift(value, axis, step):
    count = lax.axis_size(axis)
    return lax.ppermute(value, axis, [(i, (i + step) % count) for i in range(count)])


def both_ways(value, places, cross=0):
    count = lax.axis_size("attn")
    pairs = [(i, (i + (-2 if i % 2 else 2) * places) % count ^ cross) for i in range(count)]
    return lax.ppermute(value, "attn", pairs)


def swap_cores(value):
    return lax.ppermute(value, "attn", [(i, i ^ 1) for i in range(lax.axis_size("attn"))])


def prepare_kernel(tokens, ids, gates, block, ids_v, gates_v, sems):
    rows = tokens.shape[0]
    copies = (
        pltpu.make_async_copy(tokens, block.at[0:rows], sems.at[0]),
        pltpu.make_async_copy(ids, ids_v, sems.at[1]),
        pltpu.make_async_copy(gates, gates_v, sems.at[2]),
    )
    for copy in copies:
        copy.start()
    block[rows:, 2 * rows :] = jnp.zeros((META, block.shape[1] - 2 * rows), BF16)
    for copy in copies[1:]:
        copy.wait()
    block[rows:, 0:rows] = ids_v[...].astype(F32).astype(BF16)
    block[rows:, rows : 2 * rows] = gates_v[...]
    copies[0].wait()


def bundle_kernel(*refs):
    out = refs[-1]
    height = refs[0].shape[0]
    for i, ref in enumerate(refs[:-1]):
        out[i * height : (i + 1) * height, :] = ref[...]


def expert_parts(j0, info, place, tok, wg, wu, onehot, out):
    n_blocks = place.shape[0]
    rows = tok.shape[0] // n_blocks
    n_dest = len(out)
    here_count, dest_rows, ff2 = out[0].shape
    ff = ff2 // 2
    capacity = n_dest * dest_rows
    row_id = lax.broadcasted_iota(jnp.int32, (capacity, rows), 0) + info[1 + n_blocks]
    row_id = jnp.where(row_id < capacity, row_id, row_id - capacity).astype(F32)

    def expert(j, carry):
        for i in range(n_blocks):
            spot = place[info[1 + i], pl.ds(j0 + j, 1), :]
            onehot[:, i * rows : (i + 1) * rows] = jnp.where(row_id == spot, 1.0, 0.0).astype(BF16)
        mine = jnp.dot(onehot[...], tok[...], preferred_element_type=F32).astype(BF16)
        gate = jnp.dot(mine, wg[j0 + j], preferred_element_type=F32).astype(BF16)
        up = jnp.dot(mine, wu[j0 + j], preferred_element_type=F32).astype(BF16)
        for d in range(n_dest):
            out[d][j, :, 0:ff] = gate[d * dest_rows : (d + 1) * dest_rows]
            out[d][j, :, ff:] = up[d * dest_rows : (d + 1) * dest_rows]
        return carry

    lax.fori_loop(0, here_count, expert, 0)


def fetch_kernel(wg_hbm, wu_hbm, wg, wu, sems):
    copies = (
        pltpu.make_async_copy(wg_hbm, wg, sems.at[0]),
        pltpu.make_async_copy(wu_hbm, wu, sems.at[1]),
    )
    for copy in copies:
        copy.start()
    for copy in copies:
        copy.wait()


def pack_kernel(plan, local, n_dest, info, *refs):
    n_ops = 1 + max(op for op, _ in plan)
    ops = refs[:n_ops]
    wg, wu = refs[n_ops : n_ops + 2]
    out = refs[n_ops + 2 : n_ops + 2 + n_dest]
    route, tok, meta, onehot = refs[n_ops + 2 + n_dest :]
    n_blocks = len(plan)
    rows = tok.shape[0] // n_blocks
    capacity = n_dest * out[0].shape[1]

    for i, (op, r0) in enumerate(plan):
        at = pl.ds(pl.multiple_of(info[1 + i] * rows, rows), rows)
        low = r0 + rows
        tok[i * rows : (i + 1) * rows, :] = ops[op][r0:low, :]
        meta[0:8, at] = ops[op][low : low + META, 0:rows].astype(F32)
        meta[8:16, at] = ops[op][low : low + META, rows : 2 * rows].astype(F32)
    ids = meta[0:8, :]
    gates = meta[8:16, :]
    hits = [ids == (info[0] + j).astype(F32) for j in range(local)]
    stack = jnp.concatenate(
        [jnp.where(h, 1.0, 0.0) for h in hits] + [jnp.where(h, gates, 0.0) for h in hits], axis=0
    ).astype(BF16)
    one = lax.broadcasted_iota(jnp.int32, (8, 64), 0)
    two = lax.broadcasted_iota(jnp.int32, (8, 64), 1)
    pick = jnp.where(one == two // 8, 1.0, 0.0).astype(BF16)
    both = jnp.dot(pick, stack, preferred_element_type=F32)
    member = jnp.concatenate(
        [both[:, b * rows : (b + 1) * rows] for b in range(n_blocks)], axis=0
    )
    size = n_blocks * 8
    r = lax.broadcasted_iota(jnp.int32, (rows, rows), 0)
    c = lax.broadcasted_iota(jnp.int32, (rows, rows), 1)
    upper = jnp.where(r < c, 1.0, 0.0).astype(BF16)
    rr = lax.broadcasted_iota(jnp.int32, (size, size), 0)
    cc = lax.broadcasted_iota(jnp.int32, (size, size), 1)
    earlier = jnp.where((rr % 8 == cc % 8) & (cc // 8 < rr // 8), 1.0, 0.0).astype(BF16)
    member_b = member.astype(BF16)
    before = jnp.dot(earlier, member_b, preferred_element_type=F32).astype(BF16)
    place = jnp.dot(member_b, upper, preferred_element_type=F32) + jnp.dot(
        before, jnp.ones((rows, rows), BF16), preferred_element_type=F32
    )
    place = jnp.where((member > 0.5) & (place < capacity), place, -1.0)
    row = lax.broadcasted_iota(jnp.int32, (size, rows), 0)
    route[...] = jnp.where(row % 8 < local, place, member).reshape(n_blocks, 8, rows)

    expert_parts(0, info, route, tok, wg, wu, onehot, out)


def pack_more_kernel(j0, info, tok, route, wg, wu, *refs):
    *out, onehot = refs
    expert_parts(j0, info, route, tok, wg, wu, onehot, out)


def hidden_kernel(*refs):
    *terms, out = refs
    ways = 3
    row = 0
    for s in range(len(terms) // ways):
        a, b, c = (t[...].astype(F32) for t in terms[s * ways : (s + 1) * ways])
        total = a + (b + c)
        ff = total.shape[-1] // 2
        v = total[..., :ff]
        out[row : row + total.shape[0]] = (v / (1.0 + jnp.exp(-v)) * total[..., ff:]).astype(BF16)
        row += total.shape[0]


def mix_kernel(info, route, wd_hbm, mix, wd, sem):
    copy = pltpu.make_async_copy(wd_hbm, wd, sem)
    copy.start()
    n_blocks, _, rows = route.shape
    local = wd.shape[0]
    capacity = mix.shape[1] // local
    r = lax.broadcasted_iota(jnp.int32, (rows, rows), 0)
    c = lax.broadcasted_iota(jnp.int32, (rows, rows), 1)
    eye = jnp.where(r == c, 1.0, 0.0).astype(BF16)
    col_id = lax.broadcasted_iota(jnp.int32, (rows, capacity), 1).astype(F32)

    def block(i, carry):
        at = pl.ds(pl.multiple_of(i * rows, rows), rows)
        rt = lax.dot_general(
            eye, route[info[i]].astype(BF16), (((1,), (1,)), ((), ())), preferred_element_type=F32
        )
        for j in range(local):
            mix[at, j * capacity : (j + 1) * capacity] = jnp.where(
                col_id == rt[:, j : j + 1], rt[:, local + j : local + j + 1], 0.0
            ).astype(BF16)
        return carry

    lax.fori_loop(0, n_blocks, block, 0, unroll=2)
    copy.wait()


def mix_rows(quarter, mix, res, ref):
    n_dest, rows, feat = ref.shape
    group = 2

    def some(g, carry):
        at = (quarter * n_dest + g * group) * rows
        at = pl.ds(pl.multiple_of(at, group * rows), group * rows)
        got = jnp.dot(mix[at, :], res[...], preferred_element_type=F32).astype(BF16)
        ref[pl.ds(g * group, group)] = got.reshape(group, rows, feat)
        return carry

    lax.fori_loop(0, n_dest // group, some, 0)


def down_kernel(plan, info, *refs):
    n_ops = len(plan)
    ops = refs[:n_ops]
    wd, mix, away, res, hid = refs[n_ops:]
    local = wd.shape[0]
    capacity = hid.shape[1]
    for op, (j0, slot) in zip(ops, plan):
        at = pl.multiple_of(info[slot], op.shape[1])
        for j in range(op.shape[0]):
            hid[j0 + j, pl.ds(at, op.shape[1]), :] = op[j]

    def expert(j, carry):
        res[pl.ds(pl.multiple_of(j * capacity, capacity), capacity), :] = jnp.dot(
            hid[j], wd[j], preferred_element_type=F32
        ).astype(BF16)
        return carry

    lax.fori_loop(0, local, expert, 0)
    mix_rows(0, mix, res, away)


def second_kernel(mix, res, home, away):
    mix_rows(1, mix, res, away)
    mix_rows(2, mix, res, home)


def third_kernel(mix, res, home):
    mix_rows(3, mix, res, home)


def scatter_sum(pieces, axis):
    count = len(pieces[0])
    half = count // 2
    legs = {}
    for way in (1, -1):
        for s in range(2):
            start = half if (way == 1) == (s == 0) else half - 1
            legs[(way, s)] = [start, pieces[s][way * start % count]]
    for hop in range(half, 0, -1):
        for way in (1, -1):
            for s in range(2):
                leg = legs[(way, s)]
                if leg[0] != hop:
                    continue
                got = shift(leg[1], axis, way)
                if hop > 1:
                    mine = pieces[s][way * (hop - 1) % count]
                    got = (got.astype(F32) + mine.astype(F32)).astype(BF16)
                legs[(way, s)] = [hop - 1, got]
    return [(pieces[s][0], legs[(1, s)][1], legs[(-1, s)][1]) for s in range(2)]


def step(tokens, expert_ids, gate_weight, w_gate, w_up, w_down, query, cache_k, cache_v, lengths):
    rows, feat = tokens.shape
    local, _, ff = w_gate.shape
    attn_count = lax.axis_size("attn")
    n_expert = lax.axis_size("expert")
    chips = attn_count // 2
    top = expert_ids.shape[1]
    capacity = rows * top // local
    me = lax.axis_index("attn")
    col = lax.axis_index("expert")
    y = me // 2
    core = me % 2
    far = chips // 2
    dest_rows = capacity // n_expert

    x_at = [lax.rem(col + k, n_expert) for k in range(n_expert)]
    ahead = jnp.where(core == 0, 1, -1)

    def token_block(places, flip):
        return 2 * lax.rem(y + places * ahead + chips, chips) + (core ^ flip)

    order = [(0, 0), (0, 1)]
    order += [(-k, flip) for k in (1, 2, 3) for flip in (0, 1)] + [(far, 0)]
    order += [(k, flip) for k in (1, 2, 3) for flip in (1, 0)] + [(far, 1)]
    pack_info = [local * me] + [token_block(*at) for at in order]
    onward = [(3, 0), (3, 1), (far, 0), (0, 0)], [(1, 0), (1, 1), (2, 0), (2, 1)]
    for_other = [[token_block(-k, 1 - flip) for k, flip in part] for part in onward]
    for_own = [[token_block(k, flip) for k, flip in part] for part in onward]
    mix_info = for_other[0] + for_other[1] + for_own[0] + for_own[1]
    row_at = [x * dest_rows for x in x_at]
    pack_info.append(col * dest_rows)
    pack_info = jnp.stack(pack_info).astype(jnp.int32)
    mix_info = jnp.stack(mix_info).astype(jnp.int32)
    row_at = jnp.stack(row_at).astype(jnp.int32)
    tokens, pack_info, mix_info, row_at = lax.optimization_barrier(
        (tokens, pack_info, mix_info, row_at)
    )

    height = rows + META
    block = pl.pallas_call(
        prepare_kernel,
        out_shape=jax.ShapeDtypeStruct((height, feat), BF16),
        in_specs=[HBM_SPEC] * 3,
        out_specs=VMEM_SPEC,
        scratch_shapes=[
            pltpu.VMEM((top, rows), jnp.int32),
            pltpu.VMEM((top, rows), BF16),
            pltpu.SemaphoreType.DMA((3,)),
        ],
        name="prepare",
        **SMALL,
    )(in_hbm(tokens), in_hbm(expert_ids.T), in_hbm(gate_weight.T))
    attn_out = grouped_attention(query, cache_k, cache_v, lengths)

    def pass_on(value, places, cross=0):
        return both_ways(value, places, cross)

    pair = pl.pallas_call(
        bundle_kernel,
        out_shape=jax.ShapeDtypeStruct((2 * height, feat), BF16),
        in_specs=[VMEM_SPEC] * 2,
        out_specs=VMEM_SPEC,
        name="pair",
        **SMALL,
    )(*map(in_vmem, (block, swap_cores(block))))
    two, one = pass_on(pair, 2), pass_on(pair, 1)
    four, three = pass_on(two[:height], 2), pass_on(two, 1)
    operands = [pair, one, two, three, four]
    operands += [swap_cores(one), swap_cores(two), swap_cores(three), swap_cores(four)]
    pairs = [((i, 0), (i, height)) for i in range(8) if i != 4]
    plan = [at for p in pairs[:4] for at in p] + [(4, 0)] + [at for p in pairs[4:] for at in p] + [(8, 0)]

    cut = local // 2
    pack_scratch = [
        pltpu.VMEM((capacity, attn_count * rows), BF16),
    ]
    wg, wu = pl.pallas_call(
        fetch_kernel,
        out_shape=tuple(jax.ShapeDtypeStruct(w.shape, BF16) for w in (w_gate, w_up)),
        in_specs=[HBM_SPEC] * 2,
        out_specs=(VMEM_SPEC,) * 2,
        scratch_shapes=[pltpu.SemaphoreType.DMA((2,))],
        name="weights",
        **SMALL,
    )(in_hbm(w_gate), in_hbm(w_up))
    part_shapes = (jax.ShapeDtypeStruct((cut, dest_rows, 2 * ff), BF16),) * n_expert
    pack_cost = pl.CostEstimate(flops=2 * 10**9, bytes_accessed=6 * 10**6, transcendentals=0)
    *parts_a, route, tok = pl.pallas_call(
        functools.partial(pack_kernel, plan, local, n_expert),
        out_shape=(
            *part_shapes,
            jax.ShapeDtypeStruct((attn_count, 8, rows), F32),
            jax.ShapeDtypeStruct((attn_count * rows, feat), BF16),
        ),
        in_specs=[SMEM_SPEC] + [VMEM_SPEC] * (len(operands) + 2),
        out_specs=(VMEM_SPEC,) * (n_expert + 2),
        scratch_shapes=[
            pltpu.VMEM((2 * META, attn_count * rows), F32),
            *pack_scratch,
        ],
        compiler_params=pltpu.CompilerParams(vmem_limit_bytes=7 << 20),
        cost_estimate=pack_cost,
        name="pack",
    )(pack_info, *map(in_vmem, (*operands, wg, wu)))
    parts_b = pl.pallas_call(
        functools.partial(pack_more_kernel, cut),
        out_shape=part_shapes,
        in_specs=[SMEM_SPEC] + [VMEM_SPEC] * 4,
        out_specs=(VMEM_SPEC,) * n_expert,
        scratch_shapes=pack_scratch,
        compiler_params=pltpu.CompilerParams(vmem_limit_bytes=7 << 20),
        cost_estimate=pack_cost,
        name="pack_more",
    )(pack_info, *map(in_vmem, (tok, route, wg, wu)))

    terms = sum(scatter_sum([parts_a, parts_b], "expert"), ())
    hidden = pl.pallas_call(
        hidden_kernel,
        out_shape=jax.ShapeDtypeStruct((local, dest_rows, ff), BF16),
        in_specs=[VMEM_SPEC] * len(terms),
        out_specs=VMEM_SPEC,
        name="hidden",
        **SMALL,
    )(*map(in_vmem, terms))

    r2, l2 = shift(hidden, "expert", 2), shift(hidden, "expert", -2)
    r1, l1 = shift(hidden, "expert", 1), shift(hidden, "expert", -1)
    r4, l4 = shift(r2[:cut], "expert", 2), shift(l2[cut:], "expert", -2)
    r3, l3 = shift(r2, "expert", 1), shift(l2, "expert", -1)
    pieces_in = [hidden, r1, l1, r2, l2, r3, l3, r4, l4]
    where = [(0, k % n_expert) for k in (0, -1, 1, -2, 2, -3, 3, -4)] + [(cut, n_expert // 2)]

    mix, wd = pl.pallas_call(
        mix_kernel,
        out_shape=(
            jax.ShapeDtypeStruct((attn_count * rows, local * capacity), BF16),
            jax.ShapeDtypeStruct(w_down.shape, BF16),
        ),
        in_specs=[SMEM_SPEC, VMEM_SPEC, HBM_SPEC],
        out_specs=(VMEM_SPEC,) * 2,
        scratch_shapes=[pltpu.SemaphoreType.DMA],
        name="mix",
        **SMALL,
    )(mix_info, in_vmem(route), in_hbm(w_down))
    quarter = jax.ShapeDtypeStruct((attn_count // 4, rows, feat), BF16)
    away_far, res = pl.pallas_call(
        functools.partial(down_kernel, where),
        out_shape=(quarter, jax.ShapeDtypeStruct((local * capacity, feat), BF16)),
        in_specs=[SMEM_SPEC] + [VMEM_SPEC] * (len(pieces_in) + 2),
        out_specs=(VMEM_SPEC, VMEM_SPEC),
        scratch_shapes=[pltpu.VMEM((local, capacity, ff), BF16)],
        compiler_params=pltpu.CompilerParams(vmem_limit_bytes=4 << 20),
        cost_estimate=pl.CostEstimate(flops=2 * 10**9, bytes_accessed=6 * 10**6, transcendentals=0),
        name="down",
    )(row_at, *map(in_vmem, pieces_in), in_vmem(wd), in_vmem(mix))

    def small_call(kernel, shapes, *operands):
        out = pl.pallas_call(
            kernel,
            out_shape=shapes,
            in_specs=[VMEM_SPEC] * len(operands),
            out_specs=(VMEM_SPEC,) * len(shapes),
            **SMALL,
        )(*map(in_vmem, operands))
        return out if len(shapes) > 1 else out[0]

    once = jax.ShapeDtypeStruct((rows, feat), BF16)
    twice = jax.ShapeDtypeStruct((2 * rows, feat), BF16)
    came_far = swap_cores(away_far)
    home_far, away_near = small_call(second_kernel, (quarter, quarter), mix, res)
    came_near = swap_cores(away_near)
    three, four = small_call(far_kernel, (twice, once), home_far, came_far)
    four, three = pass_on(four, 2), pass_on(three, 1)
    home_near = small_call(third_kernel, (quarter,), mix, res)
    own, other = small_call(one_kernel, (once, once), home_near, came_near)
    last = [pass_on(own, 1), pass_on(other, 1, 1)]
    own, other = small_call(relay_kernel, (once, once), home_near, came_near, three, four)
    last += [pass_on(own, 2), pass_on(other, 2, 1)]
    moe_out = small_call(finish_kernel, (once,), home_far, came_far, *last)
    return (moe_out, attn_out)


def solution(mesh):
    return jax.shard_map(
        step,
        mesh=mesh,
        in_specs=(
            P(("groups", "attn"), "expert"),
            P(("groups", "attn"), None),
            P(("groups", "attn"), None),
            P("attn", "expert", None),
            P("attn", "expert", None),
            P("attn", None, "expert"),
            P(("groups", "attn", "expert"), None, None),
            P(("groups", "attn", "expert"), None, None, None),
            P(("groups", "attn", "expert"), None, None, None),
            P(("groups", "attn", "expert")),
        ),
        out_specs=(P(("groups", "attn"), "expert"), P(("groups", "attn", "expert"), None)),
        check_vma=False,
    )
```

```python
import functools

import jax
import jax.numpy as jnp
from jax import lax
from jax.experimental import pallas as pl
from jax.experimental.pallas import tpu as pltpu
from jax.sharding import PartitionSpec as P


F32 = jnp.float32
BF16 = jnp.bfloat16
META = 8
VMEM_SPEC = pl.BlockSpec(memory_space=pltpu.VMEM)
SMEM_SPEC = pl.BlockSpec(memory_space=pltpu.SMEM)
HBM_SPEC = pl.BlockSpec(memory_space=pltpu.HBM)
SMALL = {"compiler_params": pltpu.CompilerParams(vmem_limit_bytes=2 << 20)}


def both_cores(home, swapped, i):
    return home[i].astype(F32) + swapped[i].astype(F32)


def far_kernel(home, swapped, three, four):
    rows = home.shape[1]
    four[...] = both_cores(home, swapped, 2).astype(BF16)
    for c in range(2):
        three[c * rows : (c + 1) * rows, :] = both_cores(home, swapped, c).astype(BF16)


def one_kernel(home, swapped, own, other):
    own[...] = both_cores(home, swapped, 0).astype(BF16)
    other[...] = both_cores(home, swapped, 1).astype(BF16)


def relay_kernel(home, swapped, three, four, own, other):
    rows = home.shape[1]
    came = three[...].astype(F32)
    own[...] = (both_cores(home, swapped, 2) + (came[0:rows] + four[...].astype(F32))).astype(BF16)
    other[...] = (both_cores(home, swapped, 3) + came[rows:]).astype(BF16)


def finish_kernel(home, swapped, a, b, c, d, out):
    came = (a[...].astype(F32) + b[...].astype(F32)) + (c[...].astype(F32) + d[...].astype(F32))
    out[...] = (both_cores(home, swapped, 3) + came).astype(BF16)


def in_hbm(value):
    return pltpu.with_memory_space_constraint(value, pltpu.HBM)


def in_vmem(value):
    return pltpu.with_memory_space_constraint(value, pltpu.VMEM)


def attention_kernel(lengths, query, cache_k, cache_v, out):
    heads, size = query.shape[1:]
    spots, groups, _ = cache_k.shape[1:]
    columns = spots * groups
    keys = cache_k[0].reshape(columns, size)
    values = cache_v[0].reshape(columns, size)
    scores = lax.dot_general(
        query[0], keys, (((1,), (1,)), ((), ())), preferred_element_type=F32
    ) * size ** (-0.5)
    place = lax.broadcasted_iota(jnp.int32, (heads, columns), 1)
    head = lax.broadcasted_iota(jnp.int32, (heads, columns), 0)
    live = (place % groups == head // (heads // groups)) & (
        place < lengths[pl.program_id(0)] * groups
    )
    masked = jnp.where(live, scores, -jnp.inf)
    weighted = jnp.exp(masked - jnp.max(masked, axis=1, keepdims=True))
    prob = (weighted / jnp.sum(weighted, axis=1, keepdims=True)).astype(BF16)
    out[0] = jnp.dot(prob, values, preferred_element_type=F32).astype(BF16)


def grouped_attention(query, cache_k, cache_v, lengths):
    count, heads, size = query.shape
    _, spots, groups, _ = cache_k.shape
    cache = pl.BlockSpec((1, spots, groups, size), lambda i: (i, 0, 0, 0))
    row = pl.BlockSpec((1, heads, size), lambda i: (i, 0, 0))
    out = pl.pallas_call(
        attention_kernel,
        grid=(count,),
        out_shape=jax.ShapeDtypeStruct((count, heads, size), BF16),
        in_specs=[SMEM_SPEC, row, cache, cache],
        out_specs=row,
        compiler_params=pltpu.CompilerParams(vmem_limit_bytes=12 << 20),
        cost_estimate=pl.CostEstimate(
            flops=10**9, bytes_accessed=3 * 10**6, transcendentals=4 * 10**5
        ),
        name="attention",
    )(lengths, in_hbm(query), in_hbm(cache_k), in_hbm(cache_v))
    return out.reshape(count, heads * size)


def shift(value, axis, step):
    count = lax.axis_size(axis)
    return lax.ppermute(value, axis, [(i, (i + step) % count) for i in range(count)])


def both_ways(value, places, cross=0):
    count = lax.axis_size("attn")
    pairs = [(i, (i + (-2 if i % 2 else 2) * places) % count ^ cross) for i in range(count)]
    return lax.ppermute(value, "attn", pairs)


def swap_cores(value):
    return lax.ppermute(value, "attn", [(i, i ^ 1) for i in range(lax.axis_size("attn"))])


def prepare_kernel(tokens, ids, gates, block, ids_v, gates_v, sems):
    rows = tokens.shape[0]
    copies = (
        pltpu.make_async_copy(tokens, block.at[0:rows], sems.at[0]),
        pltpu.make_async_copy(ids, ids_v, sems.at[1]),
        pltpu.make_async_copy(gates, gates_v, sems.at[2]),
    )
    for copy in copies:
        copy.start()
    block[rows:, 2 * rows :] = jnp.zeros((META, block.shape[1] - 2 * rows), BF16)
    for copy in copies[1:]:
        copy.wait()
    block[rows:, 0:rows] = ids_v[...].astype(F32).astype(BF16)
    block[rows:, rows : 2 * rows] = gates_v[...]
    copies[0].wait()


def bundle_kernel(*refs):
    out = refs[-1]
    height = refs[0].shape[0]
    for i, ref in enumerate(refs[:-1]):
        out[i * height : (i + 1) * height, :] = ref[...]


def expert_parts(j0, info, place, tok, wg, wu, onehot, out):
    n_blocks = place.shape[0]
    rows = tok.shape[0] // n_blocks
    n_dest = len(out)
    here_count, dest_rows, ff2 = out[0].shape
    ff = ff2 // 2
    capacity = n_dest * dest_rows
    row_id = lax.broadcasted_iota(jnp.int32, (capacity, rows), 0) + info[1 + n_blocks]
    row_id = jnp.where(row_id < capacity, row_id, row_id - capacity).astype(F32)

    def expert(j, carry):
        def select(i, carry):
            spot = place[info[1 + i], pl.ds(j0 + j, 1), :]
            at = pl.ds(pl.multiple_of(i * rows, rows), rows)
            onehot[:, at] = jnp.where(row_id == spot, 1.0, 0.0).astype(BF16)
            return carry

        lax.fori_loop(0, n_blocks, select, 0, unroll=2)
        mine = jnp.dot(onehot[...], tok[...], preferred_element_type=F32).astype(BF16)
        gate = jnp.dot(mine, wg[j0 + j], preferred_element_type=F32).astype(BF16)
        up = jnp.dot(mine, wu[j0 + j], preferred_element_type=F32).astype(BF16)
        for d in range(n_dest):
            out[d][j, :, 0:ff] = gate[d * dest_rows : (d + 1) * dest_rows]
            out[d][j, :, ff:] = up[d * dest_rows : (d + 1) * dest_rows]
        return carry

    lax.fori_loop(0, here_count, expert, 0)


def fetch_kernel(wg_hbm, wu_hbm, wg, wu, sems):
    copies = (
        pltpu.make_async_copy(wg_hbm, wg, sems.at[0]),
        pltpu.make_async_copy(wu_hbm, wu, sems.at[1]),
    )
    for copy in copies:
        copy.start()
    for copy in copies:
        copy.wait()


def pack_kernel(plan, local, n_dest, info, *refs):
    n_ops = 1 + max(op for op, _ in plan)
    ops = refs[:n_ops]
    wg, wu = refs[n_ops : n_ops + 2]
    out = refs[n_ops + 2 : n_ops + 2 + n_dest]
    route, tok, meta, onehot = refs[n_ops + 2 + n_dest :]
    n_blocks = len(plan)
    rows = tok.shape[0] // n_blocks
    capacity = n_dest * out[0].shape[1]

    for i, (op, r0) in enumerate(plan):
        at = pl.ds(pl.multiple_of(info[1 + i] * rows, rows), rows)
        low = r0 + rows
        tok[i * rows : (i + 1) * rows, :] = ops[op][r0:low, :]
        meta[0:8, at] = ops[op][low : low + META, 0:rows].astype(F32)
        meta[8:16, at] = ops[op][low : low + META, rows : 2 * rows].astype(F32)
    ids = meta[0:8, :]
    gates = meta[8:16, :]
    hits = [ids == (info[0] + j).astype(F32) for j in range(local)]
    stack = jnp.concatenate(
        [jnp.where(h, 1.0, 0.0) for h in hits] + [jnp.where(h, gates, 0.0) for h in hits], axis=0
    ).astype(BF16)
    one = lax.broadcasted_iota(jnp.int32, (8, 64), 0)
    two = lax.broadcasted_iota(jnp.int32, (8, 64), 1)
    pick = jnp.where(one == two // 8, 1.0, 0.0).astype(BF16)
    both = jnp.dot(pick, stack, preferred_element_type=F32)
    member = jnp.concatenate(
        [both[:, b * rows : (b + 1) * rows] for b in range(n_blocks)], axis=0
    )
    size = n_blocks * 8
    r = lax.broadcasted_iota(jnp.int32, (rows, rows), 0)
    c = lax.broadcasted_iota(jnp.int32, (rows, rows), 1)
    upper = jnp.where(r < c, 1.0, 0.0).astype(BF16)
    rr = lax.broadcasted_iota(jnp.int32, (size, size), 0)
    cc = lax.broadcasted_iota(jnp.int32, (size, size), 1)
    earlier = jnp.where((rr % 8 == cc % 8) & (cc // 8 < rr // 8), 1.0, 0.0).astype(BF16)
    member_b = member.astype(BF16)
    before = jnp.dot(earlier, member_b, preferred_element_type=F32).astype(BF16)
    place = jnp.dot(member_b, upper, preferred_element_type=F32) + jnp.dot(
        before, jnp.ones((rows, rows), BF16), preferred_element_type=F32
    )
    place = jnp.where((member > 0.5) & (place < capacity), place, -1.0)
    row = lax.broadcasted_iota(jnp.int32, (size, rows), 0)
    route[...] = jnp.where(row % 8 < local, place, member).reshape(n_blocks, 8, rows)

    expert_parts(0, info, route, tok, wg, wu, onehot, out)


def pack_more_kernel(j0, info, tok, route, wg, wu, *refs):
    *out, onehot = refs
    expert_parts(j0, info, route, tok, wg, wu, onehot, out)


def hidden_kernel(*refs):
    *terms, out = refs
    ways = 3
    row = 0
    for s in range(len(terms) // ways):
        a, b, c = (t[...].astype(F32) for t in terms[s * ways : (s + 1) * ways])
        total = a + (b + c)
        ff = total.shape[-1] // 2
        v = total[..., :ff]
        out[row : row + total.shape[0]] = (v / (1.0 + jnp.exp(-v)) * total[..., ff:]).astype(BF16)
        row += total.shape[0]


def mix_kernel(info, route, wd_hbm, mix, wd, sem):
    copy = pltpu.make_async_copy(wd_hbm, wd, sem)
    copy.start()
    n_blocks, _, rows = route.shape
    local = wd.shape[0]
    capacity = mix.shape[1] // local
    r = lax.broadcasted_iota(jnp.int32, (rows, rows), 0)
    c = lax.broadcasted_iota(jnp.int32, (rows, rows), 1)
    eye = jnp.where(r == c, 1.0, 0.0).astype(BF16)
    col_id = lax.broadcasted_iota(jnp.int32, (rows, capacity), 1).astype(F32)

    def block(i, carry):
        at = pl.ds(pl.multiple_of(i * rows, rows), rows)
        rt = lax.dot_general(
            eye, route[info[i]].astype(BF16), (((1,), (1,)), ((), ())), preferred_element_type=F32
        )
        for j in range(local):
            mix[at, j * capacity : (j + 1) * capacity] = jnp.where(
                col_id == rt[:, j : j + 1], rt[:, local + j : local + j + 1], 0.0
            ).astype(BF16)
        return carry

    lax.fori_loop(0, n_blocks, block, 0, unroll=2)
    copy.wait()


def mix_rows(quarter, mix, res, ref):
    n_dest, rows, feat = ref.shape
    group = 2

    def some(g, carry):
        at = (quarter * n_dest + g * group) * rows
        at = pl.ds(pl.multiple_of(at, group * rows), group * rows)
        got = jnp.dot(mix[at, :], res[...], preferred_element_type=F32).astype(BF16)
        ref[pl.ds(g * group, group)] = got.reshape(group, rows, feat)
        return carry

    lax.fori_loop(0, n_dest // group, some, 0)


def down_kernel(plan, info, *refs):
    n_ops = len(plan)
    ops = refs[:n_ops]
    wd, mix, away, res, hid = refs[n_ops:]
    local = wd.shape[0]
    capacity = hid.shape[1]
    for op, (j0, slot) in zip(ops, plan):
        at = pl.multiple_of(info[slot], op.shape[1])
        for j in range(op.shape[0]):
            hid[j0 + j, pl.ds(at, op.shape[1]), :] = op[j]

    def expert(j, carry):
        res[pl.ds(pl.multiple_of(j * capacity, capacity), capacity), :] = jnp.dot(
            hid[j], wd[j], preferred_element_type=F32
        ).astype(BF16)
        return carry

    lax.fori_loop(0, local, expert, 0)
    mix_rows(0, mix, res, away)


def second_kernel(mix, res, home, away):
    mix_rows(1, mix, res, away)
    mix_rows(2, mix, res, home)


def third_kernel(mix, res, home):
    mix_rows(3, mix, res, home)


def scatter_sum(pieces, axis):
    count = len(pieces[0])
    half = count // 2
    legs = {}
    for way in (1, -1):
        for s in range(2):
            start = half if (way == 1) == (s == 0) else half - 1
            legs[(way, s)] = [start, pieces[s][way * start % count]]
    for hop in range(half, 0, -1):
        for way in (1, -1):
            for s in range(2):
                leg = legs[(way, s)]
                if leg[0] != hop:
                    continue
                got = shift(leg[1], axis, way)
                if hop > 1:
                    mine = pieces[s][way * (hop - 1) % count]
                    got = (got.astype(F32) + mine.astype(F32)).astype(BF16)
                legs[(way, s)] = [hop - 1, got]
    return [(pieces[s][0], legs[(1, s)][1], legs[(-1, s)][1]) for s in range(2)]


def step(tokens, expert_ids, gate_weight, w_gate, w_up, w_down, query, cache_k, cache_v, lengths):
    rows, feat = tokens.shape
    local, _, ff = w_gate.shape
    attn_count = lax.axis_size("attn")
    n_expert = lax.axis_size("expert")
    chips = attn_count // 2
    top = expert_ids.shape[1]
    capacity = rows * top // local
    me = lax.axis_index("attn")
    col = lax.axis_index("expert")
    y = me // 2
    core = me % 2
    far = chips // 2
    dest_rows = capacity // n_expert

    x_at = [lax.rem(col + k, n_expert) for k in range(n_expert)]
    ahead = jnp.where(core == 0, 1, -1)

    def token_block(places, flip):
        return 2 * lax.rem(y + places * ahead + chips, chips) + (core ^ flip)

    order = [(0, 0), (0, 1)]
    order += [(-k, flip) for k in (1, 2, 3) for flip in (0, 1)] + [(far, 0)]
    order += [(k, flip) for k in (1, 2, 3) for flip in (1, 0)] + [(far, 1)]
    pack_info = [local * me] + [token_block(*at) for at in order]
    onward = [(3, 0), (3, 1), (far, 0), (0, 0)], [(1, 0), (1, 1), (2, 0), (2, 1)]
    for_other = [[token_block(-k, 1 - flip) for k, flip in part] for part in onward]
    for_own = [[token_block(k, flip) for k, flip in part] for part in onward]
    mix_info = for_other[0] + for_other[1] + for_own[0] + for_own[1]
    row_at = [x * dest_rows for x in x_at]
    pack_info.append(col * dest_rows)
    pack_info = jnp.stack(pack_info).astype(jnp.int32)
    mix_info = jnp.stack(mix_info).astype(jnp.int32)
    row_at = jnp.stack(row_at).astype(jnp.int32)
    tokens, pack_info, mix_info, row_at = lax.optimization_barrier(
        (tokens, pack_info, mix_info, row_at)
    )

    height = rows + META
    block = pl.pallas_call(
        prepare_kernel,
        out_shape=jax.ShapeDtypeStruct((height, feat), BF16),
        in_specs=[HBM_SPEC] * 3,
        out_specs=VMEM_SPEC,
        scratch_shapes=[
            pltpu.VMEM((top, rows), jnp.int32),
            pltpu.VMEM((top, rows), BF16),
            pltpu.SemaphoreType.DMA((3,)),
        ],
        name="prepare",
        **SMALL,
    )(in_hbm(tokens), in_hbm(expert_ids.T), in_hbm(gate_weight.T))
    attn_out = grouped_attention(query, cache_k, cache_v, lengths)

    def pass_on(value, places, cross=0):
        return both_ways(value, places, cross)

    def paired(one, two):
        return pl.pallas_call(
            bundle_kernel,
            out_shape=jax.ShapeDtypeStruct((2 * height, feat), BF16),
            in_specs=[VMEM_SPEC] * 2,
            out_specs=VMEM_SPEC,
            name="pair",
            **SMALL,
        )(in_vmem(one), in_vmem(two))

    two_own = pass_on(block, 2)
    other = swap_cores(block)
    two_other = pass_on(other, 2)
    one = pass_on(paired(block, other), 1)
    four = pass_on(two_own, 2)
    two = paired(two_own, two_other)
    three = pass_on(two, 1)
    operands = [block, other, one, two_own, two_other, three, four]
    operands += [swap_cores(one), swap_cores(two), swap_cores(three), swap_cores(four)]
    plan = [(0, 0), (1, 0), (2, 0), (2, height), (3, 0), (4, 0), (5, 0), (5, height), (6, 0)]
    plan += [(i, r) for i in (7, 8, 9) for r in (0, height)] + [(10, 0)]

    cut = local // 2
    pack_scratch = [
        pltpu.VMEM((capacity, attn_count * rows), BF16),
    ]
    wg, wu = pl.pallas_call(
        fetch_kernel,
        out_shape=tuple(jax.ShapeDtypeStruct(w.shape, BF16) for w in (w_gate, w_up)),
        in_specs=[HBM_SPEC] * 2,
        out_specs=(VMEM_SPEC,) * 2,
        scratch_shapes=[pltpu.SemaphoreType.DMA((2,))],
        name="weights",
        **SMALL,
    )(in_hbm(w_gate), in_hbm(w_up))
    part_shapes = (jax.ShapeDtypeStruct((cut, dest_rows, 2 * ff), BF16),) * n_expert
    pack_cost = pl.CostEstimate(flops=2 * 10**9, bytes_accessed=6 * 10**6, transcendentals=0)
    *parts_a, route, tok = pl.pallas_call(
        functools.partial(pack_kernel, plan, local, n_expert),
        out_shape=(
            *part_shapes,
            jax.ShapeDtypeStruct((attn_count, 8, rows), F32),
            jax.ShapeDtypeStruct((attn_count * rows, feat), BF16),
        ),
        in_specs=[SMEM_SPEC] + [VMEM_SPEC] * (len(operands) + 2),
        out_specs=(VMEM_SPEC,) * (n_expert + 2),
        scratch_shapes=[
            pltpu.VMEM((2 * META, attn_count * rows), F32),
            *pack_scratch,
        ],
        compiler_params=pltpu.CompilerParams(vmem_limit_bytes=7 << 20),
        cost_estimate=pack_cost,
        name="pack",
    )(pack_info, *map(in_vmem, (*operands, wg, wu)))
    parts_b = pl.pallas_call(
        functools.partial(pack_more_kernel, cut),
        out_shape=part_shapes,
        in_specs=[SMEM_SPEC] + [VMEM_SPEC] * 4,
        out_specs=(VMEM_SPEC,) * n_expert,
        scratch_shapes=pack_scratch,
        compiler_params=pltpu.CompilerParams(vmem_limit_bytes=7 << 20),
        cost_estimate=pack_cost,
        name="pack_more",
    )(pack_info, *map(in_vmem, (tok, route, wg, wu)))

    terms = sum(scatter_sum([parts_a, parts_b], "expert"), ())
    hidden = pl.pallas_call(
        hidden_kernel,
        out_shape=jax.ShapeDtypeStruct((local, dest_rows, ff), BF16),
        in_specs=[VMEM_SPEC] * len(terms),
        out_specs=VMEM_SPEC,
        name="hidden",
        **SMALL,
    )(*map(in_vmem, terms))

    r2, l2 = shift(hidden, "expert", 2), shift(hidden, "expert", -2)
    r1, l1 = shift(hidden, "expert", 1), shift(hidden, "expert", -1)
    r4, l4 = shift(r2[:cut], "expert", 2), shift(l2[cut:], "expert", -2)
    r3, l3 = shift(r2, "expert", 1), shift(l2, "expert", -1)
    pieces_in = [hidden, r1, l1, r2, l2, r3, l3, r4, l4]
    where = [(0, k % n_expert) for k in (0, -1, 1, -2, 2, -3, 3, -4)] + [(cut, n_expert // 2)]

    mix, wd = pl.pallas_call(
        mix_kernel,
        out_shape=(
            jax.ShapeDtypeStruct((attn_count * rows, local * capacity), BF16),
            jax.ShapeDtypeStruct(w_down.shape, BF16),
        ),
        in_specs=[SMEM_SPEC, VMEM_SPEC, HBM_SPEC],
        out_specs=(VMEM_SPEC,) * 2,
        scratch_shapes=[pltpu.SemaphoreType.DMA],
        name="mix",
        **SMALL,
    )(mix_info, in_vmem(route), in_hbm(w_down))
    quarter = jax.ShapeDtypeStruct((attn_count // 4, rows, feat), BF16)
    away_far, res = pl.pallas_call(
        functools.partial(down_kernel, where),
        out_shape=(quarter, jax.ShapeDtypeStruct((local * capacity, feat), BF16)),
        in_specs=[SMEM_SPEC] + [VMEM_SPEC] * (len(pieces_in) + 2),
        out_specs=(VMEM_SPEC, VMEM_SPEC),
        scratch_shapes=[pltpu.VMEM((local, capacity, ff), BF16)],
        compiler_params=pltpu.CompilerParams(vmem_limit_bytes=4 << 20),
        cost_estimate=pl.CostEstimate(flops=2 * 10**9, bytes_accessed=6 * 10**6, transcendentals=0),
        name="down",
    )(row_at, *map(in_vmem, pieces_in), in_vmem(wd), in_vmem(mix))

    def small_call(kernel, shapes, *operands):
        out = pl.pallas_call(
            kernel,
            out_shape=shapes,
            in_specs=[VMEM_SPEC] * len(operands),
            out_specs=(VMEM_SPEC,) * len(shapes),
            **SMALL,
        )(*map(in_vmem, operands))
        return out if len(shapes) > 1 else out[0]

    once = jax.ShapeDtypeStruct((rows, feat), BF16)
    twice = jax.ShapeDtypeStruct((2 * rows, feat), BF16)
    came_far = swap_cores(away_far)
    home_far, away_near = small_call(second_kernel, (quarter, quarter), mix, res)
    came_near = swap_cores(away_near)
    three, four = small_call(far_kernel, (twice, once), home_far, came_far)
    four, three = pass_on(four, 2), pass_on(three, 1)
    home_near = small_call(third_kernel, (quarter,), mix, res)
    own, other = small_call(one_kernel, (once, once), home_near, came_near)
    last = [pass_on(own, 1), pass_on(other, 1, 1)]
    own, other = small_call(relay_kernel, (once, once), home_near, came_near, three, four)
    last += [pass_on(own, 2), pass_on(other, 2, 1)]
    moe_out = small_call(finish_kernel, (once,), home_far, came_far, *last)
    return (moe_out, attn_out)


def solution(mesh):
    return jax.shard_map(
        step,
        mesh=mesh,
        in_specs=(
            P(("groups", "attn"), "expert"),
            P(("groups", "attn"), None),
            P(("groups", "attn"), None),
            P("attn", "expert", None),
            P("attn", "expert", None),
            P("attn", None, "expert"),
            P(("groups", "attn", "expert"), None, None),
            P(("groups", "attn", "expert"), None, None, None),
            P(("groups", "attn", "expert"), None, None, None),
            P(("groups", "attn", "expert")),
        ),
        out_specs=(P(("groups", "attn"), "expert"), P(("groups", "attn", "expert"), None)),
        check_vma=False,
    )
```

```python
import functools

import jax
import jax.numpy as jnp
from jax import lax
from jax.experimental import pallas as pl
from jax.experimental.pallas import tpu as pltpu
from jax.sharding import PartitionSpec as P


F32 = jnp.float32
BF16 = jnp.bfloat16
META = 8
VMEM_SPEC = pl.BlockSpec(memory_space=pltpu.VMEM)
SMEM_SPEC = pl.BlockSpec(memory_space=pltpu.SMEM)
HBM_SPEC = pl.BlockSpec(memory_space=pltpu.HBM)
SMALL = {"compiler_params": pltpu.CompilerParams(vmem_limit_bytes=2 << 20)}


def both_cores(home, swapped, i):
    return home[i].astype(F32) + swapped[i].astype(F32)


def far_kernel(home, swapped, three, four):
    rows = home.shape[1]
    four[...] = both_cores(home, swapped, 2).astype(BF16)
    for c in range(2):
        three[c * rows : (c + 1) * rows, :] = both_cores(home, swapped, c).astype(BF16)


def one_kernel(home, swapped, own, other):
    own[...] = both_cores(home, swapped, 0).astype(BF16)
    other[...] = both_cores(home, swapped, 1).astype(BF16)


def relay_kernel(home, swapped, three, four, own, other):
    rows = home.shape[1]
    came = three[...].astype(F32)
    own[...] = (both_cores(home, swapped, 2) + (came[0:rows] + four[...].astype(F32))).astype(BF16)
    other[...] = (both_cores(home, swapped, 3) + came[rows:]).astype(BF16)


def finish_kernel(home, swapped, a, b, c, d, out):
    came = (a[...].astype(F32) + b[...].astype(F32)) + (c[...].astype(F32) + d[...].astype(F32))
    out[...] = (both_cores(home, swapped, 3) + came).astype(BF16)


def in_hbm(value):
    return pltpu.with_memory_space_constraint(value, pltpu.HBM)


def in_vmem(value):
    return pltpu.with_memory_space_constraint(value, pltpu.VMEM)


def attention_kernel(lengths, query, cache_k, cache_v, out):
    heads, size = query.shape[1:]
    spots, groups, _ = cache_k.shape[1:]
    columns = spots * groups
    keys = cache_k[0].reshape(columns, size)
    values = cache_v[0].reshape(columns, size)
    scores = lax.dot_general(
        query[0], keys, (((1,), (1,)), ((), ())), preferred_element_type=F32
    ) * size ** (-0.5)
    place = lax.broadcasted_iota(jnp.int32, (heads, columns), 1)
    head = lax.broadcasted_iota(jnp.int32, (heads, columns), 0)
    live = (place % groups == head // (heads // groups)) & (
        place < lengths[pl.program_id(0)] * groups
    )
    masked = jnp.where(live, scores, -jnp.inf)
    weighted = jnp.exp(masked - jnp.max(masked, axis=1, keepdims=True))
    prob = (weighted / jnp.sum(weighted, axis=1, keepdims=True)).astype(BF16)
    out[0] = jnp.dot(prob, values, preferred_element_type=F32).astype(BF16)


def grouped_attention(query, cache_k, cache_v, lengths):
    count, heads, size = query.shape
    _, spots, groups, _ = cache_k.shape
    cache = pl.BlockSpec((1, spots, groups, size), lambda i: (i, 0, 0, 0))
    row = pl.BlockSpec((1, heads, size), lambda i: (i, 0, 0))
    out = pl.pallas_call(
        attention_kernel,
        grid=(count,),
        out_shape=jax.ShapeDtypeStruct((count, heads, size), BF16),
        in_specs=[SMEM_SPEC, row, cache, cache],
        out_specs=row,
        compiler_params=pltpu.CompilerParams(vmem_limit_bytes=12 << 20),
        cost_estimate=pl.CostEstimate(
            flops=10**9, bytes_accessed=3 * 10**6, transcendentals=4 * 10**5
        ),
        name="attention",
    )(lengths, in_hbm(query), in_hbm(cache_k), in_hbm(cache_v))
    return out.reshape(count, heads * size)


def shift(value, axis, step):
    count = lax.axis_size(axis)
    return lax.ppermute(value, axis, [(i, (i + step) % count) for i in range(count)])


def both_ways(value, places, cross=0):
    count = lax.axis_size("attn")
    pairs = [(i, (i + (-2 if i % 2 else 2) * places) % count ^ cross) for i in range(count)]
    return lax.ppermute(value, "attn", pairs)


def swap_cores(value):
    return lax.ppermute(value, "attn", [(i, i ^ 1) for i in range(lax.axis_size("attn"))])


def prepare_kernel(tokens, ids, gates, block, ids_v, gates_v, sems):
    rows = tokens.shape[0]
    copies = (
        pltpu.make_async_copy(tokens, block.at[0:rows], sems.at[0]),
        pltpu.make_async_copy(ids, ids_v, sems.at[1]),
        pltpu.make_async_copy(gates, gates_v, sems.at[2]),
    )
    for copy in copies:
        copy.start()
    block[rows:, 2 * rows :] = jnp.zeros((META, block.shape[1] - 2 * rows), BF16)
    for copy in copies[1:]:
        copy.wait()
    block[rows:, 0:rows] = ids_v[...].astype(F32).astype(BF16)
    block[rows:, rows : 2 * rows] = gates_v[...]
    copies[0].wait()


def bundle_kernel(*refs):
    out = refs[-1]
    height = refs[0].shape[0]
    for i, ref in enumerate(refs[:-1]):
        out[i * height : (i + 1) * height, :] = ref[...]


def expert_parts(j0, info, place, tok, wg, wu, onehot, out):
    n_blocks = place.shape[0]
    rows = tok.shape[0] // n_blocks
    n_dest = len(out)
    here_count, dest_rows, ff2 = out[0].shape
    ff = ff2 // 2
    capacity = n_dest * dest_rows
    row_id = lax.broadcasted_iota(jnp.int32, (capacity, rows), 0) + info[1 + n_blocks]
    row_id = jnp.where(row_id < capacity, row_id, row_id - capacity).astype(F32)

    def expert(j, carry):
        for i in range(n_blocks):
            spot = place[info[1 + i], pl.ds(j0 + j, 1), :]
            onehot[:, i * rows : (i + 1) * rows] = jnp.where(row_id == spot, 1.0, 0.0).astype(BF16)
        mine = jnp.dot(onehot[...], tok[...], preferred_element_type=F32).astype(BF16)
        gate = jnp.dot(mine, wg[j0 + j], preferred_element_type=F32).astype(BF16)
        up = jnp.dot(mine, wu[j0 + j], preferred_element_type=F32).astype(BF16)
        for d in range(n_dest):
            out[d][j, :, 0:ff] = gate[d * dest_rows : (d + 1) * dest_rows]
            out[d][j, :, ff:] = up[d * dest_rows : (d + 1) * dest_rows]
        return carry

    lax.fori_loop(0, here_count, expert, 0)


def fetch_kernel(wg_hbm, wu_hbm, wg, wu, sems):
    copies = (
        pltpu.make_async_copy(wg_hbm, wg, sems.at[0]),
        pltpu.make_async_copy(wu_hbm, wu, sems.at[1]),
    )
    for copy in copies:
        copy.start()
    for copy in copies:
        copy.wait()


def pack_kernel(plan, local, n_dest, info, *refs):
    n_ops = 1 + max(op for op, _ in plan)
    ops = refs[:n_ops]
    wg, wu = refs[n_ops : n_ops + 2]
    out = refs[n_ops + 2 : n_ops + 2 + n_dest]
    route, tok, meta, onehot = refs[n_ops + 2 + n_dest :]
    n_blocks = len(plan)
    rows = tok.shape[0] // n_blocks
    capacity = n_dest * out[0].shape[1]

    for i, (op, r0) in enumerate(plan):
        at = pl.ds(pl.multiple_of(info[1 + i] * rows, rows), rows)
        low = r0 + rows
        tok[i * rows : (i + 1) * rows, :] = ops[op][r0:low, :]
        meta[0:8, at] = ops[op][low : low + META, 0:rows].astype(F32)
        meta[8:16, at] = ops[op][low : low + META, rows : 2 * rows].astype(F32)
    ids = meta[0:8, :]
    gates = meta[8:16, :]
    hits = [ids == (info[0] + j).astype(F32) for j in range(local)]
    stack = jnp.concatenate(
        [jnp.where(h, 1.0, 0.0) for h in hits] + [jnp.where(h, gates, 0.0) for h in hits], axis=0
    ).astype(BF16)
    one = lax.broadcasted_iota(jnp.int32, (8, 64), 0)
    two = lax.broadcasted_iota(jnp.int32, (8, 64), 1)
    pick = jnp.where(one == two // 8, 1.0, 0.0).astype(BF16)
    both = jnp.dot(pick, stack, preferred_element_type=F32)
    member = jnp.concatenate(
        [both[:, b * rows : (b + 1) * rows] for b in range(n_blocks)], axis=0
    )
    size = n_blocks * 8
    r = lax.broadcasted_iota(jnp.int32, (rows, rows), 0)
    c = lax.broadcasted_iota(jnp.int32, (rows, rows), 1)
    upper = jnp.where(r < c, 1.0, 0.0).astype(BF16)
    rr = lax.broadcasted_iota(jnp.int32, (size, size), 0)
    cc = lax.broadcasted_iota(jnp.int32, (size, size), 1)
    earlier = jnp.where((rr % 8 == cc % 8) & (cc // 8 < rr // 8), 1.0, 0.0).astype(BF16)
    member_b = member.astype(BF16)
    before = jnp.dot(earlier, member_b, preferred_element_type=F32).astype(BF16)
    place = jnp.dot(member_b, upper, preferred_element_type=F32) + jnp.dot(
        before, jnp.ones((rows, rows), BF16), preferred_element_type=F32
    )
    place = jnp.where((member > 0.5) & (place < capacity), place, -1.0)
    row = lax.broadcasted_iota(jnp.int32, (size, rows), 0)
    route[...] = jnp.where(row % 8 < local, place, member).reshape(n_blocks, 8, rows)

    expert_parts(0, info, route, tok, wg, wu, onehot, out)


def pack_more_kernel(j0, info, tok, route, wg, wu, *refs):
    *out, onehot = refs
    expert_parts(j0, info, route, tok, wg, wu, onehot, out)


def hidden_kernel(*refs):
    *terms, out = refs
    ways = 3
    row = 0
    for s in range(len(terms) // ways):
        a, b, c = (t[...].astype(F32) for t in terms[s * ways : (s + 1) * ways])
        total = a + (b + c)
        ff = total.shape[-1] // 2
        v = total[..., :ff]
        out[row : row + total.shape[0]] = (v / (1.0 + jnp.exp(-v)) * total[..., ff:]).astype(BF16)
        row += total.shape[0]


def mix_kernel(info, route, wd_hbm, mix, wd, sem):
    copy = pltpu.make_async_copy(wd_hbm, wd, sem)
    copy.start()
    n_blocks, _, rows = route.shape
    local = wd.shape[0]
    capacity = mix.shape[1] // local
    r = lax.broadcasted_iota(jnp.int32, (rows, rows), 0)
    c = lax.broadcasted_iota(jnp.int32, (rows, rows), 1)
    eye = jnp.where(r == c, 1.0, 0.0).astype(BF16)
    col_id = lax.broadcasted_iota(jnp.int32, (rows, capacity), 1).astype(F32)

    def block(i, carry):
        at = pl.ds(pl.multiple_of(i * rows, rows), rows)
        rt = lax.dot_general(
            eye, route[info[i]].astype(BF16), (((1,), (1,)), ((), ())), preferred_element_type=F32
        )
        for j in range(local):
            mix[at, j * capacity : (j + 1) * capacity] = jnp.where(
                col_id == rt[:, j : j + 1], rt[:, local + j : local + j + 1], 0.0
            ).astype(BF16)
        return carry

    lax.fori_loop(0, n_blocks, block, 0, unroll=2)
    copy.wait()


def mix_rows(quarter, mix, res, ref):
    n_dest, rows, feat = ref.shape
    group = 2

    def some(g, carry):
        at = (quarter * n_dest + g * group) * rows
        at = pl.ds(pl.multiple_of(at, group * rows), group * rows)
        got = jnp.dot(mix[at, :], res[...], preferred_element_type=F32).astype(BF16)
        ref[pl.ds(g * group, group)] = got.reshape(group, rows, feat)
        return carry

    lax.fori_loop(0, n_dest // group, some, 0)


def down_kernel(plan, info, *refs):
    n_ops = len(plan)
    ops = refs[:n_ops]
    wd, mix, away, res, hid = refs[n_ops:]
    local = wd.shape[0]
    capacity = hid.shape[1]
    for op, (j0, slot) in zip(ops, plan):
        at = pl.multiple_of(info[slot], op.shape[1])
        for j in range(op.shape[0]):
            hid[j0 + j, pl.ds(at, op.shape[1]), :] = op[j]

    def expert(j, carry):
        res[pl.ds(pl.multiple_of(j * capacity, capacity), capacity), :] = jnp.dot(
            hid[j], wd[j], preferred_element_type=F32
        ).astype(BF16)
        return carry

    lax.fori_loop(0, local, expert, 0)
    mix_rows(0, mix, res, away)


def second_kernel(mix, res, home, away):
    mix_rows(1, mix, res, away)
    mix_rows(2, mix, res, home)


def third_kernel(mix, res, home):
    mix_rows(3, mix, res, home)


def scatter_sum(pieces, axis):
    count = len(pieces[0])
    half = count // 2
    legs = {}
    for way in (1, -1):
        for s in range(2):
            start = half if (way == 1) == (s == 0) else half - 1
            legs[(way, s)] = [start, pieces[s][way * start % count]]
    for hop in range(half, 0, -1):
        for way in (1, -1):
            for s in range(2):
                leg = legs[(way, s)]
                if leg[0] != hop:
                    continue
                got = shift(leg[1], axis, way)
                if hop > 1:
                    mine = pieces[s][way * (hop - 1) % count]
                    got = (got.astype(F32) + mine.astype(F32)).astype(BF16)
                legs[(way, s)] = [hop - 1, got]
    return [(pieces[s][0], legs[(1, s)][1], legs[(-1, s)][1]) for s in range(2)]


def step(tokens, expert_ids, gate_weight, w_gate, w_up, w_down, query, cache_k, cache_v, lengths):
    rows, feat = tokens.shape
    local, _, ff = w_gate.shape
    attn_count = lax.axis_size("attn")
    n_expert = lax.axis_size("expert")
    chips = attn_count // 2
    top = expert_ids.shape[1]
    capacity = rows * top // local
    me = lax.axis_index("attn")
    col = lax.axis_index("expert")
    y = me // 2
    core = me % 2
    far = chips // 2
    dest_rows = capacity // n_expert

    x_at = [lax.rem(col + k, n_expert) for k in range(n_expert)]
    ahead = jnp.where(core == 0, 1, -1)

    def token_block(places, flip):
        return 2 * lax.rem(y + places * ahead + chips, chips) + (core ^ flip)

    order = [(0, 0), (0, 1)]
    order += [(-k, flip) for k in (1, 2, 3) for flip in (0, 1)] + [(far, 0)]
    order += [(k, flip) for k in (1, 2, 3) for flip in (1, 0)] + [(far, 1)]
    pack_info = [local * me] + [token_block(*at) for at in order]
    onward = [(3, 0), (3, 1), (far, 0), (0, 0)], [(1, 0), (1, 1), (2, 0), (2, 1)]
    for_other = [[token_block(-k, 1 - flip) for k, flip in part] for part in onward]
    for_own = [[token_block(k, flip) for k, flip in part] for part in onward]
    mix_info = for_other[0] + for_other[1] + for_own[0] + for_own[1]
    row_at = [x * dest_rows for x in x_at]
    pack_info.append(col * dest_rows)
    pack_info = jnp.stack(pack_info).astype(jnp.int32)
    mix_info = jnp.stack(mix_info).astype(jnp.int32)
    row_at = jnp.stack(row_at).astype(jnp.int32)
    tokens, pack_info, mix_info, row_at = lax.optimization_barrier(
        (tokens, pack_info, mix_info, row_at)
    )

    height = rows + META
    block = pl.pallas_call(
        prepare_kernel,
        out_shape=jax.ShapeDtypeStruct((height, feat), BF16),
        in_specs=[HBM_SPEC] * 3,
        out_specs=VMEM_SPEC,
        scratch_shapes=[
            pltpu.VMEM((top, rows), jnp.int32),
            pltpu.VMEM((top, rows), BF16),
            pltpu.SemaphoreType.DMA((3,)),
        ],
        name="prepare",
        **SMALL,
    )(in_hbm(tokens), in_hbm(expert_ids.T), in_hbm(gate_weight.T))
    attn_out = grouped_attention(query, cache_k, cache_v, lengths)

    def pass_on(value, places, cross=0):
        return both_ways(value, places, cross)

    def paired(one, two):
        return pl.pallas_call(
            bundle_kernel,
            out_shape=jax.ShapeDtypeStruct((2 * height, feat), BF16),
            in_specs=[VMEM_SPEC] * 2,
            out_specs=VMEM_SPEC,
            name="pair",
            **SMALL,
        )(in_vmem(one), in_vmem(two))

    two_own = pass_on(block, 2)
    other = swap_cores(block)
    two_other = pass_on(other, 2)
    one = pass_on(paired(block, other), 1)
    four = pass_on(two_own, 2)
    two = paired(two_own, two_other)
    three = pass_on(two, 1)
    operands = [block, other, one, two_own, two_other, three, four]
    operands += [swap_cores(one), swap_cores(two), swap_cores(three), swap_cores(four)]
    plan = [(0, 0), (1, 0), (2, 0), (2, height), (3, 0), (4, 0), (5, 0), (5, height), (6, 0)]
    plan += [(i, r) for i in (7, 8, 9) for r in (0, height)] + [(10, 0)]

    cut = local // 2
    pack_scratch = [
        pltpu.VMEM((capacity, attn_count * rows), BF16),
    ]
    wg, wu = pl.pallas_call(
        fetch_kernel,
        out_shape=tuple(jax.ShapeDtypeStruct(w.shape, BF16) for w in (w_gate, w_up)),
        in_specs=[HBM_SPEC] * 2,
        out_specs=(VMEM_SPEC,) * 2,
        scratch_shapes=[pltpu.SemaphoreType.DMA((2,))],
        name="weights",
        **SMALL,
    )(in_hbm(w_gate), in_hbm(w_up))
    part_shapes = (jax.ShapeDtypeStruct((cut, dest_rows, 2 * ff), BF16),) * n_expert
    pack_cost = pl.CostEstimate(flops=2 * 10**9, bytes_accessed=6 * 10**6, transcendentals=0)
    *parts_a, route, tok = pl.pallas_call(
        functools.partial(pack_kernel, plan, local, n_expert),
        out_shape=(
            *part_shapes,
            jax.ShapeDtypeStruct((attn_count, 8, rows), F32),
            jax.ShapeDtypeStruct((attn_count * rows, feat), BF16),
        ),
        in_specs=[SMEM_SPEC] + [VMEM_SPEC] * (len(operands) + 2),
        out_specs=(VMEM_SPEC,) * (n_expert + 2),
        scratch_shapes=[
            pltpu.VMEM((2 * META, attn_count * rows), F32),
            *pack_scratch,
        ],
        compiler_params=pltpu.CompilerParams(vmem_limit_bytes=7 << 20),
        cost_estimate=pack_cost,
        name="pack",
    )(pack_info, *map(in_vmem, (*operands, wg, wu)))
    parts_b = pl.pallas_call(
        functools.partial(pack_more_kernel, cut),
        out_shape=part_shapes,
        in_specs=[SMEM_SPEC] + [VMEM_SPEC] * 4,
        out_specs=(VMEM_SPEC,) * n_expert,
        scratch_shapes=pack_scratch,
        compiler_params=pltpu.CompilerParams(vmem_limit_bytes=7 << 20),
        cost_estimate=pack_cost,
        name="pack_more",
    )(pack_info, *map(in_vmem, (tok, route, wg, wu)))

    terms = sum(scatter_sum([parts_a, parts_b], "expert"), ())
    hidden = pl.pallas_call(
        hidden_kernel,
        out_shape=jax.ShapeDtypeStruct((local, dest_rows, ff), BF16),
        in_specs=[VMEM_SPEC] * len(terms),
        out_specs=VMEM_SPEC,
        name="hidden",
        **SMALL,
    )(*map(in_vmem, terms))

    r2, l2 = shift(hidden, "expert", 2), shift(hidden, "expert", -2)
    r1, l1 = shift(hidden, "expert", 1), shift(hidden, "expert", -1)
    r4, l4 = shift(r2[:cut], "expert", 2), shift(l2[cut:], "expert", -2)
    r3, l3 = shift(r2, "expert", 1), shift(l2, "expert", -1)
    pieces_in = [hidden, r1, l1, r2, l2, r3, l3, r4, l4]
    where = [(0, k % n_expert) for k in (0, -1, 1, -2, 2, -3, 3, -4)] + [(cut, n_expert // 2)]

    mix, wd = pl.pallas_call(
        mix_kernel,
        out_shape=(
            jax.ShapeDtypeStruct((attn_count * rows, local * capacity), BF16),
            jax.ShapeDtypeStruct(w_down.shape, BF16),
        ),
        in_specs=[SMEM_SPEC, VMEM_SPEC, HBM_SPEC],
        out_specs=(VMEM_SPEC,) * 2,
        scratch_shapes=[pltpu.SemaphoreType.DMA],
        name="mix",
        **SMALL,
    )(mix_info, in_vmem(route), in_hbm(w_down))
    quarter = jax.ShapeDtypeStruct((attn_count // 4, rows, feat), BF16)
    away_far, res = pl.pallas_call(
        functools.partial(down_kernel, where),
        out_shape=(quarter, jax.ShapeDtypeStruct((local * capacity, feat), BF16)),
        in_specs=[SMEM_SPEC] + [VMEM_SPEC] * (len(pieces_in) + 2),
        out_specs=(VMEM_SPEC, VMEM_SPEC),
        scratch_shapes=[pltpu.VMEM((local, capacity, ff), BF16)],
        compiler_params=pltpu.CompilerParams(vmem_limit_bytes=4 << 20),
        cost_estimate=pl.CostEstimate(flops=2 * 10**9, bytes_accessed=6 * 10**6, transcendentals=0),
        name="down",
    )(row_at, *map(in_vmem, pieces_in), in_vmem(wd), in_vmem(mix))

    def small_call(kernel, shapes, *operands):
        out = pl.pallas_call(
            kernel,
            out_shape=shapes,
            in_specs=[VMEM_SPEC] * len(operands),
            out_specs=(VMEM_SPEC,) * len(shapes),
            **SMALL,
        )(*map(in_vmem, operands))
        return out if len(shapes) > 1 else out[0]

    once = jax.ShapeDtypeStruct((rows, feat), BF16)
    twice = jax.ShapeDtypeStruct((2 * rows, feat), BF16)
    came_far = swap_cores(away_far)
    home_far, away_near = small_call(second_kernel, (quarter, quarter), mix, res)
    came_near = swap_cores(away_near)
    three, four = small_call(far_kernel, (twice, once), home_far, came_far)
    four, three = pass_on(four, 2), pass_on(three, 1)
    home_near = small_call(third_kernel, (quarter,), mix, res)
    own, other = small_call(one_kernel, (once, once), home_near, came_near)
    last = [pass_on(own, 1), pass_on(other, 1, 1)]
    own, other = small_call(relay_kernel, (once, once), home_near, came_near, three, four)
    last += [pass_on(own, 2), pass_on(other, 2, 1)]
    moe_out = small_call(finish_kernel, (once,), home_far, came_far, *last)
    return (moe_out, attn_out)


def solution(mesh):
    return jax.shard_map(
        step,
        mesh=mesh,
        in_specs=(
            P(("groups", "attn"), "expert"),
            P(("groups", "attn"), None),
            P(("groups", "attn"), None),
            P("attn", "expert", None),
            P("attn", "expert", None),
            P("attn", None, "expert"),
            P(("groups", "attn", "expert"), None, None),
            P(("groups", "attn", "expert"), None, None, None),
            P(("groups", "attn", "expert"), None, None, None),
            P(("groups", "attn", "expert")),
        ),
        out_specs=(P(("groups", "attn"), "expert"), P(("groups", "attn", "expert"), None)),
        check_vma=False,
    )
```
